32 devices in a mesh: dp: 8 (over z, y), tensor: 4 (over x, core).
Axes of the slice: x: 2, y: 2, z: 4, core: 2. Of those that a mesh axis runs over, the one named last changes fastest.
Arguments:
- tokens: float32 [50176, 512], P(('dp', 'tensor')), may hold values from -6 to 6
- out_grad: float32 [50176, 512], P(('dp', 'tensor')), may hold values from -6 to 6
- qkv_weight: float32 [512, 4, 384], P(None, 'tensor', 'dp'), may hold values from -0.25 to 0.25
- proj_weight: float32 [4, 128, 512], P('tensor', 'dp'), may hold values from -0.75 to 0.75
- fc1_weight: float32 [512, 4, 512], P(None, 'tensor', 'dp'), may hold values from -0.25 to 0.25
- fc2_weight: float32 [4, 512, 512], P('tensor', 'dp'), may hold values from -0.125 to 0.125
- qkv_momentum: float32 [512, 4, 384], P(None, 'tensor', 'dp'), may hold values from -3 to 3
- proj_momentum: float32 [4, 128, 512], P('tensor', 'dp'), may hold values from -3 to 3
- fc1_momentum: float32 [512, 4, 512], P(None, 'tensor', 'dp'), may hold values from -3 to 3
- fc2_momentum: float32 [4, 512, 512], P('tensor', 'dp'), may hold values from -3 to 3
- norm_gains: float32 [2, 512], replicated, may hold values from 0.5 to 1.5
- shift_biases: float32 [4, 512], replicated, may hold values from -3 to 3
- head_biases: float32 [2, 512], replicated, may hold values from -3 to 3
- hidden_bias: float32 [2048], replicated, may hold values from -3 to 3
- position_table: float32 [169, 16], replicated, may hold values from -5 to 5
- gain_momentum: float32 [2, 512], replicated, may hold values from -3 to 3
- shift_momentum: float32 [4, 512], replicated, may hold values from -3 to 3
- head_bias_momentum: float32 [2, 512], replicated, may hold values from -3 to 3
- hidden_bias_momentum: float32 [2048], replicated, may hold values from -3 to 3
- table_momentum: float32 [169, 16], replicated, may hold values from -3 to 3
- region_ids: int32 [14, 14], replicated, may hold values from 0 to 2
- position_index: int32 [49, 49], replicated, may hold values from 0 to 168
Outputs:
- out_tokens: float32 [50176, 512], P(('dp', 'tensor'))
- input_grad: float32 [50176, 512], P(('dp', 'tensor'))
- qkv_grad: float32 [512, 4, 384], P(None, 'tensor', 'dp')
- proj_grad: float32 [4, 128, 512], P('tensor', 'dp')
- fc1_grad: float32 [512, 4, 512], P(None, 'tensor', 'dp')
- fc2_grad: float32 [4, 512, 512], P('tensor', 'dp')
- qkv_new: float32 [512, 4, 384], P(None, 'tensor', 'dp')
- proj_new: float32 [4, 128, 512], P('tensor', 'dp')
- fc1_new: float32 [512, 4, 512], P(None, 'tensor', 'dp')
- fc2_new: float32 [4, 512, 512], P('tensor', 'dp')
- qkv_momentum_new: float32 [512, 4, 384], P(None, 'tensor', 'dp')
- proj_momentum_new: float32 [4, 128, 512], P('tensor', 'dp')
- fc1_momentum_new: float32 [512, 4, 512], P(None, 'tensor', 'dp')
- fc2_momentum_new: float32 [4, 512, 512], P('tensor', 'dp')
- gain_grad: float32 [2, 512], replicated
- shift_grad: float32 [4, 512], replicated
- head_bias_grad: float32 [2, 512], replicated
- hidden_bias_grad: float32 [2048], replicated
- table_grad: float32 [169, 16], replicated
- gains_new: float32 [2, 512], replicated
- shifts_new: float32 [4, 512], replicated
- head_biases_new: float32 [2, 512], replicated
- hidden_bias_new: float32 [2048], replicated
- table_new: float32 [169, 16], replicated
- gain_momentum_new: float32 [2, 512], replicated
- shift_momentum_new: float32 [4, 512], replicated
- head_bias_momentum_new: float32 [2, 512], replicated
- hidden_bias_momentum_new: float32 [2048], replicated
- table_momentum_new: float32 [169, 16], replicated
The draws below stay inside these ranges and needn't reach their ends.
All inputs are finite; a program needn't handle non-finite values.
Results may differ from the reference program's by a relative error of at most 0.019.
Values may be sent and summed in bfloat16 or wider, within the bound.
A program may use at most 320 MiB of HBM per device.

```python
import math
import jax
import jax.numpy as jnp
from jax import lax

D = 512
HEADS = 16
FF = 2048
HEAD = 32
WIN = 7
SIDE = 14
SHIFT = 3
NS_STEPS = 5
GROUPS = 4
FG = 512
QKV_COLS = 384
TABLE = 169
IMAGES = 256
TOKENS = 50176
N_TENSOR = 4


def plant(values, own_key, least, top_value):
    index_at = [jax.random.randint(jax.random.fold_in(own_key, axis), (), 0, length) for axis, length in enumerate(values.shape)]
    longest = values.shape.index(max(values.shape))
    neighbour = index_at[:longest] + [(index_at[longest] + 1) % values.shape[longest]] + index_at[longest + 1:]
    return values.at[tuple(index_at)].set(least).at[tuple(neighbour)].set(top_value)


def shard_levels(key, shape, shards, low, high):
    level, own = 1.0, jax.random.fold_in(key, 6)
    for axis_at, shards_of in shards:
        heights = jnp.exp(jax.random.uniform(jax.random.fold_in(own, axis_at), (shards_of,), jnp.float32, low / len(shards), high / len(shards)))
        level = level * jnp.repeat(heights, shape[axis_at] // shards_of).reshape([-1 if axis == axis_at else 1 for axis in range(len(shape))])
    return level


def bell_draw(stream_key, extent, spread, reach, cuts=(), kind=jnp.bfloat16):
    drawn = jax.random.normal(stream_key, extent, jnp.float32) * spread
    if len(cuts) > 0:
        drawn = shard_levels(stream_key, extent, cuts, -0.22, 0.18) * drawn
    return jnp.clip(drawn, min=-reach, max=reach).astype(kind)


def setup_inputs(seed: int = 0) -> dict:
    keys = jax.random.split(jax.random.key(seed), 23)
    return {
        "tokens": bell_draw(keys[0], (TOKENS, D), 1.0, 6.0, ((0, 32),), jnp.float32),
        "out_grad": bell_draw(keys[1], (TOKENS, D), 1.0, 6.0, ((0, 32),), jnp.float32),
        "qkv_weight": bell_draw(keys[2], (D, GROUPS, QKV_COLS), D ** -0.5, 0.25, ((1, 4), (2, 8)), jnp.float32),
        "proj_weight": bell_draw(keys[3], (GROUPS, D // GROUPS, D), (D // 8) ** -0.5, 0.75, ((0, 4), (1, 8)), jnp.float32),
        "fc1_weight": bell_draw(keys[4], (D, GROUPS, FG), D ** -0.5, 0.25, ((1, 4), (2, 8)), jnp.float32),
        "fc2_weight": bell_draw(keys[5], (GROUPS, FG, D), FF ** -0.5, 0.125, ((0, 4), (1, 8)), jnp.float32),
        "qkv_momentum": bell_draw(keys[6], (D, GROUPS, QKV_COLS), (3.0 / IMAGES ** 0.5), 3.0, ((1, 4), (2, 8)), jnp.float32),
        "proj_momentum": bell_draw(keys[7], (GROUPS, D // GROUPS, D), (3.0 / IMAGES ** 0.5), 3.0, ((0, 4), (1, 8)), jnp.float32),
        "fc1_momentum": bell_draw(keys[8], (D, GROUPS, FG), (3.0 / IMAGES ** 0.5), 3.0, ((1, 4), (2, 8)), jnp.float32),
        "fc2_momentum": bell_draw(keys[9], (GROUPS, FG, D), (3.0 / IMAGES ** 0.5), 3.0, ((0, 4), (1, 8)), jnp.float32),
        "norm_gains": jnp.clip(1.0 + 0.1 * jax.random.normal(keys[10], (2, D), jnp.float32), 0.5, 1.5),
        "shift_biases": bell_draw(keys[11], (4, D), 0.5, 3.0, (), jnp.float32),
        "head_biases": bell_draw(keys[12], (2, D), 0.5, 3.0, (), jnp.float32),
        "hidden_bias": bell_draw(keys[13], (FF,), 0.5, 3.0, (), jnp.float32),
        "position_table": bell_draw(keys[14], (TABLE, HEADS), 1.0, 5.0, (), jnp.float32),
        "gain_momentum": bell_draw(keys[15], (2, D), (3.0 / IMAGES ** 0.5), 3.0, (), jnp.float32),
        "shift_momentum": bell_draw(keys[16], (4, D), (3.0 / IMAGES ** 0.5), 3.0, (), jnp.float32),
        "head_bias_momentum": bell_draw(keys[17], (2, D), (3.0 / IMAGES ** 0.5), 3.0, (), jnp.float32),
        "hidden_bias_momentum": bell_draw(keys[18], (FF,), (3.0 / IMAGES ** 0.5), 3.0, (), jnp.float32),
        "table_momentum": bell_draw(keys[19], (TABLE, HEADS), (3.0 / IMAGES ** 0.5), 3.0, (), jnp.float32),
        "region_ids": plant(jax.random.randint(keys[20], (SIDE, SIDE), 0, 3), jax.random.fold_in(keys[20], 1), 0, 2).astype(jnp.int32),
        "position_index": plant(jax.random.randint(keys[21], (WIN * WIN, WIN * WIN), 0, TABLE), jax.random.fold_in(keys[21], 1), 0, TABLE - 1).astype(jnp.int32),
    }


NORM_EPSILON = 1e-05
MASK_VALUE = -100.0
MUON_EPSILON = 1e-07
QUINTIC_FIRST = 3.4445
QUINTIC_SECOND = -4.775
QUINTIC_THIRD = 2.0315
MOMENTUM = 0.9
MATRIX_RATE = 0.5
VECTOR_RATE = 1.0
HIGHEST = lax.Precision.HIGHEST

def product(pattern, left_op, right_op):
    return jnp.einsum(pattern, left_op.astype(jnp.float32), right_op.astype(jnp.float32), precision=HIGHEST)

def gelu_tanh(values):
    return jax.nn.gelu(values, approximate=True)

def layer_norm(values, gain_row, shift_row):
    center = values - lax.optimization_barrier(jnp.mean(values, axis=-1, keepdims=True))
    inverse_std = lax.rsqrt(lax.optimization_barrier(jnp.mean(center * center, axis=-1, keepdims=True)) + NORM_EPSILON)
    whitened = center * inverse_std
    return (whitened, inverse_std, whitened * gain_row + shift_row)

def norm_backward(grad_out, whitened, inverse_std, gain_row):
    scaled = grad_out * gain_row
    centered = scaled - lax.optimization_barrier(jnp.mean(scaled, axis=-1, keepdims=True)) - whitened * lax.optimization_barrier(jnp.mean(scaled * whitened, axis=-1, keepdims=True))
    return inverse_std * centered

def to_windows(rows, shift_by):
    images_in = rows.shape[0] // (SIDE * SIDE)
    trailing = rows.shape[1:]
    layout = rows.reshape((images_in, SIDE, SIDE) + trailing)
    if shift_by:
        layout = jnp.roll(layout, (-shift_by, -shift_by), axis=(1, 2))
    across = SIDE // WIN
    layout = layout.reshape((images_in, across, WIN, across, WIN) + trailing)
    axes_order = (0, 1, 3, 2, 4) + tuple(range(5, 5 + len(trailing)))
    return layout.transpose(axes_order).reshape((images_in * across * across, WIN * WIN) + trailing)

def from_windows(windows, shift_by):
    across = SIDE // WIN
    images_in = windows.shape[0] // (across * across)
    trailing = windows.shape[2:]
    layout = windows.reshape((images_in, across, across, WIN, WIN) + trailing)
    axes_order = (0, 1, 3, 2, 4) + tuple(range(5, 5 + len(trailing)))
    layout = layout.transpose(axes_order).reshape((images_in, SIDE, SIDE) + trailing)
    if shift_by:
        layout = jnp.roll(layout, (shift_by, shift_by), axis=(1, 2))
    return layout.reshape((images_in * SIDE * SIDE,) + trailing)

def window_masks(region_ids):
    regions = to_windows(region_ids.reshape(SIDE * SIDE, 1), 0)[:, :, 0]
    return jnp.where(regions[:, :, None] == regions[:, None, :], 0.0, MASK_VALUE).astype(jnp.float32)

def group_total(group_terms):
    rounded = lax.optimization_barrier(group_terms.astype(jnp.bfloat16))
    return lax.optimization_barrier(jnp.sum(rounded.astype(jnp.float32), 0))

def attend_block(queries, keys_in, values_in, head_bias, block_mask):
    scores = product('wighd,wjghd->wghij', queries, keys_in) + head_bias[None] + block_mask[:, None, None]
    row_peak = lax.optimization_barrier(jnp.max(scores, axis=-1, keepdims=True))
    log_total = row_peak + jnp.log(lax.optimization_barrier(jnp.sum(jnp.exp(scores - row_peak), axis=-1, keepdims=True)))
    probs_low = jnp.exp(scores - log_total).astype(jnp.bfloat16)
    mixed_out = product('wghij,wjghd->wighd', probs_low, values_in)
    return (mixed_out.astype(jnp.bfloat16), log_total)

def attend_back(queries, keys_in, values_in, head_bias, block_mask, log_total, grad_out):
    scores = product('wighd,wjghd->wghij', queries, keys_in) + head_bias[None] + block_mask[:, None, None]
    probs_full = jnp.exp(scores - log_total)
    grad_values = product('wghij,wighd->wjghd', probs_full.astype(jnp.bfloat16), grad_out)
    grad_probs = product('wighd,wjghd->wghij', grad_out, values_in)
    centered = grad_probs - lax.optimization_barrier(jnp.sum(probs_full * grad_probs, axis=-1, keepdims=True))
    grad_scores = probs_full * centered
    rounded = grad_scores.astype(jnp.bfloat16)
    grad_queries = product('wghij,wjghd->wighd', rounded, keys_in) * HEAD ** (-0.5)
    grad_keys = product('wghij,wighd->wjghd', rounded, queries)
    return (jnp.stack([grad_queries, grad_keys, grad_values], 3), lax.optimization_barrier(jnp.sum(grad_scores, 0)))

def block_layout(qkv_windows, window_mask):
    windows_total = qkv_windows.shape[0]
    per_image = window_mask.shape[0]
    block_size = 16 if windows_total % 16 == 0 else per_image
    block_mask = jnp.tile(window_mask, (block_size // per_image, 1, 1))
    return (windows_total, block_size, block_mask)

def attention_all(qkv_windows, head_bias, window_mask):
    windows_total, block_size, block_mask = block_layout(qkv_windows, window_mask)
    shaped = qkv_windows.reshape((windows_total // block_size, block_size) + qkv_windows.shape[1:])

    def forward_one(window_block):
        return attend_block(window_block[:, :, :, 0], window_block[:, :, :, 1], window_block[:, :, :, 2], head_bias, block_mask)
    mixed_out, log_total = lax.map(forward_one, shaped)
    return (mixed_out.reshape((windows_total,) + mixed_out.shape[2:]), log_total)

def attention_back(qkv_windows, head_bias, window_mask, log_total, grad_mixed):
    windows_total, block_size, block_mask = block_layout(qkv_windows, window_mask)
    shaped = qkv_windows.reshape((windows_total // block_size, block_size) + qkv_windows.shape[1:])
    grad_shaped = grad_mixed.reshape((windows_total // block_size, block_size) + grad_mixed.shape[1:])

    def backward_one(pieces):
        window_block, log_block, grad_block = pieces
        return attend_back(window_block[:, :, :, 0], window_block[:, :, :, 1], window_block[:, :, :, 2], head_bias, block_mask, log_block, grad_block)
    grad_windows, grad_bias = lax.map(backward_one, (shaped, log_total, grad_shaped))
    return (grad_windows.reshape((windows_total,) + grad_windows.shape[2:]), lax.optimization_barrier(jnp.sum(grad_bias, 0)))

def block_pass(tokens, out_grad, w_qkv, w_proj, w_fc1, w_fc2, norm_gains, shift_biases, qkv_bias, fc1_bias, head_bias, window_mask):
    all_rows = tokens.shape[0]
    groups = w_qkv.shape[1]
    group_width = w_qkv.shape[2] // 3
    whitened_one, inverse_one, normed = layer_norm(tokens, norm_gains[0], shift_biases[0])
    rows_one = normed.astype(jnp.bfloat16)
    qkv_float = jnp.dot(rows_one, w_qkv.reshape(D, -1), preferred_element_type=jnp.float32) + qkv_bias.reshape(-1)
    qkv_float = qkv_float.reshape(all_rows, groups, 3, group_width)
    qkv_round = jnp.concatenate([qkv_float[:, :, :1] * HEAD ** (-0.5), qkv_float[:, :, 1:]], 2).astype(jnp.bfloat16)
    qkv_windows = to_windows(qkv_round, SHIFT).reshape(-1, WIN * WIN, groups, 3, group_width // HEAD, HEAD)
    mixed_out, log_total = attention_all(qkv_windows, head_bias, window_mask)
    joined = from_windows(mixed_out.reshape(-1, WIN * WIN, groups, group_width), SHIFT)
    attn_out = group_total(product('tgc,gcd->gtd', joined, w_proj))
    middle = tokens + attn_out + shift_biases[2]
    whitened_two, inverse_two, normed = layer_norm(middle, norm_gains[1], shift_biases[1])
    rows_two = normed.astype(jnp.bfloat16)
    pre_act = jnp.dot(rows_two, w_fc1.reshape(D, -1), preferred_element_type=jnp.float32) + fc1_bias
    hidden = gelu_tanh(pre_act).astype(jnp.bfloat16).reshape(all_rows, groups, -1)
    mlp_out = group_total(product('tgf,gfd->gtd', hidden, w_fc2))
    output = middle + mlp_out + shift_biases[3]
    grad_rows = out_grad.astype(jnp.bfloat16)
    grad_fc2 = product('tgf,td->gfd', hidden, grad_rows)
    grad_hidden = product('td,gfd->tgf', grad_rows, w_fc2).reshape(all_rows, -1)
    grad_pre = jax.vjp(gelu_tanh, pre_act)[1](grad_hidden)[0]
    pre_round = grad_pre.astype(jnp.bfloat16)
    grad_fc1 = product('td,tf->df', rows_two, pre_round).reshape(D, groups, -1)
    grad_norm_two = group_total(product('tgf,dgf->gtd', pre_round.reshape(all_rows, groups, -1), w_fc1))
    grad_middle = out_grad + norm_backward(grad_norm_two, whitened_two, inverse_two, norm_gains[1])
    middle_rows = grad_middle.astype(jnp.bfloat16)
    grad_proj = product('tgc,td->gcd', joined, middle_rows)
    grad_joined = product('td,gcd->tgc', middle_rows, w_proj).astype(jnp.bfloat16)
    grad_mixed = to_windows(grad_joined, SHIFT).reshape(-1, WIN * WIN, groups, group_width // HEAD, HEAD)
    grad_windows, grad_bias = attention_back(qkv_windows, head_bias, window_mask, log_total, grad_mixed)
    grad_qkv = from_windows(grad_windows.reshape(-1, WIN * WIN, groups, 3, group_width), SHIFT)
    head_grad = jnp.stack([lax.optimization_barrier(jnp.sum(grad_qkv[:, :, 0], 0)), lax.optimization_barrier(jnp.sum(grad_qkv[:, :, 2], 0))])
    qkv_round_grad = grad_qkv.astype(jnp.bfloat16).reshape(all_rows, groups, -1)
    grad_qkv_w = product('td,tgc->dgc', rows_one, qkv_round_grad)
    grad_norm_one = group_total(product('tgc,dgc->gtd', qkv_round_grad, w_qkv))
    grad_input = grad_middle + norm_backward(grad_norm_one, whitened_one, inverse_one, norm_gains[0])
    gain_grad = jnp.stack([lax.optimization_barrier(jnp.sum(grad_norm_one * whitened_one, 0)), lax.optimization_barrier(jnp.sum(grad_norm_two * whitened_two, 0))])
    shift_grad = jnp.stack([lax.optimization_barrier(jnp.sum(grad_norm_one, 0)), lax.optimization_barrier(jnp.sum(grad_norm_two, 0)), lax.optimization_barrier(jnp.sum(grad_middle, 0)), lax.optimization_barrier(jnp.sum(out_grad, 0))])
    hidden_grad = lax.optimization_barrier(jnp.sum(grad_pre, 0))
    return ((output, grad_input), (grad_qkv_w, grad_proj, grad_fc1, grad_fc2, gain_grad, shift_grad, head_grad, hidden_grad, grad_bias))

def gram_of(matrix, is_wide):
    if is_wide:
        return jnp.dot(matrix, matrix.T, precision=HIGHEST)
    return jnp.dot(matrix.T, matrix, precision=HIGHEST)

def quintic(matrix, gram_sum, is_wide):
    poly_term = QUINTIC_SECOND * gram_sum + QUINTIC_THIRD * jnp.dot(gram_sum, gram_sum, precision=HIGHEST)
    if is_wide:
        return QUINTIC_FIRST * matrix + jnp.dot(poly_term, matrix, precision=HIGHEST)
    return QUINTIC_FIRST * matrix + jnp.dot(matrix, poly_term, precision=HIGHEST)

def orthogonalize(matrix, is_wide):
    current = matrix / (jnp.sqrt(jnp.sum(matrix * matrix)) + MUON_EPSILON)
    for ns_turn in range(NS_STEPS):
        current = quintic(current, gram_of(current, is_wide), is_wide)
    return current

def reference(tokens, out_grad, qkv_weight, proj_weight, fc1_weight, fc2_weight, qkv_momentum, proj_momentum, fc1_momentum, fc2_momentum, norm_gains, shift_biases, head_biases, hidden_bias, position_table, gain_momentum, shift_momentum, head_bias_momentum, hidden_bias_momentum, table_momentum, region_ids, position_index):
    groups = N_TENSOR
    group_width = D // groups
    heads_group = HEADS // groups
    w_qkv = qkv_weight.astype(jnp.bfloat16)
    w_proj = proj_weight.astype(jnp.bfloat16)
    w_fc1 = fc1_weight.astype(jnp.bfloat16)
    w_fc2 = fc2_weight.astype(jnp.bfloat16)
    split_bias = head_biases.reshape(2, groups, group_width)
    qkv_bias = jnp.stack([split_bias[0], jnp.zeros_like(split_bias[0]), split_bias[1]], 1).reshape(groups, -1)
    table_rows = position_table.shape[0]
    onehot = (position_index.reshape(-1)[:, None] == jnp.arange(table_rows, dtype=jnp.int32)[None, :]).astype(jnp.float32)
    head_bias = jnp.dot(onehot, position_table, precision=HIGHEST).T.reshape(groups, heads_group, WIN * WIN, WIN * WIN)
    window_mask = window_masks(region_ids)
    block_rows = 16 * SIDE * SIDE
    token_blocks = tokens.reshape(-1, block_rows, D)
    grad_blocks = out_grad.reshape(-1, block_rows, D)

    def scan_step(carry, pieces):
        outs_block, grads_block = block_pass(pieces[0], pieces[1], w_qkv, w_proj, w_fc1, w_fc2, norm_gains, shift_biases, qkv_bias, hidden_bias, head_bias, window_mask)
        return (tuple((total + grad_part for total, grad_part in zip(carry, grads_block))), outs_block)
    zero_sums = (jnp.zeros((D, groups, 3 * group_width), jnp.float32), jnp.zeros((groups, group_width, D), jnp.float32), jnp.zeros((D, groups, FF // groups), jnp.float32), jnp.zeros((groups, FF // groups, D), jnp.float32), jnp.zeros((2, D), jnp.float32), jnp.zeros((4, D), jnp.float32), jnp.zeros((2, groups, group_width), jnp.float32), jnp.zeros((FF,), jnp.float32), jnp.zeros((groups, heads_group, WIN * WIN, WIN * WIN), jnp.float32))
    sums, outs_all = lax.scan(scan_step, zero_sums, (token_blocks, grad_blocks))
    out_tokens = outs_all[0].reshape(-1, D)
    input_grad = outs_all[1].reshape(-1, D)
    weight_grads = tuple((member / IMAGES for member in sums[:4]))
    gain_grad = sums[4] / IMAGES
    shift_grad = sums[5] / IMAGES
    head_bias_grad = sums[6].reshape(2, D) / IMAGES
    hidden_bias_grad = sums[7] / IMAGES
    table_grad = jnp.dot(onehot.T, sums[8].reshape(HEADS, -1).T, precision=HIGHEST) / IMAGES
    weights_old = (qkv_weight, proj_weight, fc1_weight, fc2_weight)
    momenta_old = (qkv_momentum, proj_momentum, fc1_momentum, fc2_momentum)
    momenta_new = tuple((MOMENTUM * old_state + grad_part for old_state, grad_part in zip(momenta_old, weight_grads)))
    matrices = (momenta_new[0].reshape(D, -1), momenta_new[1].reshape(-1, D), momenta_new[2].reshape(D, -1), momenta_new[3].reshape(-1, D))
    wide_flags = (True, False, True, False)
    factors = (math.sqrt(max(1.0, 3.0)), 1.0, math.sqrt(max(1.0, FF / D)), math.sqrt(max(1.0, D / FF)))
    weights_new = tuple((weight - MATRIX_RATE * factor * orthogonalize(matrix, is_wide).reshape(weight.shape) for weight, matrix, is_wide, factor in zip(weights_old, matrices, wide_flags, factors)))
    small_grads = (gain_grad, shift_grad, head_bias_grad, hidden_bias_grad, table_grad)
    small_params = (norm_gains, shift_biases, head_biases, hidden_bias, position_table)
    small_moms = (gain_momentum, shift_momentum, head_bias_momentum, hidden_bias_momentum, table_momentum)
    small_moms_new = tuple((MOMENTUM * old_state + grad_part for old_state, grad_part in zip(small_moms, small_grads)))
    small_new = tuple((param - VECTOR_RATE * state for param, state in zip(small_params, small_moms_new)))
    return (out_tokens, input_grad, weight_grads[0], weight_grads[1], weight_grads[2], weight_grads[3], weights_new[0], weights_new[1], weights_new[2], weights_new[3], momenta_new[0], momenta_new[1], momenta_new[2], momenta_new[3], gain_grad, shift_grad, head_bias_grad, hidden_bias_grad, table_grad, small_new[0], small_new[1], small_new[2], small_new[3], small_new[4], small_moms_new[0], small_moms_new[1], small_moms_new[2], small_moms_new[3], small_moms_new[4])
```

```python
import functools
import math

import jax
import jax.numpy as jnp
from jax import lax
from jax.experimental import pallas as pl
from jax.experimental.pallas import tpu as pltpu
from jax.sharding import PartitionSpec as P

D = 512
HEADS = 16
FF = 2048
HEAD = 32
WIN = 7
SIDE = 14
SHIFT = 3
NS_STEPS = 5

NORM_EPSILON = 1e-05
MASK_VALUE = -100.0
MUON_EPSILON = 1e-07
QUINTIC = (3.4445, -4.775, 2.0315)
MOMENTUM = 0.9
MATRIX_RATE = 0.5
VECTOR_RATE = 1.0

AREA = SIDE * SIDE
SPOTS = WIN * WIN
ACROSS = SIDE // WIN
WINDOWS = ACROSS * ACROSS
SLOT = 64
LANES = 128
OCT = 8
OCTS = HEADS // OCT
OCT_W = OCT * HEAD
OCT_S = OCT * SLOT
PAD_SCORE = -1e30
STEP_IMAGES = 2
STEP_ROWS = STEP_IMAGES * AREA
STEP_SLOTS = STEP_IMAGES * WINDOWS * SLOT
PART = 128
GROUPS = 4
F32 = jnp.float32
BF16 = jnp.bfloat16
VMEM_LIMIT = 60 * 1024 * 1024


def window_pieces():
    pieces = []
    for down in range(ACROSS):
        for over in range(ACROSS):
            for line in range(WIN):
                src_row = (down * WIN + line + SHIFT) % SIDE
                column = 0
                while column < WIN:
                    src_col = (over * WIN + column + SHIFT) % SIDE
                    length = min(WIN - column, SIDE - src_col)
                    slot = (down * ACROSS + over) * SLOT + line * WIN + column
                    pieces.append((slot, src_row * SIDE + src_col, length))
                    column += length
    return pieces


PIECES = window_pieces()


def dot_nn(a, b):
    return lax.dot_general(a, b, (((1,), (0,)), ((), ())), preferred_element_type=F32)


def dot_nt(a, b):
    return lax.dot_general(a, b, (((1,), (1,)), ((), ())), preferred_element_type=F32)


def dot_tn(a, b):
    return lax.dot_general(a, b, (((0,), (0,)), ((), ())), preferred_element_type=F32)


def row_mean(values):
    return jnp.mean(values, axis=-1, keepdims=True)


def whiten(values):
    center = values - row_mean(values)
    inverse = lax.rsqrt(row_mean(center * center) + NORM_EPSILON)
    return center * inverse, inverse


def into_slots(src_ref, dst_ref):
    for image in range(STEP_IMAGES):
        for slot, raster, length in PIECES:
            dst_ref[image * WINDOWS * SLOT + slot : image * WINDOWS * SLOT + slot + length, :] = src_ref[
                image * AREA + raster : image * AREA + raster + length, :
            ]


def out_of_slots(src_ref, dst_ref):
    for image in range(STEP_IMAGES):
        for slot, raster, length in PIECES:
            dst_ref[image * AREA + raster : image * AREA + raster + length, :] = src_ref[
                image * WINDOWS * SLOT + slot : image * WINDOWS * SLOT + slot + length, :
            ]


def head_mask(order):
    rows = lax.broadcasted_iota(jnp.int32, (SLOT, OCT_W), 1) // HEAD
    return jnp.concatenate([(rows == head).astype(F32) for head in order], axis=0).astype(BF16)


def spread(values, mask_ref):
    return jnp.concatenate([values] * OCT, axis=0) * mask_ref[...]


def lane_iota(rows):
    return lax.broadcasted_iota(jnp.int32, (rows, LANES), 1)


def build_bias(region_ref, index_ref, table_ref, bias_ref, idx_scr, tab_scr):
    idx_scr[...] = jnp.zeros_like(idx_scr)
    idx_scr[0:SPOTS, 0:SPOTS] = index_ref[...].astype(F32)
    heads, rows = table_ref.shape
    tab_scr[...] = jnp.zeros_like(tab_scr)
    tab_scr[:, 0:rows] = table_ref[...]
    by_head = tab_scr[...]
    index = idx_scr[...].T[0:SLOT, :]
    lanes = lane_iota(SLOT)
    index = jnp.where(lanes < SLOT, index, pltpu.roll(index, SLOT, 1)).astype(jnp.int32)
    sublanes = lax.broadcasted_iota(jnp.int32, (SLOT, LANES), 0)
    spot = lanes % SLOT
    masks = []
    for down in range(ACROSS):
        for over in range(ACROSS):
            row_ids = jnp.full((SLOT, LANES), -1, jnp.int32)
            col_ids = jnp.full((SLOT, LANES), -1, jnp.int32)
            for at in range(SPOTS):
                value = region_ref[down * WIN + at // WIN, over * WIN + at % WIN]
                row_ids = jnp.where(sublanes == at, value, row_ids)
                col_ids = jnp.where(spot == at, value, col_ids)
            masks.append(
                jnp.where(sublanes < SPOTS, jnp.where(row_ids == col_ids, 0.0, MASK_VALUE), PAD_SCORE)
            )
    low = index < LANES
    index_low = jnp.where(low, index, 0)
    index_high = jnp.where(low, 0, index - LANES)

    def gathered(head):
        first = jnp.broadcast_to(by_head[head : head + 1, 0:LANES], (SLOT, LANES))
        second = jnp.broadcast_to(by_head[head : head + 1, LANES : 2 * LANES], (SLOT, LANES))
        return jnp.where(
            low,
            jnp.take_along_axis(first, index_low, axis=1),
            jnp.take_along_axis(second, index_high, axis=1),
        )

    for octet in range(OCTS):
        for pair in range(OCT // 2):
            head = octet * OCT + 2 * pair
            tile = jnp.where(lanes < SLOT, gathered(head), gathered(head + 1))
            for window in range(WINDOWS):
                bias_ref[window, octet, :, pair * LANES : (pair + 1) * LANES] = tile + masks[window]


TURNED = (0, 2, 1, 3, 4, 6, 5, 7)


def turned(values):
    tiles = []
    for at in range(0, OCT_S, 2 * LANES):
        both = jnp.concatenate([values[:, at : at + LANES], values[:, at + LANES : at + 2 * LANES]], axis=0).T
        tiles += [both[0:SLOT, :], both[SLOT:, :]]
    return jnp.concatenate(tiles, axis=1)


def attention_forward_kernel(
    x_ref,
    wqkv_ref,
    wproj_ref,
    gain_ref,
    shift_ref,
    qkvb_ref,
    table_ref,
    index_ref,
    region_ref,
    y_ref,
    xs_ref,
    qkv_ref,
    p_ref,
    o_ref,
    bias_scr,
    idx_scr,
    tab_scr,
    mask_scr,
    turn_scr,
    y_scr,
):
    @pl.when(pl.program_id(0) == 0)
    def _():
        build_bias(region_ref, index_ref, table_ref, bias_scr, idx_scr, tab_scr)
        mask_scr[...] = head_mask(range(OCT))
        turn_scr[...] = head_mask(TURNED)

    xs_ref[...] = jnp.zeros_like(xs_ref)
    into_slots(x_ref, xs_ref)
    white, _ = whiten(xs_ref[...])
    a1 = (white * gain_ref[0:1, :] + shift_ref[0:1, :]).astype(BF16)
    scale = HEAD ** (-0.5)
    for half in range(2):
        columns = 3 * PART * GROUPS // 2
        u = dot_nt(a1, wqkv_ref[half * columns : (half + 1) * columns, :])
        for inner in range(GROUPS // 2):
            group = half * (GROUPS // 2) + inner
            for part in range(3):
                piece = u[:, (inner * 3 + part) * PART : (inner * 3 + part + 1) * PART]
                if part == 0:
                    piece = (piece + qkvb_ref[0:1, group * PART : (group + 1) * PART]) * scale
                elif part == 2:
                    piece = piece + qkvb_ref[1:2, group * PART : (group + 1) * PART]
                at = part * D + group * PART
                qkv_ref[:, at : at + PART] = piece.astype(BF16)

    real_query = (lax.broadcasted_iota(jnp.int32, (1, OCT_S), 1) % SLOT < SPOTS).astype(F32)

    def one_window(at, carry):
        rows = pl.ds(pl.multiple_of(at * SLOT, SLOT), SLOT)
        for octet in range(OCTS):
            q = qkv_ref[rows, octet * OCT_W : (octet + 1) * OCT_W]
            k = qkv_ref[rows, D + octet * OCT_W : D + (octet + 1) * OCT_W]
            v = qkv_ref[rows, 2 * D + octet * OCT_W : 2 * D + (octet + 1) * OCT_W]
            scores = dot_nt(k, spread(q, mask_scr)) + bias_scr[lax.rem(at, WINDOWS), octet]
            grown = jnp.exp(scores - jnp.max(scores, axis=0, keepdims=True))
            probs = grown * (real_query / jnp.sum(grown, axis=0, keepdims=True))
            p_ref[rows, octet * OCT_S : (octet + 1) * OCT_S] = probs.astype(BF16)
            o_ref[rows, octet * OCT_W : (octet + 1) * OCT_W] = dot_nn(
                turned(probs).astype(BF16), spread(v, turn_scr)
            ).astype(BF16)
        return carry

    lax.fori_loop(0, STEP_IMAGES * WINDOWS, one_window, 0)
    y_scr[...] = xs_ref[...] + dot_nn(o_ref[...], wproj_ref[...]) + shift_ref[2:3, :]
    out_of_slots(y_scr, y_ref)


def mlp_kernel(
    y_ref,
    e_ref,
    w1_ref,
    w2_ref,
    gain_ref,
    shift_ref,
    hb_ref,
    out_ref,
    dy_ref,
    g1_ref,
    g2_ref,
    hsum_ref,
    sums_ref,
    acc1,
    acc2,
    m_scr,
    da_scr,
    a2_scr,
    e_scr,
):
    step = pl.program_id(0)

    @pl.when(step == 0)
    def _():
        acc1[...] = jnp.zeros_like(acc1)
        acc2[...] = jnp.zeros_like(acc2)
        hsum_ref[...] = jnp.zeros_like(hsum_ref)
        sums_ref[...] = jnp.zeros_like(sums_ref)

    white, inverse = whiten(y_ref[...])
    a2_scr[...] = (white * gain_ref[1:2, :] + shift_ref[1:2, :]).astype(BF16)
    e_scr[...] = e_ref[...].astype(BF16)
    m_scr[...] = jnp.zeros_like(m_scr)
    da_scr[...] = jnp.zeros_like(da_scr)
    root = math.sqrt(2.0 / math.pi)
    width = 512

    def chunk(c, carry):
        at = pl.ds(pl.multiple_of(c * width, width), width)
        w1, w2 = w1_ref[at, :], w2_ref[at, :]
        a2, e = a2_scr[...], e_scr[...]
        z = dot_nt(a2, w1) + hb_ref[0:1, at]
        square = z * z
        t = jnp.tanh(z * (root + (root * 0.044715) * square))
        half = 0.5 * z
        f = (half + half * t).astype(BF16)
        slope = 0.5 + 0.5 * t + half * (1.0 - t * t) * (root + (3.0 * root * 0.044715) * square)
        dz = dot_nt(e, w2) * slope
        hsum_ref[0:1, at] += jnp.sum(dz, axis=0, keepdims=True)
        dz = dz.astype(BF16)
        m_scr[...] += dot_nn(f, w2)
        da_scr[...] += dot_nn(dz, w1)
        acc2[at, :] += dot_tn(f, e)
        acc1[at, :] += dot_tn(dz, a2)
        return carry

    lax.fori_loop(0, w1_ref.shape[0] // width, chunk, 0)
    white, inverse = whiten(y_ref[...])
    out_ref[...] = y_ref[...] + m_scr[...] + shift_ref[3:4, :]
    da = da_scr[...]
    t2 = da * gain_ref[1:2, :]
    dy = e_ref[...] + inverse * (t2 - row_mean(t2) - white * row_mean(t2 * white))
    dy_ref[...] = dy
    sums_ref[0:1, :] += jnp.sum(da * white, axis=0, keepdims=True)
    sums_ref[1:2, :] += jnp.sum(da, axis=0, keepdims=True)
    sums_ref[2:3, :] += jnp.sum(dy, axis=0, keepdims=True)
    sums_ref[3:4, :] += jnp.sum(e_ref[...], axis=0, keepdims=True)

    @pl.when(step == pl.num_programs(0) - 1)
    def _():
        g1_ref[...] = acc1[...].astype(BF16)
        g2_ref[...] = acc2[...].astype(BF16)


def attention_backward_kernel(
    dy_ref,
    xs_ref,
    qkv_ref,
    p_ref,
    o_ref,
    wqkv_ref,
    wproj_ref,
    gain_ref,
    shift_ref,
    gin_ref,
    gqkv_ref,
    gproj_ref,
    dbias_ref,
    hsum_ref,
    sums_ref,
    accq,
    accp,
    dy_scr,
    do_scr,
    du_scr,
    mask_scr,
    turn_scr,
    g_scr,
):
    step = pl.program_id(0)

    @pl.when(step == 0)
    def _():
        mask_scr[...] = head_mask(range(OCT))
        turn_scr[...] = head_mask(TURNED)
        accq[...] = jnp.zeros_like(accq)
        accp[...] = jnp.zeros_like(accp)
        dbias_ref[...] = jnp.zeros_like(dbias_ref)
        hsum_ref[...] = jnp.zeros_like(hsum_ref)
        sums_ref[...] = jnp.zeros_like(sums_ref)
        dy_scr[...] = jnp.zeros_like(dy_scr)

    into_slots(dy_ref, dy_scr)
    dr = dy_scr[...].astype(BF16)
    do_scr[...] = dot_nt(dr, wproj_ref[...]).astype(BF16)
    accp[...] += dot_tn(o_ref[...], dr)
    scale = HEAD ** (-0.5)

    def one_window(at, carry):
        rows = pl.ds(pl.multiple_of(at * SLOT, SLOT), SLOT)
        for octet in range(OCTS):
            q = qkv_ref[rows, octet * OCT_W : (octet + 1) * OCT_W]
            k = qkv_ref[rows, D + octet * OCT_W : D + (octet + 1) * OCT_W]
            v = qkv_ref[rows, 2 * D + octet * OCT_W : 2 * D + (octet + 1) * OCT_W]
            do = do_scr[rows, octet * OCT_W : (octet + 1) * OCT_W]
            probs = p_ref[rows, octet * OCT_S : (octet + 1) * OCT_S]
            wide_do = spread(do, mask_scr)
            weighted = probs.astype(F32) * dot_nt(v, wide_do)
            ds = weighted - probs.astype(F32) * jnp.sum(weighted, axis=0, keepdims=True)
            dbias_ref[octet] += ds
            dq = dot_nn(turned(ds).astype(BF16), spread(k, turn_scr)) * scale
            dk = dot_nn(ds.astype(BF16), spread(q, mask_scr))
            dv = dot_nn(probs, wide_do)
            lanes = slice(octet * OCT_W, (octet + 1) * OCT_W)
            hsum_ref[0:1, lanes] += jnp.sum(dq, axis=0, keepdims=True)
            hsum_ref[1:2, lanes] += jnp.sum(dv, axis=0, keepdims=True)
            for part, grad in enumerate((dq, dk, dv)):
                for inner in range(OCT_W // PART):
                    group = octet * (OCT_W // PART) + inner
                    at_col = (group * 3 + part) * PART
                    du_scr[rows, at_col : at_col + PART] = grad[
                        :, inner * PART : (inner + 1) * PART
                    ].astype(BF16)
        return carry

    lax.fori_loop(0, STEP_IMAGES * WINDOWS, one_window, 0)
    white, inverse = whiten(xs_ref[...])
    a1 = (white * gain_ref[0:1, :] + shift_ref[0:1, :]).astype(BF16)
    accq[...] += dot_tn(du_scr[...], a1)
    da = dot_nn(du_scr[...], wqkv_ref[...])
    t1 = da * gain_ref[0:1, :]
    g_scr[...] = dy_scr[...] + inverse * (t1 - row_mean(t1) - white * row_mean(t1 * white))
    out_of_slots(g_scr, gin_ref)
    sums_ref[0:1, :] += jnp.sum(da * white, axis=0, keepdims=True)
    sums_ref[1:2, :] += jnp.sum(da, axis=0, keepdims=True)

    @pl.when(step == pl.num_programs(0) - 1)
    def _():
        gqkv_ref[...] = accq[...].astype(BF16)
        gproj_ref[...] = accp[...].astype(BF16)


def whole(shape):
    return pl.BlockSpec(shape, lambda i: (0,) * len(shape))


def rows_of(rows, columns):
    return pl.BlockSpec((rows, columns), lambda i: (i, 0))


def shape_of(shape, dtype):
    return jax.ShapeDtypeStruct(shape, dtype)


PARAMS = pltpu.CompilerParams(dimension_semantics=("arbitrary",), vmem_limit_bytes=VMEM_LIMIT)


def attention_forward(tokens, wqkv, wproj, gains, shifts, head_biases, table, index, regions):
    steps = tokens.shape[0] // STEP_ROWS
    slots = steps * STEP_SLOTS
    return pl.pallas_call(
        attention_forward_kernel,
        grid=(steps,),
        out_shape=(
            shape_of(tokens.shape, F32),
            shape_of((slots, D), F32),
            shape_of((slots, 3 * D), BF16),
            shape_of((slots, OCTS * OCT_S), BF16),
            shape_of((slots, D), BF16),
        ),
        in_specs=[
            rows_of(STEP_ROWS, D),
            whole(wqkv.shape),
            whole(wproj.shape),
            whole(gains.shape),
            whole(shifts.shape),
            whole(head_biases.shape),
            whole(table.shape),
            whole(index.shape),
            pl.BlockSpec(memory_space=pltpu.SMEM),
        ],
        out_specs=(
            rows_of(STEP_ROWS, D),
            rows_of(STEP_SLOTS, D),
            rows_of(STEP_SLOTS, 3 * D),
            rows_of(STEP_SLOTS, OCTS * OCT_S),
            rows_of(STEP_SLOTS, D),
        ),
        scratch_shapes=[
            pltpu.VMEM((WINDOWS, OCTS, SLOT, OCT_S), F32),
            pltpu.VMEM((LANES, LANES), F32),
            pltpu.VMEM((HEADS, 2 * LANES), F32),
            pltpu.VMEM((OCT_S, OCT_W), BF16),
            pltpu.VMEM((OCT_S, OCT_W), BF16),
            pltpu.VMEM((STEP_SLOTS, D), F32),
        ],
        compiler_params=PARAMS,
        name="attention_forward",
    )(tokens, wqkv, wproj, gains, shifts, head_biases, table, index, regions)


def mlp(middle, out_grad, w1, w2, gains, shifts, hidden_bias):
    steps = middle.shape[0] // STEP_ROWS
    hidden = w1.shape[0]
    return pl.pallas_call(
        mlp_kernel,
        grid=(steps,),
        out_shape=(
            shape_of(middle.shape, F32),
            shape_of(middle.shape, F32),
            shape_of(w1.shape, BF16),
            shape_of(w2.shape, BF16),
            shape_of((1, hidden), F32),
            shape_of((4, D), F32),
        ),
        in_specs=[
            rows_of(STEP_ROWS, D),
            rows_of(STEP_ROWS, D),
            whole(w1.shape),
            whole(w2.shape),
            whole(gains.shape),
            whole(shifts.shape),
            whole((1, hidden)),
        ],
        out_specs=(
            rows_of(STEP_ROWS, D),
            rows_of(STEP_ROWS, D),
            whole(w1.shape),
            whole(w2.shape),
            whole((1, hidden)),
            whole((4, D)),
        ),
        scratch_shapes=[
            pltpu.VMEM(w1.shape, F32),
            pltpu.VMEM(w2.shape, F32),
            pltpu.VMEM((STEP_ROWS, D), F32),
            pltpu.VMEM((STEP_ROWS, D), F32),
            pltpu.VMEM((STEP_ROWS, D), BF16),
            pltpu.VMEM((STEP_ROWS, D), BF16),
        ],
        compiler_params=PARAMS,
        name="mlp",
    )(middle, out_grad, w1, w2, gains, shifts, hidden_bias.reshape(1, hidden))


def attention_backward(dy, xs, qkv, probs, mixed, wqkv, wproj, gains, shifts):
    steps = dy.shape[0] // STEP_ROWS
    return pl.pallas_call(
        attention_backward_kernel,
        grid=(steps,),
        out_shape=(
            shape_of(dy.shape, F32),
            shape_of(wqkv.shape, BF16),
            shape_of(wproj.shape, BF16),
            shape_of((OCTS, SLOT, OCT_S), F32),
            shape_of((2, D), F32),
            shape_of((2, D), F32),
        ),
        in_specs=[
            rows_of(STEP_ROWS, D),
            rows_of(STEP_SLOTS, D),
            rows_of(STEP_SLOTS, 3 * D),
            rows_of(STEP_SLOTS, OCTS * OCT_S),
            rows_of(STEP_SLOTS, D),
            whole(wqkv.shape),
            whole(wproj.shape),
            whole(gains.shape),
            whole(shifts.shape),
        ],
        out_specs=(
            rows_of(STEP_ROWS, D),
            whole(wqkv.shape),
            whole(wproj.shape),
            whole((OCTS, SLOT, OCT_S)),
            whole((2, D)),
            whole((2, D)),
        ),
        scratch_shapes=[
            pltpu.VMEM(wqkv.shape, F32),
            pltpu.VMEM(wproj.shape, F32),
            pltpu.VMEM((STEP_SLOTS, D), F32),
            pltpu.VMEM((STEP_SLOTS, D), BF16),
            pltpu.VMEM((STEP_SLOTS, 3 * D), BF16),
            pltpu.VMEM((OCT_S, OCT_W), BF16),
            pltpu.VMEM((OCT_S, OCT_W), BF16),
            pltpu.VMEM((STEP_SLOTS, D), F32),
        ],
        compiler_params=PARAMS,
        name="attention_backward",
    )(dy, xs, qkv, probs, mixed, wqkv, wproj, gains, shifts)


def newton_schulz_kernel(g_ref, n_ref, w_ref, out_ref, x_scr, a_scr, *, rate):
    first, second, third = QUINTIC
    chunk = 512
    rows = g_ref.shape[0]

    def low(values):
        return values.astype(BF16)

    def gram(src_ref):
        a_scr[...] = jnp.zeros_like(a_scr)

        def add(at, carry):
            part = src_ref[pl.ds(pl.multiple_of(at * chunk, chunk), chunk), :]
            a_scr[...] += dot_tn(part, part)
            return carry

        lax.fori_loop(0, rows // chunk, add, 0)
        return a_scr[...]

    def advance(src_ref, factor, scale):
        factor = low(factor)

        def step(at, carry):
            at = pl.ds(pl.multiple_of(at * chunk, chunk), chunk)
            x_scr[at, :] = low(dot_nn(src_ref[at, :], factor) * scale)
            return carry

        lax.fori_loop(0, rows // chunk, step, 0)

    def bend(a):
        return second * a + third * dot_nn(low(a), low(a))

    diagonal = lax.broadcasted_iota(jnp.int32, (D, D), 0) == lax.broadcasted_iota(jnp.int32, (D, D), 1)

    def two_turns(a):
        b = bend(a)
        q = b + jnp.where(diagonal, first, 0.0)
        r = first * a + dot_nn(low(a), low(b))
        a = first * r + dot_nn(low(r), low(b))
        b = bend(a)
        return first * q + dot_nn(low(b), low(q))

    a = gram(g_ref)
    scale = 1.0 / (jnp.sqrt(jnp.sum(jnp.where(diagonal, a, 0.0))) + MUON_EPSILON)
    q = two_turns(a * scale * scale)
    advance(g_ref, q, scale)
    mine = dot_nn(low(n_ref[...]), low(q)) * scale
    q = two_turns(gram(x_scr))
    advance(x_scr, q, 1.0)
    mine = dot_nn(low(mine), low(q))
    b = bend(gram(x_scr))
    mine = first * mine + dot_nn(low(mine), low(b))
    out_ref[...] = w_ref[...] - rate * mine


def newton_schulz(gathered, slab, weight, factor):
    return pl.pallas_call(
        functools.partial(newton_schulz_kernel, rate=MATRIX_RATE * factor),
        out_shape=shape_of(slab.shape, F32),
        scratch_shapes=[pltpu.VMEM(gathered.shape, BF16), pltpu.VMEM((D, D), F32)],
        compiler_params=pltpu.CompilerParams(vmem_limit_bytes=VMEM_LIMIT),
        name="newton_schulz",
    )(gathered, slab, weight)


ALL = ("tensor", "dp")
WIDE = (True, False, True, False)
FACTORS = (
    math.sqrt(3.0),
    1.0,
    math.sqrt(max(1.0, FF / D)),
    math.sqrt(max(1.0, D / FF)),
)


def as_slab(block, wide):
    return block.reshape(D, -1).T if wide else block.reshape(-1, D)


def as_block(slab, like, wide):
    return (slab.T if wide else slab).reshape(like.shape)


def shards(
    tokens,
    out_grad,
    qkv_weight,
    proj_weight,
    fc1_weight,
    fc2_weight,
    qkv_momentum,
    proj_momentum,
    fc1_momentum,
    fc2_momentum,
    norm_gains,
    shift_biases,
    head_biases,
    hidden_bias,
    position_table,
    gain_momentum,
    shift_momentum,
    head_bias_momentum,
    hidden_bias_momentum,
    table_momentum,
    region_ids,
    position_index,
):
    devices = lax.axis_size("dp") * lax.axis_size("tensor")
    images = tokens.shape[0] // AREA * devices
    blocks = (qkv_weight, proj_weight, fc1_weight, fc2_weight)
    weights = tuple(as_slab(w, wide) for w, wide in zip(blocks, WIDE))
    momenta = tuple(
        as_slab(m, wide)
        for m, wide in zip((qkv_momentum, proj_momentum, fc1_momentum, fc2_momentum), WIDE)
    )
    wqkv, wproj, w1, w2 = (
        lax.all_gather(w.astype(BF16), ALL, axis=0, tiled=True) for w in weights
    )
    middle, xs, qkv, probs, mixed = attention_forward(
        tokens,
        wqkv,
        wproj,
        norm_gains,
        shift_biases,
        head_biases,
        position_table.T,
        position_index,
        region_ids,
    )
    output, dy, g1, g2, hidden_sum, sums2 = mlp(
        middle, out_grad, w1, w2, norm_gains, shift_biases, hidden_bias
    )
    input_grad, gqkv, gproj, dbias, head_sum, sums1 = attention_backward(
        dy, xs, qkv, probs, mixed, wqkv, wproj, norm_gains, shift_biases
    )
    by_head = (
        dbias.reshape(OCTS, SLOT, OCT, SLOT)[:, :SPOTS, :, :SPOTS]
        .transpose(0, 2, 3, 1)
        .reshape(HEADS, SPOTS * SPOTS)
    )
    onehot = (
        position_index.reshape(-1)[:, None]
        == jnp.arange(position_table.shape[0], dtype=jnp.int32)[None, :]
    ).astype(F32)
    table_part = jnp.dot(onehot.T, by_head.T, precision=lax.Precision.HIGHEST)
    smalls = lax.psum(
        (
            jnp.stack([sums1[0], sums2[0]]),
            jnp.stack([sums1[1], sums2[1], sums2[2], sums2[3]]),
            head_sum,
            hidden_sum.reshape(-1),
            table_part,
        ),
        ALL,
    )
    slab_grads = tuple(
        lax.psum_scatter(g, ALL, scatter_dimension=0, tiled=True).astype(F32) / images
        for g in (gqkv, gproj, g1, g2)
    )
    new_momenta = tuple(MOMENTUM * m + g for m, g in zip(momenta, slab_grads))
    new_weights = tuple(
        newton_schulz(lax.all_gather(n.astype(BF16), ALL, axis=0, tiled=True), n, w, factor)
        for n, w, factor in zip(new_momenta, weights, FACTORS)
    )
    small_grads = tuple(s / images for s in smalls)
    small_params = (norm_gains, shift_biases, head_biases, hidden_bias, position_table)
    small_moms = (
        gain_momentum,
        shift_momentum,
        head_bias_momentum,
        hidden_bias_momentum,
        table_momentum,
    )
    small_moms_new = tuple(MOMENTUM * m + g for m, g in zip(small_moms, small_grads))
    small_new = tuple(p - VECTOR_RATE * m for p, m in zip(small_params, small_moms_new))

    def placed(slabs):
        return tuple(as_block(s, like, wide) for s, like, wide in zip(slabs, blocks, WIDE))

    return (
        (output, input_grad)
        + placed(slab_grads)
        + placed(new_weights)
        + placed(new_momenta)
        + small_grads
        + small_new
        + small_moms_new
    )


def solution(mesh):
    rows = P(("dp", "tensor"), None)
    wide, tall = P(None, "tensor", "dp"), P("tensor", "dp", None)
    matrices = (wide, tall, wide, tall)
    return jax.shard_map(
        shards,
        mesh=mesh,
        in_specs=(rows, rows) + matrices * 2 + (P(),) * 12,
        out_specs=(rows, rows) + matrices * 3 + (P(),) * 15,
        check_vma=False,
    )
```

```python
import functools
import math

import jax
import jax.numpy as jnp
from jax import lax
from jax.experimental import pallas as pl
from jax.experimental.pallas import tpu as pltpu
from jax.sharding import PartitionSpec as P

D = 512
HEADS = 16
FF = 2048
HEAD = 32
WIN = 7
SIDE = 14
SHIFT = 3
NS_STEPS = 5

NORM_EPSILON = 1e-05
MASK_VALUE = -100.0
MUON_EPSILON = 1e-07
QUINTIC = (3.4445, -4.775, 2.0315)
MOMENTUM = 0.9
MATRIX_RATE = 0.5
VECTOR_RATE = 1.0

AREA = SIDE * SIDE
SPOTS = WIN * WIN
ACROSS = SIDE // WIN
WINDOWS = ACROSS * ACROSS
SLOT = 64
LANES = 128
OCT = 8
OCTS = HEADS // OCT
OCT_W = OCT * HEAD
OCT_S = OCT * SLOT
PAD_SCORE = -1e30
STEP_IMAGES = 2
STEP_ROWS = STEP_IMAGES * AREA
STEP_SLOTS = STEP_IMAGES * WINDOWS * SLOT
PART = 128
GROUPS = 4
F32 = jnp.float32
BF16 = jnp.bfloat16
VMEM_LIMIT = 60 * 1024 * 1024


def window_pieces():
    pieces = []
    for down in range(ACROSS):
        for over in range(ACROSS):
            for line in range(WIN):
                src_row = (down * WIN + line + SHIFT) % SIDE
                column = 0
                while column < WIN:
                    src_col = (over * WIN + column + SHIFT) % SIDE
                    length = min(WIN - column, SIDE - src_col)
                    slot = (down * ACROSS + over) * SLOT + line * WIN + column
                    pieces.append((slot, src_row * SIDE + src_col, length))
                    column += length
    return pieces


PIECES = window_pieces()


def dot_nn(a, b):
    return lax.dot_general(a, b, (((1,), (0,)), ((), ())), preferred_element_type=F32)


def dot_nt(a, b):
    return lax.dot_general(a, b, (((1,), (1,)), ((), ())), preferred_element_type=F32)


def dot_tn(a, b):
    return lax.dot_general(a, b, (((0,), (0,)), ((), ())), preferred_element_type=F32)


def row_mean(values):
    return jnp.mean(values, axis=-1, keepdims=True)


def whiten(values):
    center = values - row_mean(values)
    inverse = lax.rsqrt(row_mean(center * center) + NORM_EPSILON)
    return center * inverse, inverse


def into_slots(src_ref, dst_ref):
    for image in range(STEP_IMAGES):
        for slot, raster, length in PIECES:
            dst_ref[image * WINDOWS * SLOT + slot : image * WINDOWS * SLOT + slot + length, :] = src_ref[
                image * AREA + raster : image * AREA + raster + length, :
            ]


def out_of_slots(src_ref, dst_ref):
    for image in range(STEP_IMAGES):
        for slot, raster, length in PIECES:
            dst_ref[image * AREA + raster : image * AREA + raster + length, :] = src_ref[
                image * WINDOWS * SLOT + slot : image * WINDOWS * SLOT + slot + length, :
            ]


def head_mask(order):
    rows = lax.broadcasted_iota(jnp.int32, (SLOT, OCT_W), 1) // HEAD
    return jnp.concatenate([(rows == head).astype(F32) for head in order], axis=0).astype(BF16)


def spread(values, mask_ref):
    return jnp.concatenate([values] * OCT, axis=0) * mask_ref[...]


def lane_iota(rows):
    return lax.broadcasted_iota(jnp.int32, (rows, LANES), 1)


def build_bias(region_ref, index_ref, table_ref, bias_ref, idx_scr, tab_scr):
    idx_scr[...] = jnp.zeros_like(idx_scr)
    idx_scr[0:SPOTS, 0:SPOTS] = index_ref[...].astype(F32)
    heads, rows = table_ref.shape
    tab_scr[...] = jnp.zeros_like(tab_scr)
    tab_scr[:, 0:rows] = table_ref[...]
    by_head = tab_scr[...]
    index = idx_scr[...].T[0:SLOT, :]
    lanes = lane_iota(SLOT)
    index = jnp.where(lanes < SLOT, index, pltpu.roll(index, SLOT, 1)).astype(jnp.int32)
    sublanes = lax.broadcasted_iota(jnp.int32, (SLOT, LANES), 0)
    spot = lanes % SLOT
    masks = []
    for down in range(ACROSS):
        for over in range(ACROSS):
            row_ids = jnp.full((SLOT, LANES), -1, jnp.int32)
            col_ids = jnp.full((SLOT, LANES), -1, jnp.int32)
            for at in range(SPOTS):
                value = region_ref[down * WIN + at // WIN, over * WIN + at % WIN]
                row_ids = jnp.where(sublanes == at, value, row_ids)
                col_ids = jnp.where(spot == at, value, col_ids)
            masks.append(
                jnp.where(sublanes < SPOTS, jnp.where(row_ids == col_ids, 0.0, MASK_VALUE), PAD_SCORE)
            )
    low = index < LANES
    index_low = jnp.where(low, index, 0)
    index_high = jnp.where(low, 0, index - LANES)

    def gathered(head):
        first = jnp.broadcast_to(by_head[head : head + 1, 0:LANES], (SLOT, LANES))
        second = jnp.broadcast_to(by_head[head : head + 1, LANES : 2 * LANES], (SLOT, LANES))
        return jnp.where(
            low,
            jnp.take_along_axis(first, index_low, axis=1),
            jnp.take_along_axis(second, index_high, axis=1),
        )

    for octet in range(OCTS):
        for pair in range(OCT // 2):
            head = octet * OCT + 2 * pair
            tile = jnp.where(lanes < SLOT, gathered(head), gathered(head + 1))
            for window in range(WINDOWS):
                bias_ref[window, octet, :, pair * LANES : (pair + 1) * LANES] = tile + masks[window]


TURNED = (0, 2, 1, 3, 4, 6, 5, 7)


def turned(values):
    tiles = []
    for at in range(0, OCT_S, 2 * LANES):
        both = jnp.concatenate([values[:, at : at + LANES], values[:, at + LANES : at + 2 * LANES]], axis=0).T
        tiles += [both[0:SLOT, :], both[SLOT:, :]]
    return jnp.concatenate(tiles, axis=1)


def attention_forward_kernel(
    x_ref,
    wqkv_ref,
    wproj_ref,
    gain_ref,
    shift_ref,
    qkvb_ref,
    table_ref,
    index_ref,
    region_ref,
    y_ref,
    xs_ref,
    qkv_ref,
    p_ref,
    o_ref,
    bias_scr,
    idx_scr,
    tab_scr,
    mask_scr,
    turn_scr,
    y_scr,
):
    @pl.when(pl.program_id(0) == 0)
    def _():
        build_bias(region_ref, index_ref, table_ref, bias_scr, idx_scr, tab_scr)
        mask_scr[...] = head_mask(range(OCT))
        turn_scr[...] = head_mask(TURNED)

    xs_ref[...] = jnp.zeros_like(xs_ref)
    into_slots(x_ref, xs_ref)
    white, _ = whiten(xs_ref[...])
    a1 = (white * gain_ref[0:1, :] + shift_ref[0:1, :]).astype(BF16)
    scale = HEAD ** (-0.5)
    for half in range(2):
        columns = 3 * PART * GROUPS // 2
        u = dot_nt(a1, wqkv_ref[half * columns : (half + 1) * columns, :])
        for inner in range(GROUPS // 2):
            group = half * (GROUPS // 2) + inner
            for part in range(3):
                piece = u[:, (inner * 3 + part) * PART : (inner * 3 + part + 1) * PART]
                if part == 0:
                    piece = (piece + qkvb_ref[0:1, group * PART : (group + 1) * PART]) * scale
                elif part == 2:
                    piece = piece + qkvb_ref[1:2, group * PART : (group + 1) * PART]
                at = part * D + group * PART
                qkv_ref[:, at : at + PART] = piece.astype(BF16)

    real_query = (lax.broadcasted_iota(jnp.int32, (1, OCT_S), 1) % SLOT < SPOTS).astype(F32)

    def one_window(at, carry):
        rows = pl.ds(pl.multiple_of(at * SLOT, SLOT), SLOT)
        for octet in range(OCTS):
            q = qkv_ref[rows, octet * OCT_W : (octet + 1) * OCT_W]
            k = qkv_ref[rows, D + octet * OCT_W : D + (octet + 1) * OCT_W]
            v = qkv_ref[rows, 2 * D + octet * OCT_W : 2 * D + (octet + 1) * OCT_W]
            scores = dot_nt(k, spread(q, mask_scr)) + bias_scr[lax.rem(at, WINDOWS), octet]
            grown = jnp.exp(scores - jnp.max(scores, axis=0, keepdims=True))
            probs = grown * (real_query / jnp.sum(grown, axis=0, keepdims=True))
            p_ref[rows, octet * OCT_S : (octet + 1) * OCT_S] = probs.astype(BF16)
            o_ref[rows, octet * OCT_W : (octet + 1) * OCT_W] = dot_nn(
                turned(probs).astype(BF16), spread(v, turn_scr)
            ).astype(BF16)
        return carry

    lax.fori_loop(0, STEP_IMAGES * WINDOWS, one_window, 0)
    y_scr[...] = xs_ref[...] + dot_nn(o_ref[...], wproj_ref[...]) + shift_ref[2:3, :]
    out_of_slots(y_scr, y_ref)


def mlp_kernel(
    y_ref,
    e_ref,
    w1_ref,
    w2_ref,
    gain_ref,
    shift_ref,
    hb_ref,
    out_ref,
    dy_ref,
    g1_ref,
    g2_ref,
    hsum_ref,
    sums_ref,
    acc1,
    acc2,
    m_scr,
    da_scr,
    a2_scr,
    e_scr,
):
    step = pl.program_id(0)

    @pl.when(step == 0)
    def _():
        acc1[...] = jnp.zeros_like(acc1)
        acc2[...] = jnp.zeros_like(acc2)
        hsum_ref[...] = jnp.zeros_like(hsum_ref)
        sums_ref[...] = jnp.zeros_like(sums_ref)

    white, inverse = whiten(y_ref[...])
    a2_scr[...] = (white * gain_ref[1:2, :] + shift_ref[1:2, :]).astype(BF16)
    e_scr[...] = e_ref[...].astype(BF16)
    m_scr[...] = jnp.zeros_like(m_scr)
    da_scr[...] = jnp.zeros_like(da_scr)
    root = math.sqrt(2.0 / math.pi)
    width = 512

    def chunk(c, carry):
        at = pl.ds(pl.multiple_of(c * width, width), width)
        w1, w2 = w1_ref[at, :], w2_ref[at, :]
        a2, e = a2_scr[...], e_scr[...]
        z = dot_nt(a2, w1) + hb_ref[0:1, at]
        square = z * z
        t = jnp.tanh(z * (root + (root * 0.044715) * square))
        half = 0.5 * z
        f = (half + half * t).astype(BF16)
        slope = 0.5 + 0.5 * t + half * (1.0 - t * t) * (root + (3.0 * root * 0.044715) * square)
        dz = dot_nt(e, w2) * slope
        hsum_ref[0:1, at] += jnp.sum(dz, axis=0, keepdims=True)
        dz = dz.astype(BF16)
        m_scr[...] += dot_nn(f, w2)
        da_scr[...] += dot_nn(dz, w1)
        acc2[at, :] += dot_tn(f, e)
        acc1[at, :] += dot_tn(dz, a2)
        return carry

    lax.fori_loop(0, w1_ref.shape[0] // width, chunk, 0)
    white, inverse = whiten(y_ref[...])
    out_ref[...] = y_ref[...] + m_scr[...] + shift_ref[3:4, :]
    da = da_scr[...]
    t2 = da * gain_ref[1:2, :]
    dy = e_ref[...] + inverse * (t2 - row_mean(t2) - white * row_mean(t2 * white))
    dy_ref[...] = dy
    sums_ref[0:1, :] += jnp.sum(da * white, axis=0, keepdims=True)
    sums_ref[1:2, :] += jnp.sum(da, axis=0, keepdims=True)
    sums_ref[2:3, :] += jnp.sum(dy, axis=0, keepdims=True)
    sums_ref[3:4, :] += jnp.sum(e_ref[...], axis=0, keepdims=True)

    @pl.when(step == pl.num_programs(0) - 1)
    def _():
        g1_ref[...] = acc1[...].astype(BF16)
        g2_ref[...] = acc2[...].astype(BF16)


def attention_backward_kernel(
    dy_ref,
    xs_ref,
    qkv_ref,
    p_ref,
    o_ref,
    wqkv_ref,
    wproj_ref,
    gain_ref,
    shift_ref,
    gin_ref,
    gqkv_ref,
    gproj_ref,
    dbias_ref,
    hsum_ref,
    sums_ref,
    accq,
    accp,
    dy_scr,
    do_scr,
    du_scr,
    mask_scr,
    turn_scr,
    g_scr,
):
    step = pl.program_id(0)

    @pl.when(step == 0)
    def _():
        mask_scr[...] = head_mask(range(OCT))
        turn_scr[...] = head_mask(TURNED)
        accq[...] = jnp.zeros_like(accq)
        accp[...] = jnp.zeros_like(accp)
        dbias_ref[...] = jnp.zeros_like(dbias_ref)
        hsum_ref[...] = jnp.zeros_like(hsum_ref)
        sums_ref[...] = jnp.zeros_like(sums_ref)
        dy_scr[...] = jnp.zeros_like(dy_scr)

    into_slots(dy_ref, dy_scr)
    dr = dy_scr[...].astype(BF16)
    do_scr[...] = dot_nt(dr, wproj_ref[...]).astype(BF16)
    accp[...] += dot_tn(o_ref[...], dr)
    scale = HEAD ** (-0.5)

    def one_window(at, carry):
        rows = pl.ds(pl.multiple_of(at * SLOT, SLOT), SLOT)
        for octet in range(OCTS):
            q = qkv_ref[rows, octet * OCT_W : (octet + 1) * OCT_W]
            k = qkv_ref[rows, D + octet * OCT_W : D + (octet + 1) * OCT_W]
            v = qkv_ref[rows, 2 * D + octet * OCT_W : 2 * D + (octet + 1) * OCT_W]
            do = do_scr[rows, octet * OCT_W : (octet + 1) * OCT_W]
            probs = p_ref[rows, octet * OCT_S : (octet + 1) * OCT_S]
            wide_do = spread(do, mask_scr)
            weighted = probs.astype(F32) * dot_nt(v, wide_do)
            ds = weighted - probs.astype(F32) * jnp.sum(weighted, axis=0, keepdims=True)
            dbias_ref[octet] += ds
            dq = dot_nn(turned(ds).astype(BF16), spread(k, turn_scr)) * scale
            dk = dot_nn(ds.astype(BF16), spread(q, mask_scr))
            dv = dot_nn(probs, wide_do)
            lanes = slice(octet * OCT_W, (octet + 1) * OCT_W)
            hsum_ref[0:1, lanes] += jnp.sum(dq, axis=0, keepdims=True)
            hsum_ref[1:2, lanes] += jnp.sum(dv, axis=0, keepdims=True)
            for part, grad in enumerate((dq, dk, dv)):
                for inner in range(OCT_W // PART):
                    group = octet * (OCT_W // PART) + inner
                    at_col = (group * 3 + part) * PART
                    du_scr[rows, at_col : at_col + PART] = grad[
                        :, inner * PART : (inner + 1) * PART
                    ].astype(BF16)
        return carry

    lax.fori_loop(0, STEP_IMAGES * WINDOWS, one_window, 0)
    white, inverse = whiten(xs_ref[...])
    a1 = (white * gain_ref[0:1, :] + shift_ref[0:1, :]).astype(BF16)
    accq[...] += dot_tn(du_scr[...], a1)
    da = dot_nn(du_scr[...], wqkv_ref[...])
    t1 = da * gain_ref[0:1, :]
    g_scr[...] = dy_scr[...] + inverse * (t1 - row_mean(t1) - white * row_mean(t1 * white))
    out_of_slots(g_scr, gin_ref)
    sums_ref[0:1, :] += jnp.sum(da * white, axis=0, keepdims=True)
    sums_ref[1:2, :] += jnp.sum(da, axis=0, keepdims=True)

    @pl.when(step == pl.num_programs(0) - 1)
    def _():
        gqkv_ref[...] = accq[...].astype(BF16)
        gproj_ref[...] = accp[...].astype(BF16)


def whole(shape):
    return pl.BlockSpec(shape, lambda i: (0,) * len(shape))


def rows_of(rows, columns):
    return pl.BlockSpec((rows, columns), lambda i: (i, 0))


def shape_of(shape, dtype):
    return jax.ShapeDtypeStruct(shape, dtype)


PARAMS = pltpu.CompilerParams(dimension_semantics=("arbitrary",), vmem_limit_bytes=VMEM_LIMIT)


def attention_forward(tokens, wqkv, wproj, gains, shifts, head_biases, table, index, regions):
    steps = tokens.shape[0] // STEP_ROWS
    slots = steps * STEP_SLOTS
    return pl.pallas_call(
        attention_forward_kernel,
        grid=(steps,),
        out_shape=(
            shape_of(tokens.shape, F32),
            shape_of((slots, D), F32),
            shape_of((slots, 3 * D), BF16),
            shape_of((slots, OCTS * OCT_S), BF16),
            shape_of((slots, D), BF16),
        ),
        in_specs=[
            rows_of(STEP_ROWS, D),
            whole(wqkv.shape),
            whole(wproj.shape),
            whole(gains.shape),
            whole(shifts.shape),
            whole(head_biases.shape),
            whole(table.shape),
            whole(index.shape),
            pl.BlockSpec(memory_space=pltpu.SMEM),
        ],
        out_specs=(
            rows_of(STEP_ROWS, D),
            rows_of(STEP_SLOTS, D),
            rows_of(STEP_SLOTS, 3 * D),
            rows_of(STEP_SLOTS, OCTS * OCT_S),
            rows_of(STEP_SLOTS, D),
        ),
        scratch_shapes=[
            pltpu.VMEM((WINDOWS, OCTS, SLOT, OCT_S), F32),
            pltpu.VMEM((LANES, LANES), F32),
            pltpu.VMEM((HEADS, 2 * LANES), F32),
            pltpu.VMEM((OCT_S, OCT_W), BF16),
            pltpu.VMEM((OCT_S, OCT_W), BF16),
            pltpu.VMEM((STEP_SLOTS, D), F32),
        ],
        compiler_params=PARAMS,
        name="attention_forward",
    )(tokens, wqkv, wproj, gains, shifts, head_biases, table, index, regions)


def mlp(middle, out_grad, w1, w2, gains, shifts, hidden_bias):
    steps = middle.shape[0] // STEP_ROWS
    hidden = w1.shape[0]
    return pl.pallas_call(
        mlp_kernel,
        grid=(steps,),
        out_shape=(
            shape_of(middle.shape, F32),
            shape_of(middle.shape, F32),
            shape_of(w1.shape, BF16),
            shape_of(w2.shape, BF16),
            shape_of((1, hidden), F32),
            shape_of((4, D), F32),
        ),
        in_specs=[
            rows_of(STEP_ROWS, D),
            rows_of(STEP_ROWS, D),
            whole(w1.shape),
            whole(w2.shape),
            whole(gains.shape),
            whole(shifts.shape),
            whole((1, hidden)),
        ],
        out_specs=(
            rows_of(STEP_ROWS, D),
            rows_of(STEP_ROWS, D),
            whole(w1.shape),
            whole(w2.shape),
            whole((1, hidden)),
            whole((4, D)),
        ),
        scratch_shapes=[
            pltpu.VMEM(w1.shape, F32),
            pltpu.VMEM(w2.shape, F32),
            pltpu.VMEM((STEP_ROWS, D), F32),
            pltpu.VMEM((STEP_ROWS, D), F32),
            pltpu.VMEM((STEP_ROWS, D), BF16),
            pltpu.VMEM((STEP_ROWS, D), BF16),
        ],
        compiler_params=PARAMS,
        name="mlp",
    )(middle, out_grad, w1, w2, gains, shifts, hidden_bias.reshape(1, hidden))


def attention_backward(dy, xs, qkv, probs, mixed, wqkv, wproj, gains, shifts):
    steps = dy.shape[0] // STEP_ROWS
    return pl.pallas_call(
        attention_backward_kernel,
        grid=(steps,),
        out_shape=(
            shape_of(dy.shape, F32),
            shape_of(wqkv.shape, BF16),
            shape_of(wproj.shape, BF16),
            shape_of((OCTS, SLOT, OCT_S), F32),
            shape_of((2, D), F32),
            shape_of((2, D), F32),
        ),
        in_specs=[
            rows_of(STEP_ROWS, D),
            rows_of(STEP_SLOTS, D),
            rows_of(STEP_SLOTS, 3 * D),
            rows_of(STEP_SLOTS, OCTS * OCT_S),
            rows_of(STEP_SLOTS, D),
            whole(wqkv.shape),
            whole(wproj.shape),
            whole(gains.shape),
            whole(shifts.shape),
        ],
        out_specs=(
            rows_of(STEP_ROWS, D),
            whole(wqkv.shape),
            whole(wproj.shape),
            whole((OCTS, SLOT, OCT_S)),
            whole((2, D)),
            whole((2, D)),
        ),
        scratch_shapes=[
            pltpu.VMEM(wqkv.shape, F32),
            pltpu.VMEM(wproj.shape, F32),
            pltpu.VMEM((STEP_SLOTS, D), F32),
            pltpu.VMEM((STEP_SLOTS, D), BF16),
            pltpu.VMEM((STEP_SLOTS, 3 * D), BF16),
            pltpu.VMEM((OCT_S, OCT_W), BF16),
            pltpu.VMEM((OCT_S, OCT_W), BF16),
            pltpu.VMEM((STEP_SLOTS, D), F32),
        ],
        compiler_params=PARAMS,
        name="attention_backward",
    )(dy, xs, qkv, probs, mixed, wqkv, wproj, gains, shifts)


MESH = pl.DeviceIdType.MESH


def flipped(bit, by):
    return bit + by - 2 * bit * by


class Place:
    def __init__(self, ndp, nt):
        self.ndp, self.nt = ndp, nt
        self.nz, self.nx = ndp // 2, nt // 2
        self.dp, self.t = lax.axis_index("dp"), lax.axis_index("tensor")
        self.z, self.y = self.dp // 2, self.dp % 2
        self.x, self.c = self.t // 2, self.t % 2

    def up(self, k):
        return lax.rem(self.z + k, self.nz)

    def down(self, k):
        return lax.rem(self.z + self.nz - k, self.nz)

    def device(self, z=None, y=None, x=None, c=None):
        z, y = self.z if z is None else z, self.y if y is None else y
        x, c = self.x if x is None else x, self.c if c is None else c
        return {"dp": z * 2 + y, "tensor": x * 2 + c}

    def block(self, z, y, x, c):
        return (x * 2 + c) * self.ndp + z * 2 + y

    def across(self, c, a, b):
        return flipped(self.y, c * a + (1 - c) * b), flipped(self.x, (1 - c) * a + c * b)

    def bit_partner(self, b):
        size = 2**b
        return self.z + size * (1 - 2 * lax.rem(self.z // size, 2))

    def greet(self):
        others = [self.device(c=1 - self.c), self.device(x=1 - self.x)]
        others += [self.device(x=1 - self.x, c=1 - self.c), self.device(y=1 - self.y)]
        others += [self.device(z=self.up(k)) for k in range(1, self.nz)]
        barrier = pltpu.get_barrier_semaphore()
        for other in others:
            pl.semaphore_signal(barrier, inc=1, device_id=other, device_id_type=MESH)
        pl.semaphore_wait(barrier, len(others))


class Sender:
    def __init__(self, send_sem, recv_sem):
        self.send_sem, self.recv_sem = send_sem, recv_sem
        self.used, self.copies = 0, {}

    def start(self, key, src, dst, device):
        at = self.used
        self.used += 1
        copy = pltpu.make_async_remote_copy(
            src_ref=src,
            dst_ref=dst,
            send_sem=self.send_sem.at[at],
            recv_sem=self.recv_sem.at[at],
            device_id=device,
            device_id_type=MESH,
        )
        copy.start()
        self.copies[key] = copy

    def arrived(self, key):
        self.copies[key].wait_recv()

    def finish(self):
        for copy in self.copies.values():
            copy.wait_send()


def gather_kernel(ndp, nt, count, *refs):
    slabs, outs = refs[:count], refs[count : 2 * count]
    lows = refs[2 * count : 3 * count]
    send_sem, recv_sem, local_sem = refs[3 * count :]
    place = Place(ndp, nt)
    nz, c = place.nz, place.c
    for slab, low in zip(slabs, lows):
        low[...] = slab[...].astype(BF16)
    place.greet()
    sender = Sender(send_sem, recv_sem)
    here = place.block(place.z, place.y, place.x, c)
    own = []
    for m in range(count):
        own.append(pltpu.make_async_copy(lows[m], outs[m].at[here], local_sem.at[m]))
        own[m].start()

    def origin(a, b, k):
        y, x = place.across(1 - c, a, b)
        return place.block(place.down(k), y, x, c)

    def send(stage, a, b, k, device):
        for m in range(count):
            at = origin(a, b, k)
            src = lows[m] if (a, b, k) == (0, 0, 0) else outs[m].at[at]
            sender.start((stage, m, a, b, k), src, outs[m].at[at], device)

    def wait(stage, a, b, k):
        for m in range(count):
            sender.arrived((stage, m, a, b, k))

    y, x = place.across(1 - c, 1, 0)
    first = place.device(y=y, x=x)
    y, x = place.across(1 - c, 0, 1)
    second = place.device(y=y, x=x)
    core = place.device(c=1 - c)

    def spread_column(k):
        send("p", 0, 0, k, first)
        send("q", 0, 0, k, second)
        send("c", 0, 0, k, core)

    def spread_first(k):
        wait("p", 0, 0, k)
        send("q", 1, 0, k, second)
        send("c", 1, 0, k, core)

    for k in range(1, nz):
        for m in range(count):
            sender.start(("z", m, k), lows[m], outs[m].at[here], place.device(z=place.up(k)))
    spread_column(0)
    for k in range(1, nz):
        for m in range(count):
            sender.arrived(("z", m, k))
        spread_column(k)
        spread_first(k - 1)
    spread_first(nz - 1)
    for a in range(2):
        for k in range(nz):
            wait("q", a, 0, k)
            send("c", a, 1, k, core)
    for b in range(2):
        for a in range(2):
            for k in range(nz):
                wait("c", a, b, k)
    for copy in own:
        copy.wait()
    sender.finish()


def gather_weights(slabs, ndp, nt, collective_id):
    count, n = len(slabs), ndp * nt
    messages = count * (n - 1)
    gathered = pl.pallas_call(
        functools.partial(gather_kernel, ndp, nt, count),
        out_shape=tuple(shape_of((n,) + s.shape, BF16) for s in slabs),
        in_specs=[pl.BlockSpec(memory_space=pltpu.VMEM)] * count,
        out_specs=tuple(pl.BlockSpec(memory_space=pl.ANY) for _ in slabs),
        scratch_shapes=[pltpu.VMEM(s.shape, BF16) for s in slabs]
        + [
            pltpu.SemaphoreType.DMA((messages,)),
            pltpu.SemaphoreType.DMA((messages,)),
            pltpu.SemaphoreType.DMA((count,)),
        ],
        compiler_params=pltpu.CompilerParams(
            collective_id=collective_id, has_side_effects=True, vmem_limit_bytes=VMEM_LIMIT
        ),
        name="gather_weights",
    )(*slabs)
    return tuple(g.reshape(n * s.shape[0], D) for g, s in zip(gathered, slabs))


SMALL_ROWS = 32
TABLE_ROW = 16


def update_kernel(ndp, nt, images, tall, *refs):
    refs = list(refs)

    def take(n):
        taken = refs[:n]
        del refs[:n]
        return taken

    count = nt
    grads, momenta = take(count), take(count)
    sums1, sums2, head, hidden, table = take(5)
    grad_out = take(count)
    bundle, small_out = take(2)
    own, from_core, from_p, from_q, from_z = (take(count) for _ in range(5))
    (fresh, small, small_in) = take(3)
    send_sem, recv_sem, local_sem, near_sem = take(4)
    place = Place(ndp, nt)
    nz, c = place.nz, place.c
    small[0] = jnp.zeros_like(small[0])
    small[0, 0:1, :] = sums1[0:1, :]
    small[0, 1:2, :] = sums2[0:1, :]
    small[0, 2:3, :] = sums1[1:2, :]
    small[0, 3:6, :] = sums2[1:4, :]
    small[0, 6:8, :] = head[...]
    spans = hidden.shape[1] // D
    for i in range(spans):
        small[0, 8 + i : 9 + i, :] = hidden[0:1, i * D : (i + 1) * D]
    small[0, TABLE_ROW : TABLE_ROW + table.shape[0], 0 : table.shape[1]] = table[...]
    fresh[...] = jnp.zeros_like(fresh)
    place.greet()
    sender = Sender(send_sem, recv_sem)
    steps = [place.device(c=1 - c), place.device(x=1 - place.x), place.device(y=1 - place.y)]
    bit = 0
    while 2**bit < nz:
        steps.append(place.device(z=place.bit_partner(bit)))
        bit += 1

    def small_send(i):
        sender.start(("s", i), small.at[i], small_in.at[i], steps[i])

    def small_add(i):
        sender.arrived(("s", i))
        small[i + 1] = small[i] + small_in[i]

    order = [(a, b, k) for a in (1, 0) for b in (1, 0) for k in list(range(1, nz)) + [0]]
    locals_ = {}
    for a, b, k in order:
        y, x = place.across(1 - c, a, b)
        at = place.block(place.up(k), y, x, 1 - c)
        for m in range(count):
            sender.start(("c", m, a, b, k), grads[m].at[at], from_core[m].at[a, b, k], place.device(c=1 - c))
    small_send(0)
    for number, (a, b, k) in enumerate(order):
        y, x = place.across(c, a, b)
        at = place.block(place.up(k), y, x, c)
        for m in range(count):
            copy = pltpu.make_async_copy(
                grads[m].at[at], own[m].at[a, b, k], local_sem.at[number * count + m]
            )
            copy.start()
            locals_[m, a, b, k] = copy
    y, x = place.across(c, 1, 0)
    first = place.device(y=y, x=x)
    y, x = place.across(c, 0, 1)
    second = place.device(y=y, x=x)
    waiting = []

    def flush():
        for key, src, dst, device in waiting:
            sender.start(key, src, dst, device)
        waiting.clear()

    small_at = 0
    totals = [None] * count
    for number, (a, b, k) in enumerate(order):
        ready = []
        for m in range(count):
            locals_[m, a, b, k].wait()
            sender.arrived(("c", m, a, b, k))
            value = own[m][a, b, k].astype(F32) + from_core[m][a, b, k].astype(F32)
            if a == 0:
                sender.arrived(("p", m, b, k))
                value = value + from_p[m][b, k].astype(F32)
                if b == 0:
                    sender.arrived(("q", m, k))
                    value = value + from_q[m][k].astype(F32)
            if (a, b, k) == (0, 0, 0):
                totals[m] = value
                continue
            own[m][a, b, k] = value.astype(BF16)
            src = own[m].at[a, b, k]
            if a == 1:
                ready.append((("p", m, b, k), src, from_p[m].at[b, k], first))
            elif b == 1:
                ready.append((("q", m, k), src, from_q[m].at[k], second))
            else:
                ready.append((("z", m, k), src, from_z[m].at[k - 1], place.device(z=place.up(k))))
        flush()
        waiting.extend(ready)
        if number % 3 == 2 and small_at < len(steps):
            small_add(small_at)
            small_at += 1
            if small_at < len(steps):
                small_send(small_at)
    flush()
    while small_at < len(steps):
        small_add(small_at)
        small_at += 1
        if small_at < len(steps):
            small_send(small_at)
    for m in range(count):
        value = totals[m]
        for k in range(1, nz):
            sender.arrived(("z", m, k))
            value = value + from_z[m][k - 1].astype(F32)
        value = value / images
        grad_out[m][...] = value
        value = MOMENTUM * momenta[m][...] + value
        fresh[m, 0 : value.shape[0], :] = value.astype(BF16)
    small_out[...] = small[len(steps)] / images
    near = pltpu.make_async_copy(fresh.at[place.t], bundle.at[place.dp, place.t], near_sem)
    near.start()
    for d in range(1, nt):
        to = lax.rem(place.t + d, nt)
        sender.start(
            ("t", d), fresh.at[to], bundle.at[place.dp, place.t], {"dp": place.dp, "tensor": to}
        )
    near.wait()
    for d in range(1, nt):
        sender.arrived(("t", d))
    for k in range(1, nz):
        sender.start(("bz", k), bundle.at[place.dp], bundle.at[place.dp], place.device(z=place.up(k)))
    sideways = place.device(y=1 - place.y)
    for k in range(nz):
        if k:
            sender.arrived(("bz", k))
        at = place.down(k) * 2 + place.y
        sender.start(("by", k), bundle.at[at], bundle.at[at], sideways)
    for k in range(nz):
        sender.arrived(("by", k))
    sender.finish()


def update(grads, momenta, small_sums, ndp, nt, images, collective_id):
    n, nz = ndp * nt, ndp // 2
    slabs = [m.shape[0] for m in momenta]
    tall = max(slabs)
    grads = tuple(g.reshape(n, r, D) for g, r in zip(grads, slabs))
    small_steps = 3 + (nz - 1).bit_length()
    messages = nt * (4 * nz + 2 * nz + nz + nz - 1) + small_steps + (nt - 1) + (nz - 1) + nz
    vmem, any_ = pl.BlockSpec(memory_space=pltpu.VMEM), pl.BlockSpec(memory_space=pl.ANY)
    like = lambda arrays: tuple(shape_of(a.shape, F32) for a in arrays)
    outs = like(momenta) + (shape_of((ndp, nt, tall, D), BF16), shape_of((SMALL_ROWS, D), F32))
    scratch = []
    for lead in ((2, 2, nz), (2, 2, nz), (2, nz), (nz,), (nz - 1,)):
        scratch += [pltpu.VMEM(lead + (r, D), BF16) for r in slabs]
    scratch += [
        pltpu.VMEM((nt, tall, D), BF16),
        pltpu.VMEM((small_steps + 1, SMALL_ROWS, D), F32),
        pltpu.VMEM((small_steps, SMALL_ROWS, D), F32),
        pltpu.SemaphoreType.DMA((messages,)),
        pltpu.SemaphoreType.DMA((messages,)),
        pltpu.SemaphoreType.DMA((4 * nz * nt,)),
        pltpu.SemaphoreType.DMA,
    ]
    return pl.pallas_call(
        functools.partial(update_kernel, ndp, nt, images, tall),
        out_shape=outs,
        in_specs=[any_] * nt + [vmem] * (nt + 5),
        out_specs=(vmem,) * nt + (any_, vmem),
        scratch_shapes=scratch,
        compiler_params=pltpu.CompilerParams(
            collective_id=collective_id, has_side_effects=True, vmem_limit_bytes=VMEM_LIMIT
        ),
        name="update",
    )(*grads, *momenta, *small_sums)


def newton_schulz_kernel(g_ref, out_ref, x_scr, a_scr):
    first, second, third = QUINTIC
    chunk = 512
    rows, mine = g_ref.shape[0], out_ref.shape[0]

    def low(values):
        return values.astype(BF16)

    def gram(src_ref):
        a_scr[...] = jnp.zeros_like(a_scr)

        def add(at, carry):
            part = src_ref[pl.ds(pl.multiple_of(at * chunk, chunk), chunk), :]
            a_scr[...] += dot_tn(part, part)
            return carry

        lax.fori_loop(0, rows // chunk, add, 0)
        return a_scr[...]

    def advance(src_ref, factor, scale):
        factor = low(factor)

        def step(at, carry):
            at = pl.ds(pl.multiple_of(at * chunk, chunk), chunk)
            x_scr[at, :] = low(dot_nn(src_ref[at, :], factor) * scale)
            return carry

        lax.fori_loop(0, rows // chunk, step, 0)

    def bend(a):
        return second * a + third * dot_nn(low(a), low(a))

    diagonal = lax.broadcasted_iota(jnp.int32, (D, D), 0) == lax.broadcasted_iota(jnp.int32, (D, D), 1)

    def two_turns(a):
        b = bend(a)
        q = b + jnp.where(diagonal, first, 0.0)
        r = first * a + dot_nn(low(a), low(b))
        a = first * r + dot_nn(low(r), low(b))
        b = bend(a)
        return first * q + dot_nn(low(b), low(q))

    a = gram(g_ref)
    scale = 1.0 / (jnp.sqrt(jnp.sum(jnp.where(diagonal, a, 0.0))) + MUON_EPSILON)
    advance(g_ref, two_turns(a * scale * scale), scale)
    q = two_turns(gram(x_scr))
    at = pl.ds(pl.multiple_of(lax.axis_index("dp") * mine, mine), mine)
    here = dot_nn(x_scr[at, :], low(q))
    advance(x_scr, q, 1.0)
    b = bend(gram(x_scr))
    out_ref[...] = first * here + dot_nn(low(here), low(b))


def newton_schulz(bundle):
    ndp, nt, tall, _ = bundle.shape
    rows = ndp * nt * tall
    return pl.pallas_call(
        newton_schulz_kernel,
        out_shape=shape_of((nt * tall, D), F32),
        scratch_shapes=[pltpu.VMEM((rows, D), BF16), pltpu.VMEM((D, D), F32)],
        compiler_params=pltpu.CompilerParams(vmem_limit_bytes=VMEM_LIMIT),
        name="newton_schulz",
    )(bundle.reshape(rows, D)).reshape(nt, tall, D)


def return_kernel(ndp, nt, x_ref, landed, send_sem, recv_sem):
    dp, t = lax.axis_index("dp"), lax.axis_index("tensor")
    barrier = pltpu.get_barrier_semaphore()
    for d in range(1, nt):
        other = {"dp": dp, "tensor": lax.rem(t + d, nt)}
        pl.semaphore_signal(barrier, inc=1, device_id=other, device_id_type=MESH)
    pl.semaphore_wait(barrier, nt - 1)
    sender = Sender(send_sem, recv_sem)
    for d in range(1, nt):
        to = lax.rem(t + d, nt)
        sender.start(d, x_ref.at[to], landed.at[t], {"dp": dp, "tensor": to})
    landed[t] = x_ref[t]
    for d in range(1, nt):
        sender.arrived(d)
    sender.finish()


def return_updates(x, ndp, nt, collective_id):
    return pl.pallas_call(
        functools.partial(return_kernel, ndp, nt),
        out_shape=shape_of(x.shape, F32),
        in_specs=[pl.BlockSpec(memory_space=pltpu.VMEM)],
        out_specs=pl.BlockSpec(memory_space=pltpu.VMEM),
        scratch_shapes=[pltpu.SemaphoreType.DMA((nt - 1,)), pltpu.SemaphoreType.DMA((nt - 1,))],
        compiler_params=pltpu.CompilerParams(collective_id=collective_id, has_side_effects=True),
        name="return_updates",
    )(x)


def finish_kernel(nt, rates, *refs):
    refs = list(refs)

    def take(n):
        taken = refs[:n]
        del refs[:n]
        return taken

    landed, total = take(2)
    grads, momenta, weights = take(nt), take(nt), take(nt)
    small_par, small_mom = take(5), take(5)
    grad_out, new_out, mom_out = take(nt), take(nt), take(nt)
    small_grad_out, small_new_out, small_mom_out = take(5), take(5), take(5)
    for m in range(nt):
        grad = grads[m][...]
        grad_out[m][...] = grad
        mom_out[m][...] = MOMENTUM * momenta[m][...] + grad
        new_out[m][...] = weights[m][...] - rates[m] * landed[m, 0 : grad.shape[0], :]

    def small_update(i, at, grad):
        small_grad_out[i][at] = grad
        grad = MOMENTUM * small_mom[i][at] + grad
        small_mom_out[i][at] = grad
        small_new_out[i][at] = small_par[i][at] - VECTOR_RATE * grad

    for i, (low, high) in enumerate(((0, 2), (2, 6), (6, 8))):
        small_update(i, (slice(None), slice(None)), total[low:high, :])
    for i in range(small_par[3].shape[1] // D):
        small_update(3, (slice(0, 1), slice(i * D, (i + 1) * D)), total[8 + i : 9 + i, :])
    heads, rows = small_par[4].shape
    small_update(4, (slice(None), slice(None)), total[TABLE_ROW : TABLE_ROW + heads, 0:rows])


def finish(landed, total, grads, momenta, weights, small_params, small_moms, rates):
    nt = len(grads)
    like = lambda arrays: tuple(shape_of(a.shape, F32) for a in arrays)
    return pl.pallas_call(
        functools.partial(finish_kernel, nt, rates),
        out_shape=like(grads) * 3 + like(small_params) * 3,
        compiler_params=pltpu.CompilerParams(vmem_limit_bytes=VMEM_LIMIT),
        name="finish",
    )(landed, total, *grads, *momenta, *weights, *small_params, *small_moms)


WIDE = (True, False, True, False)
FACTORS = (
    math.sqrt(3.0),
    1.0,
    math.sqrt(max(1.0, FF / D)),
    math.sqrt(max(1.0, D / FF)),
)


def as_slab(block, wide):
    return block.reshape(D, -1).T if wide else block.reshape(-1, D)


def as_block(slab, like, wide):
    return (slab.T if wide else slab).reshape(like.shape)


def shards(
    tokens,
    out_grad,
    qkv_weight,
    proj_weight,
    fc1_weight,
    fc2_weight,
    qkv_momentum,
    proj_momentum,
    fc1_momentum,
    fc2_momentum,
    norm_gains,
    shift_biases,
    head_biases,
    hidden_bias,
    position_table,
    gain_momentum,
    shift_momentum,
    head_bias_momentum,
    hidden_bias_momentum,
    table_momentum,
    region_ids,
    position_index,
):
    devices = lax.axis_size("dp") * lax.axis_size("tensor")
    images = tokens.shape[0] // AREA * devices
    blocks = (qkv_weight, proj_weight, fc1_weight, fc2_weight)
    weights = tuple(as_slab(w, wide) for w, wide in zip(blocks, WIDE))
    momenta = tuple(
        as_slab(m, wide)
        for m, wide in zip((qkv_momentum, proj_momentum, fc1_momentum, fc2_momentum), WIDE)
    )
    ndp, nt = lax.axis_size("dp"), lax.axis_size("tensor")
    wqkv, wproj, w1, w2 = gather_weights(weights, ndp, nt, 0)
    middle, xs, qkv, probs, mixed = attention_forward(
        tokens,
        wqkv,
        wproj,
        norm_gains,
        shift_biases,
        head_biases,
        position_table.T,
        position_index,
        region_ids,
    )
    output, dy, g1, g2, hidden_sum, sums2 = mlp(
        middle, out_grad, w1, w2, norm_gains, shift_biases, hidden_bias
    )
    input_grad, gqkv, gproj, dbias, head_sum, sums1 = attention_backward(
        dy, xs, qkv, probs, mixed, wqkv, wproj, norm_gains, shift_biases
    )
    by_head = (
        dbias.reshape(OCTS, SLOT, OCT, SLOT)[:, :SPOTS, :, :SPOTS]
        .transpose(0, 2, 3, 1)
        .reshape(HEADS, SPOTS * SPOTS)
    )
    onehot = (
        position_index.reshape(-1)[:, None]
        == jnp.arange(position_table.shape[0], dtype=jnp.int32)[None, :]
    ).astype(F32)
    table_part = jnp.dot(onehot.T, by_head.T, precision=lax.Precision.HIGHEST)
    small_params = (norm_gains, shift_biases, head_biases, hidden_bias.reshape(1, -1), position_table.T)
    small_moms = (
        gain_momentum,
        shift_momentum,
        head_bias_momentum,
        hidden_bias_momentum.reshape(1, -1),
        table_momentum.T,
    )
    results = update(
        (gqkv, gproj, g1, g2),
        momenta,
        (sums1, sums2, head_sum, hidden_sum, table_part.T),
        ndp,
        nt,
        images,
        1,
    )
    slab_grads, bundle, total = results[:nt], results[nt], results[nt + 1]
    landed = return_updates(newton_schulz(bundle), ndp, nt, 2)
    rates = tuple(MATRIX_RATE * factor for factor in FACTORS)
    results = finish(landed, total, slab_grads, momenta, weights, small_params, small_moms, rates)
    slab_grads, new_weights, new_momenta = (results[i * nt : (i + 1) * nt] for i in range(3))
    smalls = tuple(
        s.reshape(-1) if i % 5 == 3 else s.T if i % 5 == 4 else s
        for i, s in enumerate(results[3 * nt :])
    )

    def placed(slabs):
        return tuple(as_block(s, like, wide) for s, like, wide in zip(slabs, blocks, WIDE))

    return (
        (output, input_grad)
        + placed(slab_grads)
        + placed(new_weights)
        + placed(new_momenta)
        + smalls
    )


def solution(mesh):
    rows = P(("dp", "tensor"), None)
    wide, tall = P(None, "tensor", "dp"), P("tensor", "dp", None)
    matrices = (wide, tall, wide, tall)
    return jax.shard_map(
        shards,
        mesh=mesh,
        in_specs=(rows, rows) + matrices * 2 + (P(),) * 12,
        out_specs=(rows, rows) + matrices * 3 + (P(),) * 15,
        check_vma=False,
    )
```

```python
import functools
import math

import jax
import jax.numpy as jnp
from jax import lax
from jax.experimental import pallas as pl
from jax.experimental.pallas import tpu as pltpu
from jax.sharding import PartitionSpec as P

D = 512
HEADS = 16
FF = 2048
HEAD = 32
WIN = 7
SIDE = 14
SHIFT = 3
NS_STEPS = 5

NORM_EPSILON = 1e-05
MASK_VALUE = -100.0
MUON_EPSILON = 1e-07
QUINTIC = (3.4445, -4.775, 2.0315)
MOMENTUM = 0.9
MATRIX_RATE = 0.5
VECTOR_RATE = 1.0

AREA = SIDE * SIDE
SPOTS = WIN * WIN
ACROSS = SIDE // WIN
WINDOWS = ACROSS * ACROSS
SLOT = 64
LANES = 128
OCT = 8
OCTS = HEADS // OCT
OCT_W = OCT * HEAD
OCT_S = OCT * SLOT
PAD_SCORE = -1e30
STEP_IMAGES = 2
STEP_ROWS = STEP_IMAGES * AREA
STEP_SLOTS = STEP_IMAGES * WINDOWS * SLOT
PART = 128
GROUPS = 4
F32 = jnp.float32
BF16 = jnp.bfloat16
VMEM_LIMIT = 60 * 1024 * 1024


def window_pieces():
    pieces = []
    for down in range(ACROSS):
        for over in range(ACROSS):
            for line in range(WIN):
                src_row = (down * WIN + line + SHIFT) % SIDE
                column = 0
                while column < WIN:
                    src_col = (over * WIN + column + SHIFT) % SIDE
                    length = min(WIN - column, SIDE - src_col)
                    slot = (down * ACROSS + over) * SLOT + line * WIN + column
                    pieces.append((slot, src_row * SIDE + src_col, length))
                    column += length
    return pieces


PIECES = window_pieces()


def dot_nn(a, b):
    return lax.dot_general(a, b, (((1,), (0,)), ((), ())), preferred_element_type=F32)


def dot_nt(a, b):
    return lax.dot_general(a, b, (((1,), (1,)), ((), ())), preferred_element_type=F32)


def dot_tn(a, b):
    return lax.dot_general(a, b, (((0,), (0,)), ((), ())), preferred_element_type=F32)


def row_mean(values):
    return jnp.mean(values, axis=-1, keepdims=True)


def whiten(values):
    center = values - row_mean(values)
    inverse = lax.rsqrt(row_mean(center * center) + NORM_EPSILON)
    return center * inverse, inverse


def into_slots(src_ref, dst_ref):
    for image in range(STEP_IMAGES):
        for slot, raster, length in PIECES:
            dst_ref[image * WINDOWS * SLOT + slot : image * WINDOWS * SLOT + slot + length, :] = src_ref[
                image * AREA + raster : image * AREA + raster + length, :
            ]


def out_of_slots(src_ref, dst_ref):
    for image in range(STEP_IMAGES):
        for slot, raster, length in PIECES:
            dst_ref[image * AREA + raster : image * AREA + raster + length, :] = src_ref[
                image * WINDOWS * SLOT + slot : image * WINDOWS * SLOT + slot + length, :
            ]


def head_mask(order):
    rows = lax.broadcasted_iota(jnp.int32, (SLOT, OCT_W), 1) // HEAD
    return jnp.concatenate([(rows == head).astype(F32) for head in order], axis=0).astype(BF16)


def spread(values, mask_ref):
    return jnp.concatenate([values] * OCT, axis=0) * mask_ref[...]


def lane_iota(rows):
    return lax.broadcasted_iota(jnp.int32, (rows, LANES), 1)


def build_bias(region_ref, index_ref, table_ref, bias_ref, idx_scr, tab_scr):
    idx_scr[...] = jnp.zeros_like(idx_scr)
    idx_scr[0:SPOTS, 0:SPOTS] = index_ref[...].astype(F32)
    heads, rows = table_ref.shape
    tab_scr[...] = jnp.zeros_like(tab_scr)
    tab_scr[:, 0:rows] = table_ref[...]
    by_head = tab_scr[...]
    index = idx_scr[...].T[0:SLOT, :]
    lanes = lane_iota(SLOT)
    index = jnp.where(lanes < SLOT, index, pltpu.roll(index, SLOT, 1)).astype(jnp.int32)
    sublanes = lax.broadcasted_iota(jnp.int32, (SLOT, LANES), 0)
    spot = lanes % SLOT
    masks = []
    for down in range(ACROSS):
        for over in range(ACROSS):
            row_ids = jnp.full((SLOT, LANES), -1, jnp.int32)
            col_ids = jnp.full((SLOT, LANES), -1, jnp.int32)
            for at in range(SPOTS):
                value = region_ref[down * WIN + at // WIN, over * WIN + at % WIN]
                row_ids = jnp.where(sublanes == at, value, row_ids)
                col_ids = jnp.where(spot == at, value, col_ids)
            masks.append(
                jnp.where(sublanes < SPOTS, jnp.where(row_ids == col_ids, 0.0, MASK_VALUE), PAD_SCORE)
            )
    low = index < LANES
    index_low = jnp.where(low, index, 0)
    index_high = jnp.where(low, 0, index - LANES)

    def gathered(head):
        first = jnp.broadcast_to(by_head[head : head + 1, 0:LANES], (SLOT, LANES))
        second = jnp.broadcast_to(by_head[head : head + 1, LANES : 2 * LANES], (SLOT, LANES))
        return jnp.where(
            low,
            jnp.take_along_axis(first, index_low, axis=1),
            jnp.take_along_axis(second, index_high, axis=1),
        )

    for octet in range(OCTS):
        for pair in range(OCT // 2):
            head = octet * OCT + 2 * pair
            tile = jnp.where(lanes < SLOT, gathered(head), gathered(head + 1))
            for window in range(WINDOWS):
                bias_ref[window, octet, :, pair * LANES : (pair + 1) * LANES] = tile + masks[window]


TURNED = (0, 2, 1, 3, 4, 6, 5, 7)


def turned(values):
    tiles = []
    for at in range(0, OCT_S, 2 * LANES):
        both = jnp.concatenate([values[:, at : at + LANES], values[:, at + LANES : at + 2 * LANES]], axis=0).T
        tiles += [both[0:SLOT, :], both[SLOT:, :]]
    return jnp.concatenate(tiles, axis=1)


MESH = pl.DeviceIdType.MESH


def flipped(bit, by):
    return bit + by - 2 * bit * by


class Place:
    def __init__(self, ndp, nt):
        self.ndp, self.nt = ndp, nt
        self.nz = ndp // 2
        self.dp, self.t = lax.axis_index("dp"), lax.axis_index("tensor")
        self.z, self.y = self.dp // 2, self.dp % 2
        self.x, self.c = self.t // 2, self.t % 2

    def up(self, k):
        return lax.rem(self.z + k, self.nz)

    def down(self, k):
        return lax.rem(self.z + self.nz - k, self.nz)

    def device(self, z=None, y=None, x=None, c=None):
        z, y = self.z if z is None else z, self.y if y is None else y
        x, c = self.x if x is None else x, self.c if c is None else c
        return {"dp": z * 2 + y, "tensor": x * 2 + c}

    def block(self, z, y, x, c):
        return (x * 2 + c) * self.ndp + z * 2 + y

    def across(self, c, a, b):
        return flipped(self.y, c * a + (1 - c) * b), flipped(self.x, (1 - c) * a + c * b)

    def chip(self, c, a, b):
        y, x = self.across(c, a, b)
        return self.device(y=y, x=x)

    def bit_partner(self, b):
        size = 2**b
        return self.z + size * (1 - 2 * lax.rem(self.z // size, 2))

    def greet(self):
        others = [self.device(c=1 - self.c), self.device(x=1 - self.x)]
        others += [self.device(x=1 - self.x, c=1 - self.c), self.device(y=1 - self.y)]
        others += [self.device(z=self.up(k)) for k in range(1, self.nz)]
        barrier = pltpu.get_barrier_semaphore()
        for other in others:
            pl.semaphore_signal(barrier, inc=1, device_id=other, device_id_type=MESH)
        pl.semaphore_wait(barrier, len(others))


def remote(src, dst, send_sem, recv_sem, device):
    return pltpu.make_async_remote_copy(
        src_ref=src,
        dst_ref=dst,
        send_sem=send_sem,
        recv_sem=recv_sem,
        device_id=device,
        device_id_type=MESH,
    )


class Gather:
    def __init__(self, place, slabs, outs, scratch):
        count = len(slabs)
        self.place, self.slabs, self.outs, self.count = place, slabs, outs, count
        self.lows = scratch[:count]
        self.send_sem, self.recv_sem, self.local_sem = scratch[count:]

    @staticmethod
    def scratch(shapes, n):
        messages = len(shapes) * (n - 1)
        return [pltpu.VMEM(s, BF16) for s in shapes] + [
            pltpu.SemaphoreType.DMA((messages,)),
            pltpu.SemaphoreType.DMA((messages,)),
            pltpu.SemaphoreType.DMA((len(shapes),)),
        ]

    def copy(self, stage, m, a, b, k):
        place, nz = self.place, self.place.nz
        order = 1 - place.c
        base = {"z": -1, "p": nz - 1, "q": 2 * nz - 1, "c": 4 * nz - 1}[stage]
        at = m * (8 * nz - 1) + base + (b * 2 + a) * nz + k
        y, x = place.across(order, a, b)
        where = place.block(place.down(k), y, x, place.c)
        device = {
            "p": lambda: place.chip(order, 1, 0),
            "q": lambda: place.chip(order, 0, 1),
            "c": lambda: place.device(c=1 - place.c),
            "z": lambda: place.device(z=place.up(k)),
        }[stage]()
        if stage == "z":
            where = place.block(place.z, place.y, place.x, place.c)
        mine = stage == "z" or (a, b, k) == (0, 0, 0)
        src = self.lows[m] if mine else self.outs[m].at[where]
        return remote(src, self.outs[m].at[where], self.send_sem.at[at], self.recv_sem.at[at], device)

    def local(self, m):
        place = self.place
        where = place.block(place.z, place.y, place.x, place.c)
        return pltpu.make_async_copy(self.lows[m], self.outs[m].at[where], self.local_sem.at[m])

    def send(self, stage, a, b, k):
        for m in range(self.count):
            self.copy(stage, m, a, b, k).start()

    def wait(self, stage, a, b, k):
        for m in range(self.count):
            self.copy(stage, m, a, b, k).wait_recv()

    def column(self, k):
        if k:
            self.wait("z", 0, 0, k)
        self.send("p", 0, 0, k)
        self.send("q", 0, 0, k)
        self.send("c", 0, 0, k)

    def first(self, k):
        self.wait("p", 0, 0, k)
        self.send("q", 1, 0, k)
        self.send("c", 1, 0, k)

    def second(self, a, k):
        self.wait("q", a, 0, k)
        self.send("c", a, 1, k)

    def round(self):
        return range(self.place.nz)

    def begin(self):
        for slab, low in zip(self.slabs, self.lows):
            low[...] = slab[...].astype(BF16)
        self.place.greet()
        for m in range(self.count):
            self.local(m).start()
        for k in self.round()[1:]:
            self.send("z", 0, 0, k)
        self.column(0)

    def end(self):
        everything = [("z", 0, 0, k) for k in self.round()[1:]]
        everything += [("p", 0, 0, k) for k in self.round()]
        everything += [("q", a, 0, k) for a in range(2) for k in self.round()]
        last = [("c", a, b, k) for b in range(2) for a in range(2) for k in self.round()]
        for key in last:
            self.wait(*key)
        for m in range(self.count):
            self.local(m).wait()
            for stage, a, b, k in everything + last:
                self.copy(stage, m, a, b, k).wait_send()

    def at_once(self):
        self.begin()
        for k in self.round()[1:]:
            self.column(k)
            self.first(k - 1)
        self.first(self.place.nz - 1)
        for a in range(2):
            for k in self.round():
                self.second(a, k)
        self.end()


class Reduce:
    def __init__(self, place, grads, scratch):
        count = len(grads)
        self.place, self.grads, self.count = place, grads, count
        self.own, self.from_core, self.from_p, self.from_q, self.from_z = (
            scratch[i * count : (i + 1) * count] for i in range(5)
        )
        self.send_sem, self.recv_sem, self.local_sem = scratch[5 * count :]

    @staticmethod
    def scratch(rows, n):
        nz, count = n // 8, len(rows)
        shapes = []
        for lead in ((2, 2, nz), (2, 2, nz), (2, nz), (nz,), (nz - 1,)):
            shapes += [pltpu.VMEM(lead + (r, D), BF16) for r in rows]
        return shapes + [
            pltpu.SemaphoreType.DMA((count * (8 * nz - 1),)),
            pltpu.SemaphoreType.DMA((count * (8 * nz - 1),)),
            pltpu.SemaphoreType.DMA((count * 4 * nz,)),
        ]

    def ks(self):
        return list(range(1, self.place.nz)) + [0]

    def copy(self, stage, m, a, b, k):
        place, nz = self.place, self.place.nz
        base = {"c": 0, "p": 4 * nz, "q": 6 * nz, "z": 7 * nz - 1}[stage]
        at = m * (8 * nz - 1) + base + {"c": (a * 2 + b) * nz + k, "p": b * nz + k}.get(stage, k)
        sems = self.send_sem.at[at], self.recv_sem.at[at]
        if stage == "c":
            y, x = place.across(1 - place.c, a, b)
            where = place.block(place.up(k), y, x, 1 - place.c)
            return remote(
                self.grads[m].at[where], self.from_core[m].at[a, b, k], *sems, place.device(c=1 - place.c)
            )
        src = self.own[m].at[a, b, k]
        if stage == "p":
            return remote(src, self.from_p[m].at[b, k], *sems, place.chip(place.c, 1, 0))
        if stage == "q":
            return remote(src, self.from_q[m].at[k], *sems, place.chip(place.c, 0, 1))
        return remote(src, self.from_z[m].at[k - 1], *sems, place.device(z=place.up(k)))

    def local(self, m, a, b, k):
        place, nz = self.place, self.place.nz
        y, x = place.across(place.c, a, b)
        where = place.block(place.up(k), y, x, place.c)
        at = m * 4 * nz + (a * 2 + b) * nz + k
        return pltpu.make_async_copy(
            self.grads[m].at[where], self.own[m].at[a, b, k], self.local_sem.at[at]
        )

    def order(self):
        return [(a, b, k) for a in (1, 0) for b in (1, 0) for k in self.ks()]

    def begin(self):
        for a, b, k in self.order():
            for m in range(self.count):
                self.copy("c", m, a, b, k).start()
        for a, b, k in self.order():
            for m in range(self.count):
                self.local(m, a, b, k).start()

    def value(self, m, a, b, k):
        self.local(m, a, b, k).wait()
        self.copy("c", m, a, b, k).wait_recv()
        value = self.own[m][a, b, k].astype(F32) + self.from_core[m][a, b, k].astype(F32)
        if a == 0:
            self.copy("p", m, 1, b, k).wait_recv()
            value = value + self.from_p[m][b, k].astype(F32)
            if b == 0:
                self.copy("q", m, 0, 1, k).wait_recv()
                value = value + self.from_q[m][k].astype(F32)
        return value

    def pass_on(self, a, b, between=None):
        stage = "p" if a else "q" if b else "z"
        waiting = []
        for k in self.ks():
            if stage == "z" and k == 0:
                continue
            for m in range(self.count):
                self.own[m][a, b, k] = self.value(m, a, b, k).astype(BF16)
            for copy in waiting:
                copy.start()
            waiting = [self.copy(stage, m, a, b, k) for m in range(self.count)]
        if between is not None:
            between()
        for copy in waiting:
            copy.start()

    def totals(self):
        values = [self.value(m, 0, 0, 0) for m in range(self.count)]
        for m in range(self.count):
            for k in self.ks()[:-1]:
                self.copy("z", m, 0, 0, k).wait_recv()
                values[m] = values[m] + self.from_z[m][k - 1].astype(F32)
        return values

    def end(self):
        for m in range(self.count):
            for a, b, k in self.order():
                self.copy("c", m, a, b, k).wait_send()
                if a:
                    self.copy("p", m, a, b, k).wait_send()
                elif b:
                    self.copy("q", m, a, b, k).wait_send()
                elif k:
                    self.copy("z", m, a, b, k).wait_send()


class Share:
    def __init__(self, place, core, fresh, bundle, scratch):
        self.place, self.core, self.fresh, self.bundle = place, core, fresh, bundle
        self.send_sem, self.recv_sem, self.near_sem = scratch

    @staticmethod
    def scratch(n, nt):
        messages = 2 + (nt - 1) + (n // 8 - 1) + n // 8
        return [
            pltpu.SemaphoreType.DMA((messages,)),
            pltpu.SemaphoreType.DMA((messages,)),
            pltpu.SemaphoreType.DMA,
        ]

    def near(self, i):
        place = self.place
        return pltpu.make_async_copy(self.fresh.at[i], self.bundle.at[place.dp, place.t], self.near_sem)

    def handed(self, i, label):
        place = self.place
        to = self.core + 2 * i
        return remote(
            self.fresh.at[i],
            self.bundle.at[place.dp, place.t],
            self.send_sem.at[i],
            self.recv_sem.at[label],
            {"dp": place.dp, "tensor": to},
        )

    def each(self, then):
        for i in range(2):
            to = self.core + 2 * i

            @pl.when(self.place.t != to)
            def _(i=i, to=to):
                then(self.handed(i, lax.rem(self.place.t + self.place.nt - to, self.place.nt) - 1))

    def hand(self):
        self.each(lambda copy: copy.start())
        for i in range(2):

            @pl.when(self.place.t == self.core + 2 * i)
            def _(i=i):
                self.near(i).start()

    def move(self, stage, k):
        place, nz = self.place, self.place.nz
        at = self.place.nt - 1 + (k - 1 if stage == "z" else nz - 1 + k)
        sems = self.send_sem.at[2 + at], self.recv_sem.at[at]
        if stage == "z":
            where, device = place.dp, place.device(z=place.up(k))
        else:
            where, device = place.down(k) * 2 + place.y, place.device(y=1 - place.y)
        return remote(self.bundle.at[where], self.bundle.at[where], *sems, device)

    def mine(self):
        return pl.when(self.place.c == self.core)

    def along_z(self):
        @self.mine()
        def _():
            self.near(0).wait()
            for label in range(self.place.nt - 1):
                self.handed(0, label).wait_recv()
            for k in range(1, self.place.nz):
                self.move("z", k).start()
            self.move("y", 0).start()

    def along_y(self):
        @self.mine()
        def _():
            for k in range(1, self.place.nz):
                self.move("z", k).wait_recv()
                self.move("y", k).start()

    def end(self):
        self.each(lambda copy: copy.wait_send())

        @self.mine()
        def _():
            for k in range(self.place.nz):
                self.move("y", k).wait_recv()
            for k in range(self.place.nz):
                self.move("y", k).wait_send()
                if k:
                    self.move("z", k).wait_send()


def renew(totals, momenta, grad_out, fresh, images):
    values = []
    for total, momentum, out in zip(totals, momenta, grad_out):
        grad = total / images
        out[...] = grad
        values.append(MOMENTUM * momentum[...] + grad)
    for i, value in enumerate(values):
        fresh[i, 0 : value.shape[0], :] = value.astype(BF16)


def gather_kernel(ndp, nt, count, *refs):
    Gather(Place(ndp, nt), refs[:count], refs[count : 2 * count], refs[2 * count :]).at_once()


def gather_weights(slabs, ndp, nt, collective_id):
    count, n = len(slabs), ndp * nt
    gathered = pl.pallas_call(
        functools.partial(gather_kernel, ndp, nt, count),
        out_shape=tuple(shape_of((n,) + s.shape, BF16) for s in slabs),
        in_specs=[pl.BlockSpec(memory_space=pltpu.VMEM)] * count,
        out_specs=tuple(pl.BlockSpec(memory_space=pl.ANY) for _ in slabs),
        scratch_shapes=Gather.scratch([s.shape for s in slabs], n),
        compiler_params=pltpu.CompilerParams(
            collective_id=collective_id, has_side_effects=True, vmem_limit_bytes=VMEM_LIMIT
        ),
        name="gather_weights",
    )(*slabs)
    return tuple(g.reshape(n * s.shape[0], D) for g, s in zip(gathered, slabs))


SMALL_ROWS = 32
TABLE_ROW = 16


class SmallSum:
    def __init__(self, place, values, arrived, send_sem, recv_sem):
        self.values, self.arrived = values, arrived
        self.send_sem, self.recv_sem = send_sem, recv_sem
        self.steps = [
            place.device(c=1 - place.c),
            place.device(x=1 - place.x),
            place.device(y=1 - place.y),
        ]
        bit = 0
        while 2**bit < place.nz:
            self.steps.append(place.device(z=place.bit_partner(bit)))
            bit += 1
        self.done = 0

    def copy(self, i):
        return remote(
            self.values.at[i], self.arrived.at[i], self.send_sem.at[i], self.recv_sem.at[i], self.steps[i]
        )

    def begin(self):
        self.copy(0).start()

    def step(self):
        i = self.done
        if i < len(self.steps):
            self.copy(i).wait_recv()
            self.values[i + 1] = self.values[i] + self.arrived[i]
            self.done += 1

    def go_on(self):
        if 0 < self.done < len(self.steps):
            self.copy(self.done).start()

    def end(self):
        while self.done < len(self.steps):
            self.step()
            self.go_on()
        for i in range(len(self.steps)):
            self.copy(i).wait_send()
        return self.values[len(self.steps)]


def update_kernel(ndp, nt, images, *refs):
    refs = list(refs)

    def take(n):
        taken = refs[:n]
        del refs[:n]
        return taken

    grads, momenta = take(2), take(2)
    sums1, sums2, head, hidden, table = take(5)
    grad_out = take(2)
    bundle, small_out = take(2)
    fresh, small, small_in, small_send, small_recv = take(5)
    share_scratch = take(3)
    place = Place(ndp, nt)
    small[0] = jnp.zeros_like(small[0])
    small[0, 0:1, :] = sums1[0:1, :]
    small[0, 1:2, :] = sums2[0:1, :]
    small[0, 2:3, :] = sums1[1:2, :]
    small[0, 3:6, :] = sums2[1:4, :]
    small[0, 6:8, :] = head[...]
    for i in range(hidden.shape[1] // D):
        small[0, 8 + i : 9 + i, :] = hidden[0:1, i * D : (i + 1) * D]
    small[0, TABLE_ROW : TABLE_ROW + table.shape[0], 0 : table.shape[1]] = table[...]
    fresh[...] = jnp.zeros_like(fresh)
    place.greet()
    reduce = Reduce(place, grads, refs)
    tiny = SmallSum(place, small, small_in, small_send, small_recv)
    tiny.begin()
    reduce.begin()
    for a, b in ((1, 1), (1, 0), (0, 1), (0, 0)):
        reduce.pass_on(a, b, tiny.step)
        tiny.go_on()
    renew(reduce.totals(), momenta, grad_out, fresh, images)
    tiny.step()
    share = Share(place, 0, fresh, bundle, share_scratch)
    share.hand()
    small_out[...] = tiny.end() / images
    share.along_z()
    share.along_y()
    share.end()
    reduce.end()


def padded(rows):
    return -(-max(rows) // 16) * 16


def update(grads, momenta, small_sums, ndp, nt, images, collective_id):
    n = ndp * nt
    slabs = [m.shape[0] for m in momenta]
    grads = tuple(g.reshape(n, r, D) for g, r in zip(grads, slabs))
    small_steps = 3 + (ndp // 2 - 1).bit_length()
    vmem, any_ = pl.BlockSpec(memory_space=pltpu.VMEM), pl.BlockSpec(memory_space=pl.ANY)
    return pl.pallas_call(
        functools.partial(update_kernel, ndp, nt, images),
        out_shape=tuple(shape_of(m.shape, F32) for m in momenta)
        + (shape_of((ndp, nt, padded(slabs), D), BF16), shape_of((SMALL_ROWS, D), F32)),
        in_specs=[any_] * 2 + [vmem] * 7,
        out_specs=(vmem, vmem, any_, vmem),
        scratch_shapes=[
            pltpu.VMEM((2, padded(slabs), D), BF16),
            pltpu.VMEM((small_steps + 1, SMALL_ROWS, D), F32),
            pltpu.VMEM((small_steps, SMALL_ROWS, D), F32),
            pltpu.SemaphoreType.DMA((small_steps,)),
            pltpu.SemaphoreType.DMA((small_steps,)),
        ]
        + Share.scratch(n, nt)
        + Reduce.scratch(slabs, n),
        compiler_params=pltpu.CompilerParams(
            collective_id=collective_id, has_side_effects=True, vmem_limit_bytes=VMEM_LIMIT
        ),
        name="update",
    )(*grads, *momenta, *small_sums)


def newton_schulz_kernel(first_ref, second_ref, out_ref, g_scr, x_scr, a_scr, sem):
    first, second, third = QUINTIC
    chunk = 512
    core = lax.axis_index("tensor") % 2
    dp = lax.axis_index("dp")
    sources = (first_ref, second_ref)
    for which, ref in enumerate(sources):

        @pl.when(core == which)
        def _(ref=ref):
            copy = pltpu.make_async_copy(ref, g_scr.at[0 : ref.shape[0]], sem)
            copy.start()
            copy.wait()

    chunks = jnp.where(core == 0, first_ref.shape[0] // chunk, second_ref.shape[0] // chunk)

    def low(values):
        return values.astype(BF16)

    def gram(src_ref):
        a_scr[...] = jnp.zeros_like(a_scr)

        def add(at, carry):
            part = src_ref[pl.ds(pl.multiple_of(at * chunk, chunk), chunk), :]
            a_scr[...] += dot_tn(part, part)
            return carry

        lax.fori_loop(0, chunks, add, 0)
        return a_scr[...]

    def advance(src_ref, factor, scale):
        factor = low(factor)

        def step(at, carry):
            at = pl.ds(pl.multiple_of(at * chunk, chunk), chunk)
            x_scr[at, :] = low(dot_nn(src_ref[at, :], factor) * scale)
            return carry

        lax.fori_loop(0, chunks, step, 0)

    def bend(a):
        return second * a + third * dot_nn(low(a), low(a))

    diagonal = lax.broadcasted_iota(jnp.int32, (D, D), 0) == lax.broadcasted_iota(jnp.int32, (D, D), 1)

    def two_turns(a):
        b = bend(a)
        q = b + jnp.where(diagonal, first, 0.0)
        r = first * a + dot_nn(low(a), low(b))
        a = first * r + dot_nn(low(r), low(b))
        b = bend(a)
        return first * q + dot_nn(low(b), low(q))

    a = gram(g_scr)
    scale = 1.0 / (jnp.sqrt(jnp.sum(jnp.where(diagonal, a, 0.0))) + MUON_EPSILON)
    advance(g_scr, two_turns(a * scale * scale), scale)
    q = two_turns(gram(x_scr))
    for which, ref in enumerate(sources):

        @pl.when(core == which)
        def _(ref=ref):
            mine = ref.shape[0] // lax.axis_size("dp")
            at = pl.ds(pl.multiple_of(dp * mine, mine), mine)
            out_ref[0:mine, :] = dot_nn(x_scr[at, :], low(q))

    advance(x_scr, q, 1.0)
    b = bend(gram(x_scr))
    here = out_ref[...]
    out_ref[...] = first * here + dot_nn(low(here), low(b))


def newton_schulz(bundles):
    ndp, nt = bundles[0].shape[:2]
    rows = [ndp * nt * b.shape[2] for b in bundles]
    tall = max(rows)
    any_ = pl.BlockSpec(memory_space=pl.ANY)
    return pl.pallas_call(
        newton_schulz_kernel,
        out_shape=shape_of((tall // ndp, D), F32),
        in_specs=[any_, any_],
        out_specs=pl.BlockSpec(memory_space=pltpu.VMEM),
        scratch_shapes=[
            pltpu.VMEM((tall, D), BF16),
            pltpu.VMEM((tall, D), BF16),
            pltpu.VMEM((D, D), F32),
            pltpu.SemaphoreType.DMA,
        ],
        compiler_params=pltpu.CompilerParams(vmem_limit_bytes=VMEM_LIMIT),
        name="newton_schulz",
    )(*(b.reshape(r, D) for b, r in zip(bundles, rows)))


def return_kernel(ndp, nt, heights, x_ref, *refs):
    outs = refs[:2]
    send_sem, recv_sem = refs[2:]
    dp, t = lax.axis_index("dp"), lax.axis_index("tensor")
    barrier = pltpu.get_barrier_semaphore()
    for d in range(1, nt):
        other = {"dp": dp, "tensor": lax.rem(t + d, nt)}
        pl.semaphore_signal(barrier, inc=1, device_id=other, device_id_type=MESH)
    pl.semaphore_wait(barrier, nt - 1)

    def copy(which, d):
        to = lax.rem(t + d, nt)
        height = heights[which]
        return remote(
            x_ref.at[pl.ds(pl.multiple_of(to * height, height), height)],
            outs[which].at[t // 2],
            send_sem.at[d - 1],
            recv_sem.at[d - 1],
            {"dp": dp, "tensor": to},
        )

    for which in range(2):

        @pl.when(t % 2 == which)
        def _(which=which):
            for d in range(1, nt):
                copy(which, d).start()
            height = heights[which]
            outs[which][t // 2] = x_ref[pl.ds(pl.multiple_of(t * height, height), height), :]

    for d in range(1, nt):
        for which in range(2):

            @pl.when(lax.rem(t + nt - d, nt) % 2 == which)
            def _(d=d, which=which):
                copy(which, d).wait_recv()

    for which in range(2):

        @pl.when(t % 2 == which)
        def _(which=which):
            for d in range(1, nt):
                copy(which, d).wait_send()


def return_updates(x, heights, ndp, nt, collective_id):
    return pl.pallas_call(
        functools.partial(return_kernel, ndp, nt, heights),
        out_shape=tuple(shape_of((nt // 2, h, D), F32) for h in heights),
        in_specs=[pl.BlockSpec(memory_space=pltpu.VMEM)],
        out_specs=(pl.BlockSpec(memory_space=pltpu.VMEM),) * 2,
        scratch_shapes=[pltpu.SemaphoreType.DMA((nt - 1,)), pltpu.SemaphoreType.DMA((nt - 1,))],
        compiler_params=pltpu.CompilerParams(collective_id=collective_id, has_side_effects=True),
        name="return_updates",
    )(x)


def finish_kernel(nt, rates, *refs):
    refs = list(refs)

    def take(n):
        taken = refs[:n]
        del refs[:n]
        return taken

    landed, (total,) = take(2), take(1)
    grads, momenta, weights = take(nt), take(nt), take(nt)
    small_par, small_mom = take(5), take(5)
    grad_out, new_out, mom_out = take(nt), take(nt), take(nt)
    small_grad_out, small_new_out, small_mom_out = take(5), take(5), take(5)
    for m in range(nt):
        grad = grads[m][...]
        grad_out[m][...] = grad
        mom_out[m][...] = MOMENTUM * momenta[m][...] + grad
        new_out[m][...] = weights[m][...] - rates[m] * landed[m % 2][m // 2, 0 : grad.shape[0], :]

    def small_update(i, at, grad):
        small_grad_out[i][at] = grad
        grad = MOMENTUM * small_mom[i][at] + grad
        small_mom_out[i][at] = grad
        small_new_out[i][at] = small_par[i][at] - VECTOR_RATE * grad

    for i, (low, high) in enumerate(((0, 2), (2, 6), (6, 8))):
        small_update(i, (slice(None), slice(None)), total[low:high, :])
    for i in range(small_par[3].shape[1] // D):
        small_update(3, (slice(0, 1), slice(i * D, (i + 1) * D)), total[8 + i : 9 + i, :])
    heads, rows = small_par[4].shape
    small_update(4, (slice(None), slice(None)), total[TABLE_ROW : TABLE_ROW + heads, 0:rows])


def finish(landed, total, grads, momenta, weights, small_params, small_moms, rates):
    nt = len(grads)
    like = lambda arrays: tuple(shape_of(a.shape, F32) for a in arrays)
    return pl.pallas_call(
        functools.partial(finish_kernel, nt, rates),
        out_shape=like(grads) * 3 + like(small_params) * 3,
        compiler_params=pltpu.CompilerParams(vmem_limit_bytes=VMEM_LIMIT),
        name="finish",
    )(*landed, total, *grads, *momenta, *weights, *small_params, *small_moms)


def attention_forward_kernel(
    ndp,
    nt,
    x_ref,
    wqkv_ref,
    wproj_ref,
    gain_ref,
    shift_ref,
    qkvb_ref,
    table_ref,
    index_ref,
    region_ref,
    slab1_ref,
    slab2_ref,
    y_ref,
    xs_ref,
    qkv_ref,
    p_ref,
    o_ref,
    all1_ref,
    all2_ref,
    bias_scr,
    idx_scr,
    tab_scr,
    mask_scr,
    turn_scr,
    y_scr,
    *gather_scr,
):
    step, last = pl.program_id(0), pl.num_programs(0) - 1
    gather = Gather(Place(ndp, nt), (slab1_ref, slab2_ref), (all1_ref, all2_ref), gather_scr)

    @pl.when(step == 0)
    def _():
        gather.begin()
        build_bias(region_ref, index_ref, table_ref, bias_scr, idx_scr, tab_scr)
        mask_scr[...] = head_mask(range(OCT))
        turn_scr[...] = head_mask(TURNED)

    xs_ref[...] = jnp.zeros_like(xs_ref)
    into_slots(x_ref, xs_ref)
    white, _ = whiten(xs_ref[...])
    a1 = (white * gain_ref[0:1, :] + shift_ref[0:1, :]).astype(BF16)
    scale = HEAD ** (-0.5)
    for half in range(2):
        columns = 3 * PART * GROUPS // 2
        u = dot_nt(a1, wqkv_ref[half * columns : (half + 1) * columns, :])
        for inner in range(GROUPS // 2):
            group = half * (GROUPS // 2) + inner
            for part in range(3):
                piece = u[:, (inner * 3 + part) * PART : (inner * 3 + part + 1) * PART]
                if part == 0:
                    piece = (piece + qkvb_ref[0:1, group * PART : (group + 1) * PART]) * scale
                elif part == 2:
                    piece = piece + qkvb_ref[1:2, group * PART : (group + 1) * PART]
                at = part * D + group * PART
                qkv_ref[:, at : at + PART] = piece.astype(BF16)

    real_query = (lax.broadcasted_iota(jnp.int32, (1, OCT_S), 1) % SLOT < SPOTS).astype(F32)

    def one_window(at, carry):
        rows = pl.ds(pl.multiple_of(at * SLOT, SLOT), SLOT)
        for octet in range(OCTS):
            q = qkv_ref[rows, octet * OCT_W : (octet + 1) * OCT_W]
            k = qkv_ref[rows, D + octet * OCT_W : D + (octet + 1) * OCT_W]
            v = qkv_ref[rows, 2 * D + octet * OCT_W : 2 * D + (octet + 1) * OCT_W]
            scores = dot_nt(k, spread(q, mask_scr)) + bias_scr[lax.rem(at, WINDOWS), octet]
            grown = jnp.exp(scores - jnp.max(scores, axis=0, keepdims=True))
            probs = grown * (real_query / jnp.sum(grown, axis=0, keepdims=True))
            p_ref[rows, octet * OCT_S : (octet + 1) * OCT_S] = probs.astype(BF16)
            o_ref[rows, octet * OCT_W : (octet + 1) * OCT_W] = dot_nn(
                turned(probs).astype(BF16), spread(v, turn_scr)
            ).astype(BF16)
        return carry

    lax.fori_loop(0, STEP_IMAGES * WINDOWS, one_window, 0)
    y_scr[...] = xs_ref[...] + dot_nn(o_ref[...], wproj_ref[...]) + shift_ref[2:3, :]
    out_of_slots(y_scr, y_ref)

    @pl.when(step == 0)
    def _():
        for k in gather.round()[1:]:
            gather.column(k)

    @pl.when(step == 1)
    def _():
        for k in gather.round():
            gather.first(k)

    @pl.when(step == 2)
    def _():
        for a in range(2):
            for k in gather.round():
                gather.second(a, k)

    @pl.when(step == last)
    def _():
        gather.end()


def mlp_kernel(
    y_ref,
    e_ref,
    w1_ref,
    w2_ref,
    gain_ref,
    shift_ref,
    hb_ref,
    out_ref,
    dy_ref,
    g1_ref,
    g2_ref,
    hsum_ref,
    sums_ref,
    acc1,
    acc2,
    m_scr,
    da_scr,
    a2_scr,
    e_scr,
):
    step = pl.program_id(0)

    @pl.when(step == 0)
    def _():
        acc1[...] = jnp.zeros_like(acc1)
        acc2[...] = jnp.zeros_like(acc2)
        hsum_ref[...] = jnp.zeros_like(hsum_ref)
        sums_ref[...] = jnp.zeros_like(sums_ref)

    white, inverse = whiten(y_ref[...])
    a2_scr[...] = (white * gain_ref[1:2, :] + shift_ref[1:2, :]).astype(BF16)
    e_scr[...] = e_ref[...].astype(BF16)
    m_scr[...] = jnp.zeros_like(m_scr)
    da_scr[...] = jnp.zeros_like(da_scr)
    root = math.sqrt(2.0 / math.pi)
    width = 512

    def chunk(c, carry):
        at = pl.ds(pl.multiple_of(c * width, width), width)
        w1, w2 = w1_ref[at, :], w2_ref[at, :]
        a2, e = a2_scr[...], e_scr[...]
        z = dot_nt(a2, w1) + hb_ref[0:1, at]
        square = z * z
        t = jnp.tanh(z * (root + (root * 0.044715) * square))
        half = 0.5 * z
        f = (half + half * t).astype(BF16)
        slope = 0.5 + 0.5 * t + half * (1.0 - t * t) * (root + (3.0 * root * 0.044715) * square)
        dz = dot_nt(e, w2) * slope
        hsum_ref[0:1, at] += jnp.sum(dz, axis=0, keepdims=True)
        dz = dz.astype(BF16)
        m_scr[...] += dot_nn(f, w2)
        da_scr[...] += dot_nn(dz, w1)
        acc2[at, :] += dot_tn(f, e)
        acc1[at, :] += dot_tn(dz, a2)
        return carry

    lax.fori_loop(0, w1_ref.shape[0] // width, chunk, 0)
    white, inverse = whiten(y_ref[...])
    out_ref[...] = y_ref[...] + m_scr[...] + shift_ref[3:4, :]
    da = da_scr[...]
    t2 = da * gain_ref[1:2, :]
    dy = e_ref[...] + inverse * (t2 - row_mean(t2) - white * row_mean(t2 * white))
    dy_ref[...] = dy
    sums_ref[0:1, :] += jnp.sum(da * white, axis=0, keepdims=True)
    sums_ref[1:2, :] += jnp.sum(da, axis=0, keepdims=True)
    sums_ref[2:3, :] += jnp.sum(dy, axis=0, keepdims=True)
    sums_ref[3:4, :] += jnp.sum(e_ref[...], axis=0, keepdims=True)

    @pl.when(step == pl.num_programs(0) - 1)
    def _():
        g1_ref[...] = acc1[...].astype(BF16)
        g2_ref[...] = acc2[...].astype(BF16)


def attention_backward_kernel(
    ndp,
    nt,
    images,
    dy_ref,
    xs_ref,
    qkv_ref,
    p_ref,
    o_ref,
    wqkv_ref,
    wproj_ref,
    gain_ref,
    shift_ref,
    g1_ref,
    g2_ref,
    m1_ref,
    m2_ref,
    gin_ref,
    gqkv_ref,
    gproj_ref,
    dbias_ref,
    hsum_ref,
    sums_ref,
    slab1_ref,
    slab2_ref,
    bundle_ref,
    accq,
    accp,
    dy_scr,
    do_scr,
    du_scr,
    mask_scr,
    turn_scr,
    g_scr,
    fresh,
    *comm_scr,
):
    step, last = pl.program_id(0), pl.num_programs(0) - 1
    place = Place(ndp, nt)
    share = Share(place, 1, fresh, bundle_ref, comm_scr[:3])
    reduce = Reduce(place, (g1_ref, g2_ref), comm_scr[3:])

    @pl.when(step == 0)
    def _():
        place.greet()
        reduce.begin()
        fresh[...] = jnp.zeros_like(fresh)
        mask_scr[...] = head_mask(range(OCT))
        turn_scr[...] = head_mask(TURNED)
        accq[...] = jnp.zeros_like(accq)
        accp[...] = jnp.zeros_like(accp)
        dbias_ref[...] = jnp.zeros_like(dbias_ref)
        hsum_ref[...] = jnp.zeros_like(hsum_ref)
        sums_ref[...] = jnp.zeros_like(sums_ref)
        dy_scr[...] = jnp.zeros_like(dy_scr)

    @pl.when(step == 2)
    def _():
        reduce.pass_on(0, 0)

    @pl.when(step == last)
    def _():
        share.along_z()

    into_slots(dy_ref, dy_scr)
    dr = dy_scr[...].astype(BF16)
    do_scr[...] = dot_nt(dr, wproj_ref[...]).astype(BF16)
    accp[...] += dot_tn(o_ref[...], dr)
    scale = HEAD ** (-0.5)

    def one_window(at, carry):
        rows = pl.ds(pl.multiple_of(at * SLOT, SLOT), SLOT)
        for octet in range(OCTS):
            q = qkv_ref[rows, octet * OCT_W : (octet + 1) * OCT_W]
            k = qkv_ref[rows, D + octet * OCT_W : D + (octet + 1) * OCT_W]
            v = qkv_ref[rows, 2 * D + octet * OCT_W : 2 * D + (octet + 1) * OCT_W]
            do = do_scr[rows, octet * OCT_W : (octet + 1) * OCT_W]
            probs = p_ref[rows, octet * OCT_S : (octet + 1) * OCT_S]
            wide_do = spread(do, mask_scr)
            weighted = probs.astype(F32) * dot_nt(v, wide_do)
            ds = weighted - probs.astype(F32) * jnp.sum(weighted, axis=0, keepdims=True)
            dbias_ref[octet] += ds
            dq = dot_nn(turned(ds).astype(BF16), spread(k, turn_scr)) * scale
            dk = dot_nn(ds.astype(BF16), spread(q, mask_scr))
            dv = dot_nn(probs, wide_do)
            lanes = slice(octet * OCT_W, (octet + 1) * OCT_W)
            hsum_ref[0:1, lanes] += jnp.sum(dq, axis=0, keepdims=True)
            hsum_ref[1:2, lanes] += jnp.sum(dv, axis=0, keepdims=True)
            for part, grad in enumerate((dq, dk, dv)):
                for inner in range(OCT_W // PART):
                    group = octet * (OCT_W // PART) + inner
                    at_col = (group * 3 + part) * PART
                    du_scr[rows, at_col : at_col + PART] = grad[
                        :, inner * PART : (inner + 1) * PART
                    ].astype(BF16)
        return carry

    lax.fori_loop(0, STEP_IMAGES * WINDOWS, one_window, 0)

    @pl.when(step == 0)
    def _():
        reduce.pass_on(1, 1)
        reduce.pass_on(1, 0)

    @pl.when(step == 1)
    def _():
        reduce.pass_on(0, 1)

    @pl.when(step == 2)
    def _():
        renew(reduce.totals(), (m1_ref, m2_ref), (slab1_ref, slab2_ref), fresh, images)
        share.hand()

    @pl.when(step == last)
    def _():
        share.along_y()

    white, inverse = whiten(xs_ref[...])
    a1 = (white * gain_ref[0:1, :] + shift_ref[0:1, :]).astype(BF16)
    accq[...] += dot_tn(du_scr[...], a1)
    da = dot_nn(du_scr[...], wqkv_ref[...])
    t1 = da * gain_ref[0:1, :]
    g_scr[...] = dy_scr[...] + inverse * (t1 - row_mean(t1) - white * row_mean(t1 * white))
    out_of_slots(g_scr, gin_ref)
    sums_ref[0:1, :] += jnp.sum(da * white, axis=0, keepdims=True)
    sums_ref[1:2, :] += jnp.sum(da, axis=0, keepdims=True)

    @pl.when(step == pl.num_programs(0) - 1)
    def _():
        gqkv_ref[...] = accq[...].astype(BF16)
        gproj_ref[...] = accp[...].astype(BF16)
        share.end()
        reduce.end()


def whole(shape):
    return pl.BlockSpec(shape, lambda i: (0,) * len(shape))


def rows_of(rows, columns):
    return pl.BlockSpec((rows, columns), lambda i: (i, 0))


def shape_of(shape, dtype):
    return jax.ShapeDtypeStruct(shape, dtype)


PARAMS = pltpu.CompilerParams(dimension_semantics=("arbitrary",), vmem_limit_bytes=VMEM_LIMIT)


def remote_params(collective_id):
    return pltpu.CompilerParams(
        dimension_semantics=("arbitrary",),
        vmem_limit_bytes=VMEM_LIMIT,
        collective_id=collective_id,
        has_side_effects=True,
    )


def attention_forward(
    tokens, wqkv, wproj, gains, shifts, head_biases, table, index, regions, slabs, ndp, nt, collective_id
):
    n = ndp * nt
    steps = tokens.shape[0] // STEP_ROWS
    slots = steps * STEP_SLOTS
    return pl.pallas_call(
        functools.partial(attention_forward_kernel, ndp, nt),
        grid=(steps,),
        out_shape=(
            shape_of(tokens.shape, F32),
            shape_of((slots, D), F32),
            shape_of((slots, 3 * D), BF16),
            shape_of((slots, OCTS * OCT_S), BF16),
            shape_of((slots, D), BF16),
        )
        + tuple(shape_of((n,) + s.shape, BF16) for s in slabs),
        in_specs=[
            rows_of(STEP_ROWS, D),
            whole(wqkv.shape),
            whole(wproj.shape),
            whole(gains.shape),
            whole(shifts.shape),
            whole(head_biases.shape),
            whole(table.shape),
            whole(index.shape),
            pl.BlockSpec(memory_space=pltpu.SMEM),
            whole(slabs[0].shape),
            whole(slabs[1].shape),
        ],
        out_specs=(
            rows_of(STEP_ROWS, D),
            rows_of(STEP_SLOTS, D),
            rows_of(STEP_SLOTS, 3 * D),
            rows_of(STEP_SLOTS, OCTS * OCT_S),
            rows_of(STEP_SLOTS, D),
            pl.BlockSpec(memory_space=pl.ANY),
            pl.BlockSpec(memory_space=pl.ANY),
        ),
        scratch_shapes=[
            pltpu.VMEM((WINDOWS, OCTS, SLOT, OCT_S), F32),
            pltpu.VMEM((LANES, LANES), F32),
            pltpu.VMEM((HEADS, 2 * LANES), F32),
            pltpu.VMEM((OCT_S, OCT_W), BF16),
            pltpu.VMEM((OCT_S, OCT_W), BF16),
            pltpu.VMEM((STEP_SLOTS, D), F32),
        ]
        + Gather.scratch([s.shape for s in slabs], n),
        compiler_params=remote_params(collective_id),
        name="attention_forward",
    )(tokens, wqkv, wproj, gains, shifts, head_biases, table, index, regions, *slabs)


def mlp(middle, out_grad, w1, w2, gains, shifts, hidden_bias):
    steps = middle.shape[0] // STEP_ROWS
    hidden = w1.shape[0]
    return pl.pallas_call(
        mlp_kernel,
        grid=(steps,),
        out_shape=(
            shape_of(middle.shape, F32),
            shape_of(middle.shape, F32),
            shape_of(w1.shape, BF16),
            shape_of(w2.shape, BF16),
            shape_of((1, hidden), F32),
            shape_of((4, D), F32),
        ),
        in_specs=[
            rows_of(STEP_ROWS, D),
            rows_of(STEP_ROWS, D),
            whole(w1.shape),
            whole(w2.shape),
            whole(gains.shape),
            whole(shifts.shape),
            whole((1, hidden)),
        ],
        out_specs=(
            rows_of(STEP_ROWS, D),
            rows_of(STEP_ROWS, D),
            whole(w1.shape),
            whole(w2.shape),
            whole((1, hidden)),
            whole((4, D)),
        ),
        scratch_shapes=[
            pltpu.VMEM(w1.shape, F32),
            pltpu.VMEM(w2.shape, F32),
            pltpu.VMEM((STEP_ROWS, D), F32),
            pltpu.VMEM((STEP_ROWS, D), F32),
            pltpu.VMEM((STEP_ROWS, D), BF16),
            pltpu.VMEM((STEP_ROWS, D), BF16),
        ],
        compiler_params=PARAMS,
        name="mlp",
    )(middle, out_grad, w1, w2, gains, shifts, hidden_bias.reshape(1, hidden))


def attention_backward(
    dy, xs, qkv, probs, mixed, wqkv, wproj, gains, shifts, grads, momenta, ndp, nt, images, collective_id
):
    n = ndp * nt
    slabs = [m.shape[0] for m in momenta]
    grads = tuple(g.reshape(n, r, D) for g, r in zip(grads, slabs))
    any_ = pl.BlockSpec(memory_space=pl.ANY)
    steps = dy.shape[0] // STEP_ROWS
    return pl.pallas_call(
        functools.partial(attention_backward_kernel, ndp, nt, images),
        grid=(steps,),
        out_shape=(
            shape_of(dy.shape, F32),
            shape_of(wqkv.shape, BF16),
            shape_of(wproj.shape, BF16),
            shape_of((OCTS, SLOT, OCT_S), F32),
            shape_of((2, D), F32),
            shape_of((2, D), F32),
        )
        + tuple(shape_of(m.shape, F32) for m in momenta)
        + (shape_of((ndp, nt, padded(slabs), D), BF16),),
        in_specs=[
            rows_of(STEP_ROWS, D),
            rows_of(STEP_SLOTS, D),
            rows_of(STEP_SLOTS, 3 * D),
            rows_of(STEP_SLOTS, OCTS * OCT_S),
            rows_of(STEP_SLOTS, D),
            whole(wqkv.shape),
            whole(wproj.shape),
            whole(gains.shape),
            whole(shifts.shape),
            any_,
            any_,
            whole(momenta[0].shape),
            whole(momenta[1].shape),
        ],
        out_specs=(
            rows_of(STEP_ROWS, D),
            whole(wqkv.shape),
            whole(wproj.shape),
            whole((OCTS, SLOT, OCT_S)),
            whole((2, D)),
            whole((2, D)),
            whole(momenta[0].shape),
            whole(momenta[1].shape),
            any_,
        ),
        scratch_shapes=[
            pltpu.VMEM(wqkv.shape, F32),
            pltpu.VMEM(wproj.shape, F32),
            pltpu.VMEM((STEP_SLOTS, D), F32),
            pltpu.VMEM((STEP_SLOTS, D), BF16),
            pltpu.VMEM((STEP_SLOTS, 3 * D), BF16),
            pltpu.VMEM((OCT_S, OCT_W), BF16),
            pltpu.VMEM((OCT_S, OCT_W), BF16),
            pltpu.VMEM((STEP_SLOTS, D), F32),
            pltpu.VMEM((2, padded(slabs), D), BF16),
        ]
        + Share.scratch(n, nt)
        + Reduce.scratch(slabs, n),
        compiler_params=remote_params(collective_id),
        name="attention_backward",
    )(dy, xs, qkv, probs, mixed, wqkv, wproj, gains, shifts, *grads, *momenta)


ORDER = (0, 2, 1, 3)
WIDE = (True, True, False, False)
FACTORS = (
    math.sqrt(3.0),
    math.sqrt(max(1.0, FF / D)),
    1.0,
    math.sqrt(max(1.0, D / FF)),
)


def as_slab(block, wide):
    return block.reshape(D, -1).T if wide else block.reshape(-1, D)


def as_block(slab, like, wide):
    return (slab.T if wide else slab).reshape(like.shape)


def shards(
    tokens,
    out_grad,
    qkv_weight,
    proj_weight,
    fc1_weight,
    fc2_weight,
    qkv_momentum,
    proj_momentum,
    fc1_momentum,
    fc2_momentum,
    norm_gains,
    shift_biases,
    head_biases,
    hidden_bias,
    position_table,
    gain_momentum,
    shift_momentum,
    head_bias_momentum,
    hidden_bias_momentum,
    table_momentum,
    region_ids,
    position_index,
):
    devices = lax.axis_size("dp") * lax.axis_size("tensor")
    images = tokens.shape[0] // AREA * devices
    blocks = (qkv_weight, fc1_weight, proj_weight, fc2_weight)
    weights = tuple(as_slab(w, wide) for w, wide in zip(blocks, WIDE))
    momenta = tuple(
        as_slab(m, wide)
        for m, wide in zip((qkv_momentum, fc1_momentum, proj_momentum, fc2_momentum), WIDE)
    )
    ndp, nt = lax.axis_size("dp"), lax.axis_size("tensor")
    wqkv, wproj = gather_weights(weights[0::2], ndp, nt, 0)
    middle, xs, qkv, probs, mixed, w1, w2 = attention_forward(
        tokens,
        wqkv,
        wproj,
        norm_gains,
        shift_biases,
        head_biases,
        position_table.T,
        position_index,
        region_ids,
        weights[1::2],
        ndp,
        nt,
        1,
    )
    w1, w2 = w1.reshape(-1, D), w2.reshape(-1, D)
    output, dy, g1, g2, hidden_sum, sums2 = mlp(
        middle, out_grad, w1, w2, norm_gains, shift_biases, hidden_bias
    )
    input_grad, gqkv, gproj, dbias, head_sum, sums1, slab1, slab2, bundle1 = attention_backward(
        dy,
        xs,
        qkv,
        probs,
        mixed,
        wqkv,
        wproj,
        norm_gains,
        shift_biases,
        (g1, g2),
        momenta[1::2],
        ndp,
        nt,
        images,
        2,
    )
    by_head = (
        dbias.reshape(OCTS, SLOT, OCT, SLOT)[:, :SPOTS, :, :SPOTS]
        .transpose(0, 2, 3, 1)
        .reshape(HEADS, SPOTS * SPOTS)
    )
    onehot = (
        position_index.reshape(-1)[:, None]
        == jnp.arange(position_table.shape[0], dtype=jnp.int32)[None, :]
    ).astype(F32)
    table_part = jnp.dot(onehot.T, by_head.T, precision=lax.Precision.HIGHEST)
    small_params = (norm_gains, shift_biases, head_biases, hidden_bias.reshape(1, -1), position_table.T)
    small_moms = (
        gain_momentum,
        shift_momentum,
        head_bias_momentum,
        hidden_bias_momentum.reshape(1, -1),
        table_momentum.T,
    )
    slab0, slab3, bundle0, total = update(
        (gqkv, gproj),
        momenta[0::2],
        (sums1, sums2, head_sum, hidden_sum, table_part.T),
        ndp,
        nt,
        images,
        3,
    )
    slab_grads = (slab0, slab1, slab3, slab2)
    bundles = (bundle0, bundle1)
    landed = return_updates(
        newton_schulz(bundles), tuple(b.shape[2] for b in bundles), ndp, nt, 4
    )
    rates = tuple(MATRIX_RATE * factor for factor in FACTORS)
    results = finish(landed, total, slab_grads, momenta, weights, small_params, small_moms, rates)
    slab_grads, new_weights, new_momenta = (results[i * nt : (i + 1) * nt] for i in range(3))
    smalls = tuple(
        s.reshape(-1) if i % 5 == 3 else s.T if i % 5 == 4 else s
        for i, s in enumerate(results[3 * nt :])
    )

    def placed(slabs):
        placed = tuple(as_block(s, like, wide) for s, like, wide in zip(slabs, blocks, WIDE))
        return tuple(placed[i] for i in ORDER)

    return (
        (output, input_grad)
        + placed(slab_grads)
        + placed(new_weights)
        + placed(new_momenta)
        + smalls
    )


def solution(mesh):
    rows = P(("dp", "tensor"), None)
    wide, tall = P(None, "tensor", "dp"), P("tensor", "dp", None)
    matrices = (wide, tall, wide, tall)
    return jax.shard_map(
        shards,
        mesh=mesh,
        in_specs=(rows, rows) + matrices * 2 + (P(),) * 12,
        out_specs=(rows, rows) + matrices * 3 + (P(),) * 15,
        check_vma=False,
    )
```

```python
import functools
import math

import jax
import jax.numpy as jnp
from jax import lax
from jax.experimental import pallas as pl
from jax.experimental.pallas import tpu as pltpu
from jax.sharding import PartitionSpec as P

D = 512
HEADS = 16
FF = 2048
HEAD = 32
WIN = 7
SIDE = 14
SHIFT = 3
NS_STEPS = 5

NORM_EPSILON = 1e-05
MASK_VALUE = -100.0
MUON_EPSILON = 1e-07
QUINTIC = (3.4445, -4.775, 2.0315)
MOMENTUM = 0.9
MATRIX_RATE = 0.5
VECTOR_RATE = 1.0

AREA = SIDE * SIDE
SPOTS = WIN * WIN
ACROSS = SIDE // WIN
WINDOWS = ACROSS * ACROSS
SLOT = 64
LANES = 128
OCT = 8
OCTS = HEADS // OCT
OCT_W = OCT * HEAD
PAIRS = OCT // 2
ROWS_S = PAIRS * SLOT
PAD_SCORE = -1e30
STEP_IMAGES = 2
STEP_ROWS = STEP_IMAGES * AREA
STEP_SLOTS = STEP_IMAGES * WINDOWS * SLOT
PART = 128
GROUPS = 4
F32 = jnp.float32
BF16 = jnp.bfloat16
VMEM_LIMIT = 60 * 1024 * 1024


def window_pieces():
    pieces = []
    for down in range(ACROSS):
        for over in range(ACROSS):
            for line in range(WIN):
                src_row = (down * WIN + line + SHIFT) % SIDE
                column = 0
                while column < WIN:
                    src_col = (over * WIN + column + SHIFT) % SIDE
                    length = min(WIN - column, SIDE - src_col)
                    slot = (down * ACROSS + over) * SLOT + line * WIN + column
                    pieces.append((slot, src_row * SIDE + src_col, length))
                    column += length
    return pieces


PIECES = window_pieces()


def dot_nn(a, b):
    return lax.dot_general(a, b, (((1,), (0,)), ((), ())), preferred_element_type=F32)


def dot_nt(a, b):
    return lax.dot_general(a, b, (((1,), (1,)), ((), ())), preferred_element_type=F32)


def dot_tn(a, b):
    return lax.dot_general(a, b, (((0,), (0,)), ((), ())), preferred_element_type=F32)


def row_mean(values):
    return jnp.mean(values, axis=-1, keepdims=True)


def whiten(values):
    center = values - row_mean(values)
    inverse = lax.rsqrt(row_mean(center * center) + NORM_EPSILON)
    return center * inverse, inverse


def into_slots(src_ref, dst_ref):
    for image in range(STEP_IMAGES):
        for slot, raster, length in PIECES:
            dst_ref[image * WINDOWS * SLOT + slot : image * WINDOWS * SLOT + slot + length, :] = src_ref[
                image * AREA + raster : image * AREA + raster + length, :
            ]


def out_of_slots(src_ref, dst_ref):
    for image in range(STEP_IMAGES):
        for slot, raster, length in PIECES:
            dst_ref[image * AREA + raster : image * AREA + raster + length, :] = src_ref[
                image * WINDOWS * SLOT + slot : image * WINDOWS * SLOT + slot + length, :
            ]


def pair_mask():
    pair = lax.broadcasted_iota(jnp.int32, (SLOT, OCT_W), 1) // (2 * HEAD)
    return jnp.concatenate([(pair == at).astype(F32) for at in range(PAIRS)], axis=0).astype(BF16)


def side_mask():
    side = lax.broadcasted_iota(jnp.int32, (SLOT, OCT_W), 1) // HEAD % 2
    return jnp.concatenate([(side == at).astype(F32) for at in range(2)], axis=0).astype(BF16)


def spread(values, mask_ref):
    return jnp.concatenate([values] * (mask_ref.shape[0] // SLOT), axis=0) * mask_ref[...]


def turned(values):
    return jnp.concatenate([values[at : at + LANES].T for at in range(0, ROWS_S, LANES)], axis=1)


def by_side(values, first_side):
    return jnp.where(first_side, values[0:SLOT], values[SLOT:])


def by_pair(weights, side_values):
    tiles = []
    first = lane_iota(SLOT) < SLOT
    for at in range(0, OCT_W, LANES):
        tile = dot_nn(weights[at : at + LANES], side_values[:, at : at + LANES])
        tiles.append(jnp.where(first, tile[0:SLOT], tile[SLOT:]))
    return jnp.concatenate(tiles, axis=1)


def lane_iota(rows):
    return lax.broadcasted_iota(jnp.int32, (rows, LANES), 1)


def build_bias(region_ref, index_ref, table_ref, bias_ref, idx_scr, tab_scr):
    heads, rows = table_ref.shape
    tab_scr[...] = jnp.zeros_like(tab_scr)
    tab_scr[:, 0:rows] = table_ref[...]
    by_head = tab_scr[...]
    lanes = lane_iota(SLOT)
    index = key_by_query(index_ref, idx_scr).astype(jnp.int32)
    sublanes = lax.broadcasted_iota(jnp.int32, (SLOT, LANES), 0)
    spot = lanes % SLOT
    masks = []
    for down in range(ACROSS):
        for over in range(ACROSS):
            row_ids = jnp.full((SLOT, LANES), -1, jnp.int32)
            col_ids = jnp.full((SLOT, LANES), -1, jnp.int32)
            for at in range(SPOTS):
                value = region_ref[down * WIN + at // WIN, over * WIN + at % WIN]
                row_ids = jnp.where(sublanes == at, value, row_ids)
                col_ids = jnp.where(spot == at, value, col_ids)
            masks.append(
                jnp.where(sublanes < SPOTS, jnp.where(row_ids == col_ids, 0.0, MASK_VALUE), PAD_SCORE)
            )
    low = index < LANES
    index_low = jnp.where(low, index, 0)
    index_high = jnp.where(low, 0, index - LANES)

    def gathered(head):
        first = jnp.broadcast_to(by_head[head : head + 1, 0:LANES], (SLOT, LANES))
        second = jnp.broadcast_to(by_head[head : head + 1, LANES : 2 * LANES], (SLOT, LANES))
        return jnp.where(
            low,
            jnp.take_along_axis(first, index_low, axis=1),
            jnp.take_along_axis(second, index_high, axis=1),
        )

    for octet in range(OCTS):
        for pair in range(PAIRS):
            head = octet * OCT + 2 * pair
            tile = jnp.where(lanes < SLOT, gathered(head), gathered(head + 1))
            for window in range(WINDOWS):
                bias_ref[window, octet, pair * SLOT : (pair + 1) * SLOT, :] = tile + masks[window]


MESH = pl.DeviceIdType.MESH


def flipped(bit, by):
    return bit + by - 2 * bit * by


class Place:
    def __init__(self, ndp, nt):
        self.ndp, self.nt = ndp, nt
        self.nz = ndp // 2
        self.dp, self.t = lax.axis_index("dp"), lax.axis_index("tensor")
        self.z, self.y = self.dp // 2, self.dp % 2
        self.x, self.c = self.t // 2, self.t % 2

    def up(self, k):
        return lax.rem(self.z + k, self.nz)

    def down(self, k):
        return lax.rem(self.z + self.nz - k, self.nz)

    def device(self, z=None, y=None, x=None, c=None):
        z, y = self.z if z is None else z, self.y if y is None else y
        x, c = self.x if x is None else x, self.c if c is None else c
        return {"dp": z * 2 + y, "tensor": x * 2 + c}

    def block(self, z, y, x, c):
        return (x * 2 + c) * self.ndp + z * 2 + y

    def across(self, c, a, b):
        return flipped(self.y, c * a + (1 - c) * b), flipped(self.x, (1 - c) * a + c * b)

    def chip(self, c, a, b):
        y, x = self.across(c, a, b)
        return self.device(y=y, x=x)

    def bit_partner(self, b):
        size = 2**b
        return self.z + size * (1 - 2 * lax.rem(self.z // size, 2))

    def greet(self):
        others = [self.device(c=1 - self.c), self.device(x=1 - self.x)]
        others += [self.device(x=1 - self.x, c=1 - self.c), self.device(y=1 - self.y)]
        others += [self.device(z=self.up(k)) for k in range(1, self.nz)]
        barrier = pltpu.get_barrier_semaphore()
        for other in others:
            pl.semaphore_signal(barrier, inc=1, device_id=other, device_id_type=MESH)
        pl.semaphore_wait(barrier, len(others))


def remote(src, dst, send_sem, recv_sem, device):
    return pltpu.make_async_remote_copy(
        src_ref=src,
        dst_ref=dst,
        send_sem=send_sem,
        recv_sem=recv_sem,
        device_id=device,
        device_id_type=MESH,
    )


class Gather:
    def __init__(self, place, slabs, outs, scratch):
        count = len(slabs)
        self.place, self.slabs, self.outs, self.count = place, slabs, outs, count
        self.lows = scratch[:count]
        self.send_sem, self.recv_sem, self.local_sem = scratch[count:]

    @staticmethod
    def scratch(shapes, n):
        messages = len(shapes) * (n - 1)
        return [pltpu.VMEM(s, BF16) for s in shapes] + [
            pltpu.SemaphoreType.DMA((messages,)),
            pltpu.SemaphoreType.DMA((messages,)),
            pltpu.SemaphoreType.DMA((len(shapes),)),
        ]

    def copy(self, stage, m, a, b, k):
        place, nz = self.place, self.place.nz
        order = 1 - place.c
        base = {"z": -1, "p": nz - 1, "q": 2 * nz - 1, "c": 4 * nz - 1}[stage]
        at = m * (8 * nz - 1) + base + (b * 2 + a) * nz + k
        y, x = place.across(order, a, b)
        where = place.block(place.down(k), y, x, place.c)
        device = {
            "p": lambda: place.chip(order, 1, 0),
            "q": lambda: place.chip(order, 0, 1),
            "c": lambda: place.device(c=1 - place.c),
            "z": lambda: place.device(z=place.up(k)),
        }[stage]()
        if stage == "z":
            where = place.block(place.z, place.y, place.x, place.c)
        mine = stage == "z" or (a, b, k) == (0, 0, 0)
        src = self.lows[m] if mine else self.outs[m].at[where]
        return remote(src, self.outs[m].at[where], self.send_sem.at[at], self.recv_sem.at[at], device)

    def local(self, m):
        place = self.place
        where = place.block(place.z, place.y, place.x, place.c)
        return pltpu.make_async_copy(self.lows[m], self.outs[m].at[where], self.local_sem.at[m])

    def send(self, stage, a, b, k):
        for m in range(self.count):
            self.copy(stage, m, a, b, k).start()

    def wait(self, stage, a, b, k):
        for m in range(self.count):
            self.copy(stage, m, a, b, k).wait_recv()

    def column(self, k):
        if k:
            self.wait("z", 0, 0, k)
        self.send("p", 0, 0, k)
        self.send("q", 0, 0, k)
        self.send("c", 0, 0, k)

    def first(self, k):
        self.wait("p", 0, 0, k)
        self.send("q", 1, 0, k)
        self.send("c", 1, 0, k)

    def second(self, a, k):
        self.wait("q", a, 0, k)
        self.send("c", a, 1, k)

    def round(self):
        return range(self.place.nz)

    def begin(self):
        for slab, low in zip(self.slabs, self.lows):
            low[...] = slab[...].astype(BF16)
        for m in range(self.count):
            self.local(m).start()
        for k in self.round()[1:]:
            self.send("z", 0, 0, k)
        self.column(0)

    def end(self):
        everything = [("z", 0, 0, k) for k in self.round()[1:]]
        everything += [("p", 0, 0, k) for k in self.round()]
        everything += [("q", a, 0, k) for a in range(2) for k in self.round()]
        last = [("c", a, b, k) for b in range(2) for a in range(2) for k in self.round()]
        for key in last:
            self.wait(*key)
        for m in range(self.count):
            self.local(m).wait()
            for stage, a, b, k in everything + last:
                self.copy(stage, m, a, b, k).wait_send()

    def at_once(self):
        self.place.greet()
        self.begin()
        for k in self.round()[1:]:
            self.column(k)
            self.first(k - 1)
        self.first(self.place.nz - 1)
        for a in range(2):
            for k in self.round():
                self.second(a, k)
        self.end()


class Reduce:
    def __init__(self, place, grads, scratch):
        count = len(grads)
        self.place, self.grads, self.count = place, grads, count
        self.own, self.from_core, self.from_p, self.from_q, self.from_z = (
            scratch[i * count : (i + 1) * count] for i in range(5)
        )
        self.send_sem, self.recv_sem, self.local_sem = scratch[5 * count :]

    @staticmethod
    def scratch(rows, n):
        nz, count = n // 8, len(rows)
        shapes = []
        for lead in ((2, 2, nz), (2, 2, nz), (2, nz), (nz,), (nz - 1,)):
            shapes += [pltpu.VMEM(lead + (r, D), BF16) for r in rows]
        return shapes + [
            pltpu.SemaphoreType.DMA((count * (8 * nz - 1),)),
            pltpu.SemaphoreType.DMA((count * (8 * nz - 1),)),
            pltpu.SemaphoreType.DMA((count * 4 * nz,)),
        ]

    def ks(self):
        return list(range(1, self.place.nz)) + [0]

    def copy(self, stage, m, a, b, k):
        place, nz = self.place, self.place.nz
        base = {"c": 0, "p": 4 * nz, "q": 6 * nz, "z": 7 * nz - 1}[stage]
        at = m * (8 * nz - 1) + base + {"c": (a * 2 + b) * nz + k, "p": b * nz + k}.get(stage, k)
        sems = self.send_sem.at[at], self.recv_sem.at[at]
        if stage == "c":
            y, x = place.across(1 - place.c, a, b)
            where = place.block(place.up(k), y, x, 1 - place.c)
            return remote(
                self.grads[m].at[where], self.from_core[m].at[a, b, k], *sems, place.device(c=1 - place.c)
            )
        src = self.own[m].at[a, b, k]
        if stage == "p":
            return remote(src, self.from_p[m].at[b, k], *sems, place.chip(place.c, 1, 0))
        if stage == "q":
            return remote(src, self.from_q[m].at[k], *sems, place.chip(place.c, 0, 1))
        return remote(src, self.from_z[m].at[k - 1], *sems, place.device(z=place.up(k)))

    def local(self, m, a, b, k):
        place, nz = self.place, self.place.nz
        y, x = place.across(place.c, a, b)
        where = place.block(place.up(k), y, x, place.c)
        at = m * 4 * nz + (a * 2 + b) * nz + k
        return pltpu.make_async_copy(
            self.grads[m].at[where], self.own[m].at[a, b, k], self.local_sem.at[at]
        )

    def order(self):
        return [(a, b, k) for a in (1, 0) for b in (1, 0) for k in self.ks()]

    def begin(self):
        for a, b, k in self.order():
            for m in range(self.count):
                self.copy("c", m, a, b, k).start()
        for a, b, k in self.order():
            for m in range(self.count):
                self.local(m, a, b, k).start()

    def value(self, m, a, b, k):
        self.local(m, a, b, k).wait()
        self.copy("c", m, a, b, k).wait_recv()
        value = self.own[m][a, b, k].astype(F32) + self.from_core[m][a, b, k].astype(F32)
        if a == 0:
            self.copy("p", m, 1, b, k).wait_recv()
            value = value + self.from_p[m][b, k].astype(F32)
            if b == 0:
                self.copy("q", m, 0, 1, k).wait_recv()
                value = value + self.from_q[m][k].astype(F32)
        return value

    def pass_on(self, a, b, between=None):
        stage = "p" if a else "q" if b else "z"
        waiting = []
        for k in self.ks():
            if stage == "z" and k == 0:
                continue
            for m in range(self.count):
                self.own[m][a, b, k] = self.value(m, a, b, k).astype(BF16)
            for copy in waiting:
                copy.start()
            waiting = [self.copy(stage, m, a, b, k) for m in range(self.count)]
        if between is not None:
            between()
        for copy in waiting:
            copy.start()

    def totals(self):
        values = [self.value(m, 0, 0, 0) for m in range(self.count)]
        for m in range(self.count):
            for k in self.ks()[:-1]:
                self.copy("z", m, 0, 0, k).wait_recv()
                values[m] = values[m] + self.from_z[m][k - 1].astype(F32)
        return values

    def end(self):
        for m in range(self.count):
            for a, b, k in self.order():
                self.copy("c", m, a, b, k).wait_send()
                if a:
                    self.copy("p", m, a, b, k).wait_send()
                elif b:
                    self.copy("q", m, a, b, k).wait_send()
                elif k:
                    self.copy("z", m, a, b, k).wait_send()


class Share:
    def __init__(self, place, core, fresh, bundle, scratch):
        self.place, self.core, self.fresh, self.bundle = place, core, fresh, bundle
        self.send_sem, self.recv_sem, self.near_sem = scratch

    @staticmethod
    def scratch(n, nt):
        messages = 2 + (nt - 1) + (n // 8 - 1) + n // 8
        return [
            pltpu.SemaphoreType.DMA((messages,)),
            pltpu.SemaphoreType.DMA((messages,)),
            pltpu.SemaphoreType.DMA,
        ]

    def near(self, i):
        place = self.place
        return pltpu.make_async_copy(self.fresh.at[i], self.bundle.at[place.dp, place.t], self.near_sem)

    def handed(self, i, label):
        place = self.place
        to = self.core + 2 * i
        return remote(
            self.fresh.at[i],
            self.bundle.at[place.dp, place.t],
            self.send_sem.at[i],
            self.recv_sem.at[label],
            {"dp": place.dp, "tensor": to},
        )

    def each(self, then):
        for i in range(2):
            to = self.core + 2 * i

            @pl.when(self.place.t != to)
            def _(i=i, to=to):
                then(self.handed(i, lax.rem(self.place.t + self.place.nt - to, self.place.nt) - 1))

    def hand(self):
        self.each(lambda copy: copy.start())
        for i in range(2):

            @pl.when(self.place.t == self.core + 2 * i)
            def _(i=i):
                self.near(i).start()

    def move(self, stage, k):
        place, nz = self.place, self.place.nz
        at = self.place.nt - 1 + (k - 1 if stage == "z" else nz - 1 + k)
        sems = self.send_sem.at[2 + at], self.recv_sem.at[at]
        if stage == "z":
            where, device = place.dp, place.device(z=place.up(k))
        else:
            where, device = place.down(k) * 2 + place.y, place.device(y=1 - place.y)
        return remote(self.bundle.at[where], self.bundle.at[where], *sems, device)

    def mine(self):
        return pl.when(self.place.c == self.core)

    def along_z(self):
        @self.mine()
        def _():
            self.near(0).wait()
            for label in range(self.place.nt - 1):
                self.handed(0, label).wait_recv()
            for k in range(1, self.place.nz):
                self.move("z", k).start()
            self.move("y", 0).start()

    def along_y(self):
        @self.mine()
        def _():
            for k in range(1, self.place.nz):
                self.move("z", k).wait_recv()
                self.move("y", k).start()

    def end(self):
        self.each(lambda copy: copy.wait_send())

        @self.mine()
        def _():
            for k in range(self.place.nz):
                self.move("y", k).wait_recv()
            for k in range(self.place.nz):
                self.move("y", k).wait_send()
                if k:
                    self.move("z", k).wait_send()


def renew(totals, momenta, grad_out, fresh, images):
    values = []
    for total, momentum, out in zip(totals, momenta, grad_out):
        grad = total / images
        out[...] = grad
        values.append(MOMENTUM * momentum[...] + grad)
    for value, ref in zip(values, fresh):
        ref[0 : value.shape[0], :] = value.astype(BF16)


def gather_kernel(ndp, nt, count, *refs):
    Gather(Place(ndp, nt), refs[:count], refs[count : 2 * count], refs[2 * count :]).at_once()


def gather_weights(slabs, ndp, nt, collective_id):
    count, n = len(slabs), ndp * nt
    gathered = pl.pallas_call(
        functools.partial(gather_kernel, ndp, nt, count),
        out_shape=tuple(shape_of((n,) + s.shape, BF16) for s in slabs),
        in_specs=[pl.BlockSpec(memory_space=pltpu.VMEM)] * count,
        out_specs=tuple(pl.BlockSpec(memory_space=pl.ANY) for _ in slabs),
        scratch_shapes=Gather.scratch([s.shape for s in slabs], n),
        compiler_params=pltpu.CompilerParams(
            collective_id=collective_id, has_side_effects=True, vmem_limit_bytes=VMEM_LIMIT
        ),
        name="gather_weights",
    )(*slabs)
    return tuple(g.reshape(n * s.shape[0], D) for g, s in zip(gathered, slabs))


SMALL_ROWS = 32
TABLE_ROW = 16


class SmallSum:
    def __init__(self, place, values, arrived, send_sem, recv_sem):
        self.values, self.arrived = values, arrived
        self.send_sem, self.recv_sem = send_sem, recv_sem
        self.steps = [
            place.device(c=1 - place.c),
            place.device(x=1 - place.x),
            place.device(y=1 - place.y),
        ]
        bit = 0
        while 2**bit < place.nz:
            self.steps.append(place.device(z=place.bit_partner(bit)))
            bit += 1
        self.done = 0

    def copy(self, i):
        return remote(
            self.values.at[i], self.arrived.at[i], self.send_sem.at[i], self.recv_sem.at[i], self.steps[i]
        )

    def begin(self):
        self.copy(0).start()

    def step(self):
        i = self.done
        if i < len(self.steps):
            self.copy(i).wait_recv()
            self.values[i + 1] = self.values[i] + self.arrived[i]
            self.done += 1

    def go_on(self):
        if 0 < self.done < len(self.steps):
            self.copy(self.done).start()

    def end(self):
        while self.done < len(self.steps):
            self.step()
            self.go_on()
        for i in range(len(self.steps)):
            self.copy(i).wait_send()
        return self.values[len(self.steps)]


def padded(rows):
    return -(-max(rows) // 16) * 16


def pack_small(small, sums1, sums2, head, hidden, table):
    small[0] = jnp.zeros_like(small[0])
    small[0, 0:1, :] = sums1[0:1, :]
    small[0, 1:2, :] = sums2[0:1, :]
    small[0, 2:3, :] = sums1[1:2, :]
    small[0, 3:6, :] = sums2[1:4, :]
    small[0, 6:8, :] = head[...]
    for i in range(hidden.shape[1] // D):
        small[0, 8 + i : 9 + i, :] = hidden[0:1, i * D : (i + 1) * D]
    small[0, TABLE_ROW : TABLE_ROW + table.shape[0], 0 : table.shape[1]] = table[...]


def newton_schulz_kernel(nt, heights, first_ref, second_ref, landed0, landed1, g_scr, x_scr, a_scr, y_scr, back, sem, send_sem, recv_sem):
    first, second, third = QUINTIC
    chunk = 512
    t, dp = lax.axis_index("tensor"), lax.axis_index("dp")
    core = t % 2
    sources = (first_ref, second_ref)
    landed = (landed0, landed1)
    barrier = pltpu.get_barrier_semaphore()
    for d in range(1, nt):
        other = {"dp": dp, "tensor": lax.rem(t + d, nt)}
        pl.semaphore_signal(barrier, inc=1, device_id=other, device_id_type=MESH)
    for which, ref in enumerate(sources):

        @pl.when(core == which)
        def _(ref=ref):
            copy = pltpu.make_async_copy(ref, g_scr.at[0 : ref.shape[0]], sem)
            copy.start()
            copy.wait()

    chunks = jnp.where(core == 0, first_ref.shape[0] // chunk, second_ref.shape[0] // chunk)

    def low(values):
        return values.astype(BF16)

    def gram(src_ref):
        a_scr[...] = jnp.zeros_like(a_scr)

        def add(at, carry):
            part = src_ref[pl.ds(pl.multiple_of(at * chunk, chunk), chunk), :]
            a_scr[...] += dot_tn(part, part)
            return carry

        lax.fori_loop(0, chunks, add, 0)
        return a_scr[...]

    def advance(src_ref, factor, scale):
        factor = low(factor)

        def step(at, carry):
            at = pl.ds(pl.multiple_of(at * chunk, chunk), chunk)
            x_scr[at, :] = low(dot_nn(src_ref[at, :], factor) * scale)
            return carry

        lax.fori_loop(0, chunks, step, 0)

    def bend(a):
        return second * a + third * dot_nn(low(a), low(a))

    diagonal = lax.broadcasted_iota(jnp.int32, (D, D), 0) == lax.broadcasted_iota(jnp.int32, (D, D), 1)

    def two_turns(a):
        b = bend(a)
        q = b + jnp.where(diagonal, first, 0.0)
        r = first * a + dot_nn(low(a), low(b))
        a = first * r + dot_nn(low(r), low(b))
        b = bend(a)
        return first * q + dot_nn(low(b), low(q))

    a = gram(g_scr)
    scale = 1.0 / (jnp.sqrt(jnp.sum(jnp.where(diagonal, a, 0.0))) + MUON_EPSILON)
    advance(g_scr, two_turns(a * scale * scale), scale)
    q = two_turns(gram(x_scr))
    for which, ref in enumerate(sources):

        @pl.when(core == which)
        def _(ref=ref):
            mine = nt * heights[which]
            at = pl.ds(pl.multiple_of(dp * mine, mine), mine)
            y_scr[0:mine, :] = dot_nn(x_scr[at, :], low(q))

    advance(x_scr, q, 1.0)
    b = bend(gram(x_scr))
    here = y_scr[...]
    back[...] = low(first * here + dot_nn(low(here), low(b)))
    pl.semaphore_wait(barrier, nt - 1)

    def copy(which, d):
        to = lax.rem(t + d, nt)
        height = heights[which]
        return remote(
            back.at[pl.ds(pl.multiple_of(to * height, height), height)],
            landed[which].at[t // 2],
            send_sem.at[d - 1],
            recv_sem.at[d - 1],
            {"dp": dp, "tensor": to},
        )

    for which in range(2):

        @pl.when(core == which)
        def _(which=which):
            for d in range(1, nt):
                copy(which, d).start()
            height = heights[which]
            landed[which][t // 2] = back[pl.ds(pl.multiple_of(t * height, height), height), :]

    for d in range(1, nt):
        for which in range(2):

            @pl.when(lax.rem(t + nt - d, nt) % 2 == which)
            def _(d=d, which=which):
                copy(which, d).wait_recv()

    for which in range(2):

        @pl.when(core == which)
        def _(which=which):
            for d in range(1, nt):
                copy(which, d).wait_send()


def newton_schulz(bundles, collective_id):
    ndp, nt = bundles[0].shape[:2]
    heights = tuple(b.shape[2] for b in bundles)
    rows = [ndp * nt * h for h in heights]
    tall = max(rows)
    any_, vmem = pl.BlockSpec(memory_space=pl.ANY), pl.BlockSpec(memory_space=pltpu.VMEM)
    return pl.pallas_call(
        functools.partial(newton_schulz_kernel, nt, heights),
        out_shape=tuple(shape_of((nt // 2, h, D), BF16) for h in heights),
        in_specs=[any_, any_],
        out_specs=(vmem, vmem),
        scratch_shapes=[
            pltpu.VMEM((tall, D), BF16),
            pltpu.VMEM((tall, D), BF16),
            pltpu.VMEM((D, D), F32),
            pltpu.VMEM((tall // ndp, D), F32),
            pltpu.VMEM((tall // ndp, D), BF16),
            pltpu.SemaphoreType.DMA,
            pltpu.SemaphoreType.DMA((nt - 1,)),
            pltpu.SemaphoreType.DMA((nt - 1,)),
        ],
        compiler_params=pltpu.CompilerParams(
            collective_id=collective_id, has_side_effects=True, vmem_limit_bytes=VMEM_LIMIT
        ),
        name="newton_schulz",
    )(*(b.reshape(r, D) for b, r in zip(bundles, rows)))


def finish_kernel(nt, rates, *refs):
    refs = list(refs)

    def take(n):
        taken = refs[:n]
        del refs[:n]
        return taken

    landed, (total,) = take(2), take(1)
    grads, momenta, weights = take(nt), take(nt), take(nt)
    small_par, small_mom = take(5), take(5)
    grad_out, new_out, mom_out = take(nt), take(nt), take(nt)
    small_grad_out, small_new_out, small_mom_out = take(5), take(5), take(5)
    for m in range(nt):
        grad = grads[m][...]
        grad_out[m][...] = grad
        mom_out[m][...] = MOMENTUM * momenta[m][...] + grad
        new_out[m][...] = weights[m][...] - rates[m] * landed[m % 2][m // 2, 0 : grad.shape[0], :].astype(F32)

    def small_update(i, at, grad):
        small_grad_out[i][at] = grad
        grad = MOMENTUM * small_mom[i][at] + grad
        small_mom_out[i][at] = grad
        small_new_out[i][at] = small_par[i][at] - VECTOR_RATE * grad

    for i, (low, high) in enumerate(((0, 2), (2, 6), (6, 8))):
        small_update(i, (slice(None), slice(None)), total[low:high, :])
    for i in range(small_par[3].shape[1] // D):
        small_update(3, (slice(0, 1), slice(i * D, (i + 1) * D)), total[8 + i : 9 + i, :])
    heads, rows = small_par[4].shape
    small_update(4, (slice(None), slice(None)), total[TABLE_ROW : TABLE_ROW + heads, 0:rows])


def finish(landed, total, grads, momenta, weights, small_params, small_moms, rates):
    nt = len(grads)
    like = lambda arrays: tuple(shape_of(a.shape, F32) for a in arrays)
    return pl.pallas_call(
        functools.partial(finish_kernel, nt, rates),
        out_shape=like(grads) * 3 + like(small_params) * 3,
        compiler_params=pltpu.CompilerParams(vmem_limit_bytes=VMEM_LIMIT),
        name="finish",
    )(*landed, total, *grads, *momenta, *weights, *small_params, *small_moms)


def key_by_query(index_ref, idx_scr):
    idx_scr[...] = jnp.zeros_like(idx_scr)
    idx_scr[0:SPOTS, 0:SPOTS] = index_ref[...].astype(F32)
    index = idx_scr[...].T[0:SLOT, :]
    return jnp.where(lane_iota(SLOT) < SLOT, index, pltpu.roll(index, SLOT, 1))


def table_sums(dbias_ref, index_ref, table_scr, idx_scr, turned_idx):
    turned_idx[...] = key_by_query(index_ref, idx_scr)
    table_scr[...] = jnp.zeros_like(table_scr)
    lanes = lane_iota(PAIRS)
    entries = lax.broadcasted_iota(jnp.int32, (2 * LANES, LANES), 0).astype(F32)
    count = OCTS * OCT

    def one_key(key, carry):
        picks = (entries == turned_idx[pl.ds(key, 1), :]).astype(F32).astype(BF16)
        values = []
        for octet in range(OCTS):
            pairs = dbias_ref[octet, pl.ds(key, PAIRS, SLOT), :]
            values += [jnp.where(lanes < SLOT, pairs, 0.0), jnp.where(lanes < SLOT, 0.0, pairs)]
        values = jnp.concatenate(values, axis=0)
        parts = []
        for _ in range(3):
            low = values.astype(BF16).astype(F32)
            parts.append(low)
            values = values - low
        sums = dot_nt(jnp.concatenate(parts, axis=0).astype(BF16), picks)
        table_scr[...] += sums[0:count] + sums[count : 2 * count] + sums[2 * count :]
        return carry

    lax.fori_loop(0, SPOTS, one_key, 0)
    sums = table_scr[...]
    for octet in range(OCTS):
        for head in range(OCT):
            at = octet * OCT + head % 2 * PAIRS + head // 2
            table_scr[octet * OCT + head : octet * OCT + head + 1, :] = sums[at : at + 1]


def attention_forward_kernel(ndp, nt, steps, fused, *refs):
    refs = list(refs)

    def take(n):
        taken = refs[:n]
        del refs[:n]
        return taken

    x_ref, gain_ref, shift_ref, qkvb_ref, table_ref, index_ref, region_ref = take(7)
    slabs, (wqkv_in,) = take(3), take(1)
    xs_ref, a1_ref, qkv_ref, p_ref, o_ref = take(5)
    gathered = take(3)
    wqkv_all = take(1) if fused else None
    bias_scr, idx_scr, tab_scr, pair_scr, side_scr, a1_scr = take(6)
    place = Place(ndp, nt)
    rest = Gather(place, slabs, gathered, take(6))
    step, last = pl.program_id(0), pl.num_programs(0) - 1
    if fused:
        qkv_gather = Gather(place, (wqkv_in,), wqkv_all, take(4))
        wqkv_ref, load_sem = take(2)
    else:
        wqkv_ref = wqkv_in

    @pl.when(step == 0)
    def _():
        place.greet()
        if fused:
            qkv_gather.begin()

    @pl.when(step < steps)
    def _():
        xs_ref[...] = jnp.zeros_like(xs_ref)
        into_slots(x_ref, xs_ref)
        white, _ = whiten(xs_ref[...])
        a1 = (white * gain_ref[0:1, :] + shift_ref[0:1, :]).astype(BF16)
        a1_ref[...] = a1
        a1_scr[pl.ds(pl.multiple_of(step * STEP_SLOTS, STEP_SLOTS), STEP_SLOTS), :] = a1

    @pl.when(step == 0)
    def _():
        if fused:
            for k in qkv_gather.round()[1:]:
                qkv_gather.column(k)
        build_bias(region_ref, index_ref, table_ref, bias_scr, idx_scr, tab_scr)
        pair_scr[...] = pair_mask()
        side_scr[...] = side_mask()

    if fused:

        @pl.when(step == 1)
        def _():
            for k in qkv_gather.round():
                qkv_gather.first(k)

        @pl.when(step == 2)
        def _():
            for a in range(2):
                for k in qkv_gather.round():
                    qkv_gather.second(a, k)

    @pl.when(step == 2)
    def _():
        rest.begin()

    @pl.when(step == steps - 1)
    def _():
        if fused:
            qkv_gather.end()
            copies = []
            for i in range(ndp * nt):
                rows = wqkv_in.shape[0]
                copies.append(
                    pltpu.make_async_copy(
                        wqkv_all[0].at[i], wqkv_ref.at[i * rows : (i + 1) * rows], load_sem.at[i]
                    )
                )
                copies[i].start()
            for copy in copies:
                copy.wait()

    @pl.when(step >= steps)
    def _():
        at = pl.multiple_of((step - steps) * STEP_SLOTS, STEP_SLOTS)
        a1 = a1_scr[pl.ds(at, STEP_SLOTS), :]
        scale = HEAD ** (-0.5)
        for half in range(2):
            columns = 3 * PART * GROUPS // 2
            u = dot_nt(a1, wqkv_ref[half * columns : (half + 1) * columns, :])
            for inner in range(GROUPS // 2):
                group = half * (GROUPS // 2) + inner
                for part in range(3):
                    piece = u[:, (inner * 3 + part) * PART : (inner * 3 + part + 1) * PART]
                    if part == 0:
                        piece = (piece + qkvb_ref[0:1, group * PART : (group + 1) * PART]) * scale
                    elif part == 2:
                        piece = piece + qkvb_ref[1:2, group * PART : (group + 1) * PART]
                    lanes = part * D + group * PART
                    qkv_ref[:, lanes : lanes + PART] = piece.astype(BF16)

    real_query = (lane_iota(1) % SLOT < SPOTS).astype(F32)
    first_side = lax.broadcasted_iota(jnp.int32, (SLOT, OCT_W), 1) // HEAD % 2 == 0

    def one_window(at, carry):
        rows = pl.ds(pl.multiple_of(at * SLOT, SLOT), SLOT)
        for octet in range(OCTS):
            q = qkv_ref[rows, octet * OCT_W : (octet + 1) * OCT_W]
            k = qkv_ref[rows, D + octet * OCT_W : D + (octet + 1) * OCT_W]
            v = qkv_ref[rows, 2 * D + octet * OCT_W : 2 * D + (octet + 1) * OCT_W]
            scores = dot_nt(spread(k, pair_scr), spread(q, side_scr)) + bias_scr[lax.rem(at, WINDOWS), octet]
            probs = []
            for pair in range(PAIRS):
                part = scores[pair * SLOT : (pair + 1) * SLOT]
                grown = jnp.exp(part - jnp.max(part, axis=0, keepdims=True))
                probs.append(grown * (real_query / jnp.sum(grown, axis=0, keepdims=True)))
            probs = jnp.concatenate(probs, axis=0)
            p_ref[pl.ds(pl.multiple_of((at * OCTS + octet) * ROWS_S, ROWS_S), ROWS_S), :] = probs.astype(BF16)
            mixed = dot_nn(turned(probs).astype(BF16), spread(v, pair_scr))
            o_ref[rows, octet * OCT_W : (octet + 1) * OCT_W] = by_side(mixed, first_side).astype(BF16)
        return carry

    half_loop = STEP_IMAGES * WINDOWS // 2

    @pl.when(step >= steps)
    def _():
        lax.fori_loop(0, half_loop, one_window, 0, unroll=4)

    @pl.when(step == steps + 1)
    def _():
        for k in rest.round()[1:]:
            rest.column(k)

    @pl.when(step == steps + 2)
    def _():
        for k in rest.round():
            rest.first(k)

    @pl.when(step == last)
    def _():
        for a in range(2):
            for k in rest.round():
                rest.second(a, k)

    @pl.when(step >= steps)
    def _():
        lax.fori_loop(half_loop, 2 * half_loop, one_window, 0, unroll=4)

    @pl.when(step == last)
    def _():
        rest.end()


def mlp_kernel(
    xs_ref,
    o_ref,
    e_ref,
    wproj_ref,
    w1_ref,
    w2_ref,
    gain_ref,
    shift_ref,
    hb_ref,
    out_ref,
    dy_ref,
    g1_ref,
    g2_ref,
    gproj_ref,
    hsum_ref,
    sums_ref,
    acc1,
    acc2,
    accp,
    m_scr,
    da_scr,
    a2_scr,
    e_scr,
    slot_scr,
    y_ref,
):
    step = pl.program_id(0)

    @pl.when(step == 0)
    def _():
        acc1[...] = jnp.zeros_like(acc1)
        acc2[...] = jnp.zeros_like(acc2)
        accp[...] = jnp.zeros_like(accp)
        hsum_ref[...] = jnp.zeros_like(hsum_ref)
        sums_ref[...] = jnp.zeros_like(sums_ref)

    slot_scr[...] = xs_ref[...] + dot_nn(o_ref[...], wproj_ref[...]) + shift_ref[2:3, :]
    out_of_slots(slot_scr, y_ref)
    white, inverse = whiten(y_ref[...])
    a2_scr[...] = (white * gain_ref[1:2, :] + shift_ref[1:2, :]).astype(BF16)
    e_scr[...] = e_ref[...].astype(BF16)
    m_scr[...] = jnp.zeros_like(m_scr)
    da_scr[...] = jnp.zeros_like(da_scr)
    root = math.sqrt(2.0 / math.pi)
    width = 512

    def chunk(c, carry):
        at = pl.ds(pl.multiple_of(c * width, width), width)
        w1, w2 = w1_ref[at, :], w2_ref[at, :]
        a2, e = a2_scr[...], e_scr[...]
        z = dot_nt(a2, w1) + hb_ref[0:1, at]
        square = z * z
        t = jnp.tanh(z * (root + (root * 0.044715) * square))
        half = 0.5 * z
        f = (half + half * t).astype(BF16)
        slope = 0.5 + 0.5 * t + half * (1.0 - t * t) * (root + (3.0 * root * 0.044715) * square)
        dz = dot_nt(e, w2) * slope
        hsum_ref[0:1, at] += jnp.sum(dz, axis=0, keepdims=True)
        dz = dz.astype(BF16)
        m_scr[...] += dot_nn(f, w2)
        da_scr[...] += dot_nn(dz, w1)
        acc2[at, :] += dot_tn(f, e)
        acc1[at, :] += dot_tn(dz, a2)
        return carry

    lax.fori_loop(0, w1_ref.shape[0] // width, chunk, 0)
    white, inverse = whiten(y_ref[...])
    out_ref[...] = y_ref[...] + m_scr[...] + shift_ref[3:4, :]
    da = da_scr[...]
    t2 = da * gain_ref[1:2, :]
    dy = e_ref[...] + inverse * (t2 - row_mean(t2) - white * row_mean(t2 * white))
    m_scr[...] = dy
    dy_ref[...] = jnp.zeros_like(dy_ref)
    into_slots(m_scr, dy_ref)
    accp[...] += dot_tn(o_ref[...], dy_ref[...].astype(BF16))
    sums_ref[0:1, :] += jnp.sum(da * white, axis=0, keepdims=True)
    sums_ref[1:2, :] += jnp.sum(da, axis=0, keepdims=True)
    sums_ref[2:3, :] += jnp.sum(dy, axis=0, keepdims=True)
    sums_ref[3:4, :] += jnp.sum(e_ref[...], axis=0, keepdims=True)

    @pl.when(step == pl.num_programs(0) - 1)
    def _():
        g1_ref[...] = acc1[...].astype(BF16)
        g2_ref[...] = acc2[...].astype(BF16)
        gproj_ref[...] = accp[...].astype(BF16)


def attention_backward_kernel(ndp, nt, images, steps, *refs):
    refs = list(refs)

    def take(n):
        taken = refs[:n]
        del refs[:n]
        return taken

    dy_ref, xs_ref, a1_ref, qkv_ref, p_ref, wqkv_ref, wproj_ref, gain_ref, index_ref = take(9)
    hidden_ref, sums2_ref = take(2)
    grads, momenta, (qkv_momentum,) = take(3), take(3), take(1)
    (gin_ref,) = take(1)
    slabs, (qkv_slab,) = take(3), take(1)
    bundle0, bundle1, small_out = take(3)
    accq, gq, do_scr, du_scr, pair_scr, side_scr, g_scr, dbias_ref, hsum_ref, sums_ref = take(10)
    idx_scr, turned_idx, table_scr, fresh0, fresh1 = take(5)
    small, small_in, small_send, small_recv = take(4)
    place = Place(ndp, nt)
    step, last = pl.program_id(0), pl.num_programs(0) - 1
    share0 = Share(place, 0, fresh0, bundle0, take(3))
    share1 = Share(place, 1, fresh1, bundle1, take(3))
    early = Reduce(place, grads, take(18))
    late = Reduce(place, (gq,), take(8))
    tiny = SmallSum(place, small, small_in, small_send, small_recv)

    @pl.when(step == 0)
    def _():
        place.greet()
        early.begin()
        fresh0[...] = jnp.zeros_like(fresh0)
        fresh1[...] = jnp.zeros_like(fresh1)
        pair_scr[...] = pair_mask()
        side_scr[...] = side_mask()
        accq[...] = jnp.zeros_like(accq)
        dbias_ref[...] = jnp.zeros_like(dbias_ref)
        hsum_ref[...] = jnp.zeros_like(hsum_ref)
        sums_ref[...] = jnp.zeros_like(sums_ref)

    first_row = pl.multiple_of(lax.rem(step, steps) * STEP_SLOTS, STEP_SLOTS)
    step_rows = pl.ds(first_row, STEP_SLOTS)

    @pl.when(step < steps)
    def _():
        do_scr[...] = dot_nt(dy_ref[...].astype(BF16), wproj_ref[...]).astype(BF16)

    scale = HEAD ** (-0.5)
    first_side = lax.broadcasted_iota(jnp.int32, (SLOT, OCT_W), 1) // HEAD % 2 == 0

    def one_window(at, carry):
        rows = pl.ds(pl.multiple_of(at * SLOT, SLOT), SLOT)
        out_rows = pl.ds(pl.multiple_of(first_row + at * SLOT, SLOT), SLOT)
        for octet in range(OCTS):
            q = qkv_ref[rows, octet * OCT_W : (octet + 1) * OCT_W]
            k = qkv_ref[rows, D + octet * OCT_W : D + (octet + 1) * OCT_W]
            v = qkv_ref[rows, 2 * D + octet * OCT_W : 2 * D + (octet + 1) * OCT_W]
            do = do_scr[rows, octet * OCT_W : (octet + 1) * OCT_W]
            probs = p_ref[pl.ds(pl.multiple_of((at * OCTS + octet) * ROWS_S, ROWS_S), ROWS_S), :]
            side_do = spread(do, side_scr)
            weighted = probs.astype(F32) * dot_nt(spread(v, pair_scr), side_do)
            ds = []
            for pair in range(PAIRS):
                part = slice(pair * SLOT, (pair + 1) * SLOT)
                total = jnp.sum(weighted[part], axis=0, keepdims=True)
                ds.append(weighted[part] - probs[part].astype(F32) * total)
            ds = jnp.concatenate(ds, axis=0)
            dbias_ref[octet] += ds
            dq = by_side(dot_nn(turned(ds).astype(BF16), spread(k, pair_scr)), first_side) * scale
            dk = by_pair(ds.astype(BF16), spread(q, side_scr))
            dv = by_pair(probs, side_do)
            lanes = slice(octet * OCT_W, (octet + 1) * OCT_W)
            hsum_ref[0:1, lanes] += jnp.sum(dq, axis=0, keepdims=True)
            hsum_ref[1:2, lanes] += jnp.sum(dv, axis=0, keepdims=True)
            for part, grad in enumerate((dq, dk, dv)):
                for inner in range(OCT_W // PART):
                    group = octet * (OCT_W // PART) + inner
                    at_col = (group * 3 + part) * PART
                    du_scr[out_rows, at_col : at_col + PART] = grad[
                        :, inner * PART : (inner + 1) * PART
                    ].astype(BF16)
        return carry

    half_loop = STEP_IMAGES * WINDOWS // 2

    @pl.when(step < steps)
    def _():
        lax.fori_loop(0, half_loop, one_window, 0, unroll=4)

    @pl.when(step == 0)
    def _():
        early.pass_on(1, 1)
        early.pass_on(1, 0)

    @pl.when(step == 2)
    def _():
        early.pass_on(0, 0)

    @pl.when(step < steps)
    def _():
        lax.fori_loop(half_loop, 2 * half_loop, one_window, 0, unroll=4)

    @pl.when(step == 1)
    def _():
        early.pass_on(0, 1)

    @pl.when(step == steps - 1)
    def _():
        renew(early.totals(), momenta, slabs, (fresh0.at[1], fresh1.at[0], fresh1.at[1]), images)
        share1.hand()

    @pl.when(step < steps)
    def _():
        accq[...] += dot_tn(du_scr[step_rows, :], a1_ref[...])

    @pl.when(step == steps - 1)
    def _():
        rows = gq.shape[1]
        for i in range(gq.shape[0]):
            gq[i] = accq[i * rows : (i + 1) * rows, :].astype(BF16)
        share1.along_z()
        late.begin()

    @pl.when(step >= steps)
    def _():
        white, inverse = whiten(xs_ref[...])
        da = dot_nn(du_scr[step_rows, :], wqkv_ref[...])
        t1 = da * gain_ref[0:1, :]
        g_scr[...] = dy_ref[...] + inverse * (t1 - row_mean(t1) - white * row_mean(t1 * white))
        out_of_slots(g_scr, gin_ref)
        sums_ref[0:1, :] += jnp.sum(da * white, axis=0, keepdims=True)
        sums_ref[1:2, :] += jnp.sum(da, axis=0, keepdims=True)

    @pl.when(step == steps)
    def _():
        late.pass_on(1, 1)
        late.pass_on(1, 0)

    @pl.when(step == steps + 1)
    def _():
        table_sums(dbias_ref, index_ref, table_scr, idx_scr, turned_idx)
        share1.along_y()

    @pl.when(step == steps + 2)
    def _():
        late.pass_on(0, 1)

    @pl.when(step == last)
    def _():
        pack_small(small, sums_ref, sums2_ref, hsum_ref, hidden_ref, table_scr)
        late.pass_on(0, 0, tiny.begin)
        tiny.step()
        tiny.go_on()
        renew(late.totals(), (qkv_momentum,), (qkv_slab,), (fresh0.at[0],), images)
        tiny.step()
        share0.hand()
        tiny.go_on()
        tiny.step()
        tiny.go_on()
        share0.along_z()
        tiny.step()
        tiny.go_on()
        share0.along_y()
        small_out[...] = tiny.end() / images
        share1.end()
        share0.end()
        early.end()
        late.end()


def whole(shape):
    return pl.BlockSpec(shape, lambda i: (0,) * len(shape))


def rows_of(rows, columns):
    return pl.BlockSpec((rows, columns), lambda i: (i, 0))


def shape_of(shape, dtype):
    return jax.ShapeDtypeStruct(shape, dtype)


PARAMS = pltpu.CompilerParams(dimension_semantics=("arbitrary",), vmem_limit_bytes=VMEM_LIMIT)


def remote_params(collective_id):
    return pltpu.CompilerParams(
        dimension_semantics=("arbitrary",),
        vmem_limit_bytes=VMEM_LIMIT,
        collective_id=collective_id,
        has_side_effects=True,
    )


def attention_forward(
    tokens, gains, shifts, head_biases, table, index, regions, slabs, qkv_slab, ndp, nt, collective_ids
):
    n = ndp * nt
    steps = tokens.shape[0] // STEP_ROWS
    slots = steps * STEP_SLOTS
    fused = qkv_slab.shape[0] % 16 == 0
    if not fused:
        (qkv_slab,) = gather_weights((qkv_slab,), ndp, nt, collective_ids[1])
    early = lambda i: (jnp.minimum(i, steps - 1), 0)
    late = lambda i: (jnp.maximum(i - steps, 0), 0)
    any_ = pl.BlockSpec(memory_space=pl.ANY)
    gathered = tuple(slabs) + ((qkv_slab,) if fused else ())
    results = pl.pallas_call(
        functools.partial(attention_forward_kernel, ndp, nt, steps, fused),
        grid=(2 * steps,),
        out_shape=(
            shape_of((slots, D), F32),
            shape_of((slots, D), BF16),
            shape_of((slots, 3 * D), BF16),
            shape_of((slots * OCTS * PAIRS, LANES), BF16),
            shape_of((slots, D), BF16),
        )
        + tuple(shape_of((n,) + s.shape, BF16) for s in gathered),
        in_specs=[
            pl.BlockSpec((STEP_ROWS, D), early),
            whole(gains.shape),
            whole(shifts.shape),
            whole(head_biases.shape),
            whole(table.shape),
            whole(index.shape),
            pl.BlockSpec(memory_space=pltpu.SMEM),
        ]
        + [whole(s.shape) for s in slabs]
        + [whole(qkv_slab.shape)],
        out_specs=(
            pl.BlockSpec((STEP_SLOTS, D), early),
            pl.BlockSpec((STEP_SLOTS, D), early),
            pl.BlockSpec((STEP_SLOTS, 3 * D), late),
            pl.BlockSpec((STEP_SLOTS * OCTS * PAIRS, LANES), late),
            pl.BlockSpec((STEP_SLOTS, D), late),
        )
        + (any_,) * len(gathered),
        scratch_shapes=[
            pltpu.VMEM((WINDOWS, OCTS, ROWS_S, LANES), F32),
            pltpu.VMEM((LANES, LANES), F32),
            pltpu.VMEM((HEADS, 2 * LANES), F32),
            pltpu.VMEM((ROWS_S, OCT_W), BF16),
            pltpu.VMEM((2 * SLOT, OCT_W), BF16),
            pltpu.VMEM((slots, D), BF16),
        ]
        + Gather.scratch([s.shape for s in slabs], n)
        + (
            Gather.scratch([qkv_slab.shape], n)
            + [pltpu.VMEM((n * qkv_slab.shape[0], D), BF16), pltpu.SemaphoreType.DMA((n,))]
            if fused
            else []
        ),
        compiler_params=remote_params(collective_ids[0]),
        name="attention_forward",
    )(tokens, gains, shifts, head_biases, table, index, regions, *slabs, qkv_slab)
    weights = [g.reshape(-1, D) for g in results[5:]]
    if not fused:
        weights.append(qkv_slab)
    return results[:5], weights


def mlp(xs, mixed, out_grad, wproj, w1, w2, gains, shifts, hidden_bias):
    steps = out_grad.shape[0] // STEP_ROWS
    hidden = w1.shape[0]
    return pl.pallas_call(
        mlp_kernel,
        grid=(steps,),
        out_shape=(
            shape_of(out_grad.shape, F32),
            shape_of(xs.shape, F32),
            shape_of(w1.shape, BF16),
            shape_of(w2.shape, BF16),
            shape_of(wproj.shape, BF16),
            shape_of((1, hidden), F32),
            shape_of((4, D), F32),
        ),
        in_specs=[
            rows_of(STEP_SLOTS, D),
            rows_of(STEP_SLOTS, D),
            rows_of(STEP_ROWS, D),
            whole(wproj.shape),
            whole(w1.shape),
            whole(w2.shape),
            whole(gains.shape),
            whole(shifts.shape),
            whole((1, hidden)),
        ],
        out_specs=(
            rows_of(STEP_ROWS, D),
            rows_of(STEP_SLOTS, D),
            whole(w1.shape),
            whole(w2.shape),
            whole(wproj.shape),
            whole((1, hidden)),
            whole((4, D)),
        ),
        scratch_shapes=[
            pltpu.VMEM(w1.shape, F32),
            pltpu.VMEM(w2.shape, F32),
            pltpu.VMEM(wproj.shape, F32),
            pltpu.VMEM((STEP_ROWS, D), F32),
            pltpu.VMEM((STEP_ROWS, D), F32),
            pltpu.VMEM((STEP_ROWS, D), BF16),
            pltpu.VMEM((STEP_ROWS, D), BF16),
            pltpu.VMEM((STEP_SLOTS, D), F32),
            pltpu.VMEM((STEP_ROWS, D), F32),
        ],
        compiler_params=PARAMS,
        name="mlp",
    )(xs, mixed, out_grad, wproj, w1, w2, gains, shifts, hidden_bias.reshape(1, hidden))


def attention_backward(
    dy,
    xs,
    a1,
    qkv,
    probs,
    wqkv,
    wproj,
    gains,
    index,
    hidden_sum,
    sums2,
    grads,
    momenta,
    qkv_momentum,
    ndp,
    nt,
    images,
    collective_id,
):
    n = ndp * nt
    rows = [m.shape[0] for m in momenta]
    qkv_rows = qkv_momentum.shape[0]
    steps = dy.shape[0] // STEP_SLOTS
    grads = tuple(g.reshape(n, r, D) for g, r in zip(grads, rows))
    any_ = pl.BlockSpec(memory_space=pl.ANY)
    early = lambda i: (jnp.minimum(i, steps - 1), 0)
    late = lambda i: (jnp.maximum(i - steps, 0), 0)
    both = lambda i: (lax.rem(i, steps), 0)
    tall0, tall1 = padded((qkv_rows, rows[0])), padded(rows[1:])
    small_steps = 3 + (ndp // 2 - 1).bit_length()
    return pl.pallas_call(
        functools.partial(attention_backward_kernel, ndp, nt, images, steps),
        grid=(2 * steps,),
        out_shape=(shape_of((steps * STEP_ROWS, D), F32),)
        + tuple(shape_of((r, D), F32) for r in rows + [qkv_rows])
        + (
            shape_of((ndp, nt, tall0, D), BF16),
            shape_of((ndp, nt, tall1, D), BF16),
            shape_of((SMALL_ROWS, D), F32),
        ),
        in_specs=[
            pl.BlockSpec((STEP_SLOTS, D), both),
            pl.BlockSpec((STEP_SLOTS, D), late),
            pl.BlockSpec((STEP_SLOTS, D), early),
            pl.BlockSpec((STEP_SLOTS, 3 * D), early),
            pl.BlockSpec((STEP_SLOTS * OCTS * PAIRS, LANES), early),
            whole(wqkv.shape),
            whole(wproj.shape),
            whole(gains.shape),
            whole(index.shape),
            whole(hidden_sum.shape),
            whole(sums2.shape),
            any_,
            any_,
            any_,
        ]
        + [whole((r, D)) for r in rows + [qkv_rows]],
        out_specs=(pl.BlockSpec((STEP_ROWS, D), late),)
        + tuple(whole((r, D)) for r in rows + [qkv_rows])
        + (any_, any_, whole((SMALL_ROWS, D))),
        scratch_shapes=[
            pltpu.VMEM(wqkv.shape, F32),
            pltpu.VMEM((n, qkv_rows, D), BF16),
            pltpu.VMEM((STEP_SLOTS, D), BF16),
            pltpu.VMEM((steps * STEP_SLOTS, 3 * D), BF16),
            pltpu.VMEM((ROWS_S, OCT_W), BF16),
            pltpu.VMEM((2 * SLOT, OCT_W), BF16),
            pltpu.VMEM((STEP_SLOTS, D), F32),
            pltpu.VMEM((OCTS, ROWS_S, LANES), F32),
            pltpu.VMEM((2, D), F32),
            pltpu.VMEM((2, D), F32),
            pltpu.VMEM((LANES, LANES), F32),
            pltpu.VMEM((SLOT, LANES), F32),
            pltpu.VMEM((HEADS, 2 * LANES), F32),
            pltpu.VMEM((2, tall0, D), BF16),
            pltpu.VMEM((2, tall1, D), BF16),
            pltpu.VMEM((small_steps + 1, SMALL_ROWS, D), F32),
            pltpu.VMEM((small_steps, SMALL_ROWS, D), F32),
            pltpu.SemaphoreType.DMA((small_steps,)),
            pltpu.SemaphoreType.DMA((small_steps,)),
        ]
        + Share.scratch(n, nt)
        + Share.scratch(n, nt)
        + Reduce.scratch(rows, n)
        + Reduce.scratch([qkv_rows], n),
        compiler_params=remote_params(collective_id),
        name="attention_backward",
    )(
        dy,
        xs,
        a1,
        qkv,
        probs,
        wqkv,
        wproj,
        gains,
        index,
        hidden_sum,
        sums2,
        *grads,
        *momenta,
        qkv_momentum,
    )


ORDER = (0, 2, 1, 3)
WIDE = (True, True, False, False)
FACTORS = (
    math.sqrt(3.0),
    math.sqrt(max(1.0, FF / D)),
    1.0,
    math.sqrt(max(1.0, D / FF)),
)


def as_slab(block, wide):
    return block.reshape(D, -1).T if wide else block.reshape(-1, D)


def as_block(slab, like, wide):
    return (slab.T if wide else slab).reshape(like.shape)


def shards(
    tokens,
    out_grad,
    qkv_weight,
    proj_weight,
    fc1_weight,
    fc2_weight,
    qkv_momentum,
    proj_momentum,
    fc1_momentum,
    fc2_momentum,
    norm_gains,
    shift_biases,
    head_biases,
    hidden_bias,
    position_table,
    gain_momentum,
    shift_momentum,
    head_bias_momentum,
    hidden_bias_momentum,
    table_momentum,
    region_ids,
    position_index,
):
    devices = lax.axis_size("dp") * lax.axis_size("tensor")
    images = tokens.shape[0] // AREA * devices
    blocks = (qkv_weight, fc1_weight, proj_weight, fc2_weight)
    weights = tuple(as_slab(w, wide) for w, wide in zip(blocks, WIDE))
    momenta = tuple(
        as_slab(m, wide)
        for m, wide in zip((qkv_momentum, fc1_momentum, proj_momentum, fc2_momentum), WIDE)
    )
    ndp, nt = lax.axis_size("dp"), lax.axis_size("tensor")
    forward, gathered = attention_forward(
        tokens,
        norm_gains,
        shift_biases,
        head_biases,
        position_table.T,
        position_index,
        region_ids,
        weights[1:],
        weights[0],
        ndp,
        nt,
        (1, 0),
    )
    xs, a1, qkv, probs, mixed = forward
    w1, wproj, w2, wqkv = gathered
    output, dy, g1, g2, gproj, hidden_sum, sums2 = mlp(
        xs, mixed, out_grad, wproj, w1, w2, norm_gains, shift_biases, hidden_bias
    )
    input_grad, slab2, slab1, slab3, slab0, bundle0, bundle1, total = attention_backward(
        dy,
        xs,
        a1,
        qkv,
        probs,
        wqkv,
        wproj,
        norm_gains,
        position_index,
        hidden_sum,
        sums2,
        (gproj, g1, g2),
        (momenta[2], momenta[1], momenta[3]),
        momenta[0],
        ndp,
        nt,
        images,
        2,
    )
    small_params = (norm_gains, shift_biases, head_biases, hidden_bias.reshape(1, -1), position_table.T)
    small_moms = (
        gain_momentum,
        shift_momentum,
        head_bias_momentum,
        hidden_bias_momentum.reshape(1, -1),
        table_momentum.T,
    )
    slab_grads = (slab0, slab1, slab2, slab3)
    landed = newton_schulz((bundle0, bundle1), 3)
    rates = tuple(MATRIX_RATE * factor for factor in FACTORS)
    results = finish(landed, total, slab_grads, momenta, weights, small_params, small_moms, rates)
    slab_grads, new_weights, new_momenta = (results[i * nt : (i + 1) * nt] for i in range(3))
    smalls = tuple(
        s.reshape(-1) if i % 5 == 3 else s.T if i % 5 == 4 else s
        for i, s in enumerate(results[3 * nt :])
    )

    def placed(slabs):
        placed = tuple(as_block(s, like, wide) for s, like, wide in zip(slabs, blocks, WIDE))
        return tuple(placed[i] for i in ORDER)

    return (
        (output, input_grad)
        + placed(slab_grads)
        + placed(new_weights)
        + placed(new_momenta)
        + smalls
    )


def solution(mesh):
    rows = P(("dp", "tensor"), None)
    wide, tall = P(None, "tensor", "dp"), P("tensor", "dp", None)
    matrices = (wide, tall, wide, tall)
    return jax.shard_map(
        shards,
        mesh=mesh,
        in_specs=(rows, rows) + matrices * 2 + (P(),) * 12,
        out_specs=(rows, rows) + matrices * 3 + (P(),) * 15,
        check_vma=False,
    )
```

```python
import functools
import math

import jax
import jax.numpy as jnp
from jax import lax
from jax.experimental import pallas as pl
from jax.experimental.pallas import tpu as pltpu
from jax.sharding import PartitionSpec as P

D = 512
HEADS = 16
FF = 2048
HEAD = 32
WIN = 7
SIDE = 14
SHIFT = 3
NS_STEPS = 5

NORM_EPSILON = 1e-05
MASK_VALUE = -100.0
MUON_EPSILON = 1e-07
QUINTIC = (3.4445, -4.775, 2.0315)
MOMENTUM = 0.9
MATRIX_RATE = 0.5
VECTOR_RATE = 1.0

AREA = SIDE * SIDE
SPOTS = WIN * WIN
ACROSS = SIDE // WIN
WINDOWS = ACROSS * ACROSS
SLOT = 64
LANES = 128
OCT = 8
OCTS = HEADS // OCT
OCT_W = OCT * HEAD
PAIRS = OCT // 2
ROWS_S = PAIRS * SLOT
PAD_SCORE = -1e30
STEP_IMAGES = 2
STEP_ROWS = STEP_IMAGES * AREA
STEP_SLOTS = STEP_IMAGES * WINDOWS * SLOT
PART = 128
GROUPS = 4
F32 = jnp.float32
BF16 = jnp.bfloat16
VMEM_LIMIT = 60 * 1024 * 1024


def window_pieces():
    pieces = []
    for down in range(ACROSS):
        for over in range(ACROSS):
            for line in range(WIN):
                src_row = (down * WIN + line + SHIFT) % SIDE
                column = 0
                while column < WIN:
                    src_col = (over * WIN + column + SHIFT) % SIDE
                    length = min(WIN - column, SIDE - src_col)
                    slot = (down * ACROSS + over) * SLOT + line * WIN + column
                    pieces.append((slot, src_row * SIDE + src_col, length))
                    column += length
    return pieces


PIECES = window_pieces()


def dot_nn(a, b):
    return lax.dot_general(a, b, (((1,), (0,)), ((), ())), preferred_element_type=F32)


def dot_nt(a, b):
    return lax.dot_general(a, b, (((1,), (1,)), ((), ())), preferred_element_type=F32)


def dot_tn(a, b):
    return lax.dot_general(a, b, (((0,), (0,)), ((), ())), preferred_element_type=F32)


def row_mean(values):
    return jnp.mean(values, axis=-1, keepdims=True)


def whiten(values):
    center = values - row_mean(values)
    inverse = lax.rsqrt(row_mean(center * center) + NORM_EPSILON)
    return center * inverse, inverse


def into_slots(src_ref, dst_ref):
    for image in range(STEP_IMAGES):
        for slot, raster, length in PIECES:
            dst_ref[image * WINDOWS * SLOT + slot : image * WINDOWS * SLOT + slot + length, :] = src_ref[
                image * AREA + raster : image * AREA + raster + length, :
            ]


def out_of_slots(src_ref, dst_ref):
    for image in range(STEP_IMAGES):
        for slot, raster, length in PIECES:
            dst_ref[image * AREA + raster : image * AREA + raster + length, :] = src_ref[
                image * WINDOWS * SLOT + slot : image * WINDOWS * SLOT + slot + length, :
            ]


def pair_mask():
    pair = lax.broadcasted_iota(jnp.int32, (SLOT, OCT_W), 1) // (2 * HEAD)
    return jnp.concatenate([(pair == at).astype(F32) for at in range(PAIRS)], axis=0).astype(BF16)


def side_mask():
    side = lax.broadcasted_iota(jnp.int32, (SLOT, OCT_W), 1) // HEAD % 2
    return jnp.concatenate([(side == at).astype(F32) for at in range(2)], axis=0).astype(BF16)


def spread(values, mask_ref):
    return jnp.concatenate([values] * (mask_ref.shape[0] // SLOT), axis=0) * mask_ref[...]


def turned(values):
    return jnp.concatenate([values[at : at + LANES].T for at in range(0, ROWS_S, LANES)], axis=1)


def by_side(values, first_side):
    return jnp.where(first_side, values[0:SLOT], values[SLOT:])


def by_pair(weights, side_values):
    tiles = []
    first = lane_iota(SLOT) < SLOT
    for at in range(0, OCT_W, LANES):
        tile = dot_nn(weights[at : at + LANES], side_values[:, at : at + LANES])
        tiles.append(jnp.where(first, tile[0:SLOT], tile[SLOT:]))
    return jnp.concatenate(tiles, axis=1)


def lane_iota(rows):
    return lax.broadcasted_iota(jnp.int32, (rows, LANES), 1)


def build_bias(region_ref, index_ref, table_ref, bias_ref, idx_scr, tab_scr):
    heads, rows = table_ref.shape
    tab_scr[...] = jnp.zeros_like(tab_scr)
    tab_scr[:, 0:rows] = table_ref[...]
    by_head = tab_scr[...]
    lanes = lane_iota(SLOT)
    index = key_by_query(index_ref, idx_scr).astype(jnp.int32)
    sublanes = lax.broadcasted_iota(jnp.int32, (SLOT, LANES), 0)
    spot = lanes % SLOT
    masks = []
    for down in range(ACROSS):
        for over in range(ACROSS):
            row_ids = jnp.full((SLOT, LANES), -1, jnp.int32)
            col_ids = jnp.full((SLOT, LANES), -1, jnp.int32)
            for at in range(SPOTS):
                value = region_ref[down * WIN + at // WIN, over * WIN + at % WIN]
                row_ids = jnp.where(sublanes == at, value, row_ids)
                col_ids = jnp.where(spot == at, value, col_ids)
            masks.append(
                jnp.where(sublanes < SPOTS, jnp.where(row_ids == col_ids, 0.0, MASK_VALUE), PAD_SCORE)
            )
    low = index < LANES
    index_low = jnp.where(low, index, 0)
    index_high = jnp.where(low, 0, index - LANES)

    def gathered(head):
        first = jnp.broadcast_to(by_head[head : head + 1, 0:LANES], (SLOT, LANES))
        second = jnp.broadcast_to(by_head[head : head + 1, LANES : 2 * LANES], (SLOT, LANES))
        return jnp.where(
            low,
            jnp.take_along_axis(first, index_low, axis=1),
            jnp.take_along_axis(second, index_high, axis=1),
        )

    for octet in range(OCTS):
        for pair in range(PAIRS):
            head = octet * OCT + 2 * pair
            tile = jnp.where(lanes < SLOT, gathered(head), gathered(head + 1))
            for window in range(WINDOWS):
                bias_ref[window, octet, pair * SLOT : (pair + 1) * SLOT, :] = tile + masks[window]


MESH = pl.DeviceIdType.MESH


def flipped(bit, by):
    return bit + by - 2 * bit * by


class Place:
    def __init__(self, ndp, nt):
        self.ndp, self.nt = ndp, nt
        self.nz = ndp // 2
        self.dp, self.t = lax.axis_index("dp"), lax.axis_index("tensor")
        self.z, self.y = self.dp // 2, self.dp % 2
        self.x, self.c = self.t // 2, self.t % 2

    def up(self, k):
        return lax.rem(self.z + k, self.nz)

    def down(self, k):
        return lax.rem(self.z + self.nz - k, self.nz)

    def device(self, z=None, y=None, x=None, c=None):
        z, y = self.z if z is None else z, self.y if y is None else y
        x, c = self.x if x is None else x, self.c if c is None else c
        return {"dp": z * 2 + y, "tensor": x * 2 + c}

    def block(self, z, y, x, c):
        return (x * 2 + c) * self.ndp + z * 2 + y

    def across(self, c, a, b):
        return flipped(self.y, c * a + (1 - c) * b), flipped(self.x, (1 - c) * a + c * b)

    def chip(self, c, a, b):
        y, x = self.across(c, a, b)
        return self.device(y=y, x=x)

    def bit_partner(self, b):
        size = 2**b
        return self.z + size * (1 - 2 * lax.rem(self.z // size, 2))

    def greet(self):
        others = [self.device(c=1 - self.c), self.device(x=1 - self.x)]
        others += [self.device(x=1 - self.x, c=1 - self.c), self.device(y=1 - self.y)]
        others += [self.device(z=self.up(k)) for k in range(1, self.nz)]
        barrier = pltpu.get_barrier_semaphore()
        for other in others:
            pl.semaphore_signal(barrier, inc=1, device_id=other, device_id_type=MESH)
        pl.semaphore_wait(barrier, len(others))


def remote(src, dst, send_sem, recv_sem, device):
    return pltpu.make_async_remote_copy(
        src_ref=src,
        dst_ref=dst,
        send_sem=send_sem,
        recv_sem=recv_sem,
        device_id=device,
        device_id_type=MESH,
    )


class Gather:
    def __init__(self, place, slabs, outs, scratch):
        count = len(slabs)
        self.place, self.slabs, self.outs, self.count = place, slabs, outs, count
        self.lows = scratch[:count]
        self.send_sem, self.recv_sem, self.local_sem = scratch[count:]

    @staticmethod
    def scratch(shapes, n):
        messages = len(shapes) * (n - 1)
        return [pltpu.VMEM(s, BF16) for s in shapes] + [
            pltpu.SemaphoreType.DMA((messages,)),
            pltpu.SemaphoreType.DMA((messages,)),
            pltpu.SemaphoreType.DMA((len(shapes),)),
        ]

    def copy(self, stage, m, a, b, k):
        place, nz = self.place, self.place.nz
        order = 1 - place.c
        base = {"z": -1, "p": nz - 1, "q": 2 * nz - 1, "c": 4 * nz - 1}[stage]
        at = m * (8 * nz - 1) + base + (b * 2 + a) * nz + k
        y, x = place.across(order, a, b)
        where = place.block(place.down(k), y, x, place.c)
        device = {
            "p": lambda: place.chip(order, 1, 0),
            "q": lambda: place.chip(order, 0, 1),
            "c": lambda: place.device(c=1 - place.c),
            "z": lambda: place.device(z=place.up(k)),
        }[stage]()
        if stage == "z":
            where = place.block(place.z, place.y, place.x, place.c)
        mine = stage == "z" or (a, b, k) == (0, 0, 0)
        src = self.lows[m] if mine else self.outs[m].at[where]
        return remote(src, self.outs[m].at[where], self.send_sem.at[at], self.recv_sem.at[at], device)

    def local(self, m):
        place = self.place
        where = place.block(place.z, place.y, place.x, place.c)
        return pltpu.make_async_copy(self.lows[m], self.outs[m].at[where], self.local_sem.at[m])

    def send(self, stage, a, b, k):
        for m in range(self.count):
            self.copy(stage, m, a, b, k).start()

    def wait(self, stage, a, b, k):
        for m in range(self.count):
            self.copy(stage, m, a, b, k).wait_recv()

    def column(self, k):
        if k:
            self.wait("z", 0, 0, k)
        self.send("p", 0, 0, k)
        self.send("q", 0, 0, k)
        self.send("c", 0, 0, k)

    def first(self, k):
        self.wait("p", 0, 0, k)
        self.send("q", 1, 0, k)
        self.send("c", 1, 0, k)

    def second(self, a, k):
        self.wait("q", a, 0, k)
        self.send("c", a, 1, k)

    def round(self):
        return range(self.place.nz)

    def begin(self):
        for slab, low in zip(self.slabs, self.lows):
            low[...] = slab[...].astype(BF16)
        for m in range(self.count):
            self.local(m).start()
        for k in self.round()[1:]:
            self.send("z", 0, 0, k)

    def end(self):
        everything = [("z", 0, 0, k) for k in self.round()[1:]]
        everything += [("p", 0, 0, k) for k in self.round()]
        everything += [("q", a, 0, k) for a in range(2) for k in self.round()]
        last = [("c", a, b, k) for b in range(2) for a in range(2) for k in self.round()]
        for key in last:
            self.wait(*key)
        for m in range(self.count):
            self.local(m).wait()
            for stage, a, b, k in everything + last:
                self.copy(stage, m, a, b, k).wait_send()

    def at_once(self):
        self.place.greet()
        self.begin()
        self.column(0)
        self.spread()
        self.end()

    def spread(self):
        for k in self.round()[1:]:
            self.column(k)
            self.first(k - 1)
        self.first(self.place.nz - 1)
        for a in range(2):
            for k in self.round():
                self.second(a, k)


class Reduce:
    def __init__(self, place, grads, scratch):
        count = len(grads)
        self.place, self.grads, self.count = place, grads, count
        self.own, self.from_core, self.from_p, self.from_q, self.from_z = (
            scratch[i * count : (i + 1) * count] for i in range(5)
        )
        self.send_sem, self.recv_sem, self.local_sem = scratch[5 * count :]

    @staticmethod
    def scratch(rows, n):
        nz, count = n // 8, len(rows)
        shapes = []
        for lead in ((2, 2, nz), (2, 2, nz), (2, nz), (nz,), (nz - 1,)):
            shapes += [pltpu.VMEM(lead + (r, D), BF16) for r in rows]
        return shapes + [
            pltpu.SemaphoreType.DMA((count * (8 * nz - 1),)),
            pltpu.SemaphoreType.DMA((count * (8 * nz - 1),)),
            pltpu.SemaphoreType.DMA((count * 4 * nz,)),
        ]

    def ks(self):
        return list(range(1, self.place.nz)) + [0]

    def copy(self, stage, m, a, b, k):
        place, nz = self.place, self.place.nz
        base = {"c": 0, "p": 4 * nz, "q": 6 * nz, "z": 7 * nz - 1}[stage]
        at = m * (8 * nz - 1) + base + {"c": (a * 2 + b) * nz + k, "p": b * nz + k}.get(stage, k)
        sems = self.send_sem.at[at], self.recv_sem.at[at]
        if stage == "c":
            y, x = place.across(1 - place.c, a, b)
            where = place.block(place.up(k), y, x, 1 - place.c)
            return remote(
                self.grads[m].at[where], self.from_core[m].at[a, b, k], *sems, place.device(c=1 - place.c)
            )
        src = self.own[m].at[a, b, k]
        if stage == "p":
            return remote(src, self.from_p[m].at[b, k], *sems, place.chip(place.c, 1, 0))
        if stage == "q":
            return remote(src, self.from_q[m].at[k], *sems, place.chip(place.c, 0, 1))
        return remote(src, self.from_z[m].at[k - 1], *sems, place.device(z=place.up(k)))

    def local(self, m, a, b, k):
        place, nz = self.place, self.place.nz
        y, x = place.across(place.c, a, b)
        where = place.block(place.up(k), y, x, place.c)
        at = m * 4 * nz + (a * 2 + b) * nz + k
        return pltpu.make_async_copy(
            self.grads[m].at[where], self.own[m].at[a, b, k], self.local_sem.at[at]
        )

    def order(self):
        return [(a, b, k) for a in (1, 0) for b in (1, 0) for k in self.ks()]

    def begin(self):
        for a, b, k in self.order():
            for m in range(self.count):
                self.copy("c", m, a, b, k).start()
        for a, b, k in self.order():
            for m in range(self.count):
                self.local(m, a, b, k).start()

    def value(self, m, a, b, k):
        self.local(m, a, b, k).wait()
        self.copy("c", m, a, b, k).wait_recv()
        value = self.own[m][a, b, k].astype(F32) + self.from_core[m][a, b, k].astype(F32)
        if a == 0:
            self.copy("p", m, 1, b, k).wait_recv()
            value = value + self.from_p[m][b, k].astype(F32)
            if b == 0:
                self.copy("q", m, 0, 1, k).wait_recv()
                value = value + self.from_q[m][k].astype(F32)
        return value

    def pass_on(self, a, b, between=None):
        stage = "p" if a else "q" if b else "z"
        waiting = []
        for k in self.ks():
            if stage == "z" and k == 0:
                continue
            for m in range(self.count):
                self.own[m][a, b, k] = self.value(m, a, b, k).astype(BF16)
            for copy in waiting:
                copy.start()
            waiting = [self.copy(stage, m, a, b, k) for m in range(self.count)]
        if between is not None:
            between()
        for copy in waiting:
            copy.start()

    def totals(self):
        values = [self.value(m, 0, 0, 0) for m in range(self.count)]
        for m in range(self.count):
            for k in self.ks()[:-1]:
                self.copy("z", m, 0, 0, k).wait_recv()
                values[m] = values[m] + self.from_z[m][k - 1].astype(F32)
        return values

    def end(self):
        for m in range(self.count):
            for a, b, k in self.order():
                self.copy("c", m, a, b, k).wait_send()
                if a:
                    self.copy("p", m, a, b, k).wait_send()
                elif b:
                    self.copy("q", m, a, b, k).wait_send()
                elif k:
                    self.copy("z", m, a, b, k).wait_send()


class Share:
    def __init__(self, place, core, fresh, bundle, scratch):
        self.place, self.core, self.fresh, self.bundle = place, core, fresh, bundle
        self.send_sem, self.recv_sem, self.near_sem = scratch

    @staticmethod
    def scratch(n, nt):
        messages = 2 + (nt - 1) + (n // 8 - 1) + n // 8
        return [
            pltpu.SemaphoreType.DMA((messages,)),
            pltpu.SemaphoreType.DMA((messages,)),
            pltpu.SemaphoreType.DMA,
        ]

    def near(self, i):
        place = self.place
        return pltpu.make_async_copy(self.fresh.at[i], self.bundle.at[place.dp, place.t], self.near_sem)

    def handed(self, i, label):
        place = self.place
        to = self.core + 2 * i
        return remote(
            self.fresh.at[i],
            self.bundle.at[place.dp, place.t],
            self.send_sem.at[i],
            self.recv_sem.at[label],
            {"dp": place.dp, "tensor": to},
        )

    def each(self, then):
        for i in range(2):
            to = self.core + 2 * i

            @pl.when(self.place.t != to)
            def _(i=i, to=to):
                then(self.handed(i, lax.rem(self.place.t + self.place.nt - to, self.place.nt) - 1))

    def hand(self):
        self.each(lambda copy: copy.start())
        for i in range(2):

            @pl.when(self.place.t == self.core + 2 * i)
            def _(i=i):
                self.near(i).start()

    def move(self, stage, k):
        place, nz = self.place, self.place.nz
        at = self.place.nt - 1 + (k - 1 if stage == "z" else nz - 1 + k)
        sems = self.send_sem.at[2 + at], self.recv_sem.at[at]
        if stage == "z":
            where, device = place.dp, place.device(z=place.up(k))
        else:
            where, device = place.down(k) * 2 + place.y, place.device(y=1 - place.y)
        return remote(self.bundle.at[where], self.bundle.at[where], *sems, device)

    def mine(self):
        return pl.when(self.place.c == self.core)

    def along_z(self):
        @self.mine()
        def _():
            self.near(0).wait()
            for label in range(self.place.nt - 1):
                self.handed(0, label).wait_recv()
            for k in range(1, self.place.nz):
                self.move("z", k).start()
            self.move("y", 0).start()

    def along_y(self):
        @self.mine()
        def _():
            for k in range(1, self.place.nz):
                self.move("z", k).wait_recv()
                self.move("y", k).start()

    def end(self):
        self.each(lambda copy: copy.wait_send())

        @self.mine()
        def _():
            for k in range(self.place.nz):
                self.move("y", k).wait_recv()
            for k in range(self.place.nz):
                self.move("y", k).wait_send()
                if k:
                    self.move("z", k).wait_send()


def renew(totals, momenta, grad_out, fresh, images):
    values = []
    for total, momentum, out in zip(totals, momenta, grad_out):
        grad = total / images
        out[...] = grad
        values.append(MOMENTUM * momentum[...] + grad)
    for value, ref in zip(values, fresh):
        ref[0 : value.shape[0], :] = value.astype(BF16)


def gather_kernel(ndp, nt, count, *refs):
    Gather(Place(ndp, nt), refs[:count], refs[count : 2 * count], refs[2 * count :]).at_once()


def gather_weights(slabs, ndp, nt, collective_id):
    count, n = len(slabs), ndp * nt
    gathered = pl.pallas_call(
        functools.partial(gather_kernel, ndp, nt, count),
        out_shape=tuple(shape_of((n,) + s.shape, BF16) for s in slabs),
        in_specs=[pl.BlockSpec(memory_space=pltpu.VMEM)] * count,
        out_specs=tuple(pl.BlockSpec(memory_space=pl.ANY) for _ in slabs),
        scratch_shapes=Gather.scratch([s.shape for s in slabs], n),
        compiler_params=pltpu.CompilerParams(
            collective_id=collective_id, has_side_effects=True, vmem_limit_bytes=VMEM_LIMIT
        ),
        name="gather_weights",
    )(*slabs)
    return tuple(g.reshape(n * s.shape[0], D) for g, s in zip(gathered, slabs))


SMALL_ROWS = 32
TABLE_ROW = 16


class SmallSum:
    def __init__(self, place, values, arrived, send_sem, recv_sem):
        self.values, self.arrived = values, arrived
        self.send_sem, self.recv_sem = send_sem, recv_sem
        self.steps = [
            place.device(c=1 - place.c),
            place.device(x=1 - place.x),
            place.device(y=1 - place.y),
        ]
        bit = 0
        while 2**bit < place.nz:
            self.steps.append(place.device(z=place.bit_partner(bit)))
            bit += 1
        self.done = 0

    def copy(self, i):
        return remote(
            self.values.at[i], self.arrived.at[i], self.send_sem.at[i], self.recv_sem.at[i], self.steps[i]
        )

    def begin(self):
        self.copy(0).start()

    def step(self):
        i = self.done
        if i < len(self.steps):
            self.copy(i).wait_recv()
            self.values[i + 1] = self.values[i] + self.arrived[i]
            self.done += 1

    def go_on(self):
        if 0 < self.done < len(self.steps):
            self.copy(self.done).start()

    def end(self):
        while self.done < len(self.steps):
            self.step()
            self.go_on()
        for i in range(len(self.steps)):
            self.copy(i).wait_send()
        return self.values[len(self.steps)]


def padded(rows):
    return -(-max(rows) // 16) * 16


def pack_small(small, sums1, sums2, head, hidden, table):
    small[0] = jnp.zeros_like(small[0])
    small[0, 0:1, :] = sums1[0:1, :]
    small[0, 1:2, :] = sums2[0:1, :]
    small[0, 2:3, :] = sums1[1:2, :]
    small[0, 3:6, :] = sums2[1:4, :]
    small[0, 6:8, :] = head[...]
    for i in range(hidden.shape[1] // D):
        small[0, 8 + i : 9 + i, :] = hidden[0:1, i * D : (i + 1) * D]
    small[0, TABLE_ROW : TABLE_ROW + table.shape[0], 0 : table.shape[1]] = table[...]


def newton_schulz_kernel(nt, heights, first_ref, second_ref, landed0, landed1, g_scr, x_scr, a_scr, y_scr, back, sem, send_sem, recv_sem):
    first, second, third = QUINTIC
    chunk = 512
    t, dp = lax.axis_index("tensor"), lax.axis_index("dp")
    core = t % 2
    sources = (first_ref, second_ref)
    landed = (landed0, landed1)
    barrier = pltpu.get_barrier_semaphore()
    for d in range(1, nt):
        other = {"dp": dp, "tensor": lax.rem(t + d, nt)}
        pl.semaphore_signal(barrier, inc=1, device_id=other, device_id_type=MESH)
    for which, ref in enumerate(sources):

        @pl.when(core == which)
        def _(ref=ref):
            copy = pltpu.make_async_copy(ref, g_scr.at[0 : ref.shape[0]], sem)
            copy.start()
            copy.wait()

    chunks = jnp.where(core == 0, first_ref.shape[0] // chunk, second_ref.shape[0] // chunk)

    def low(values):
        return values.astype(BF16)

    def gram(src_ref):
        a_scr[...] = jnp.zeros_like(a_scr)

        def add(at, carry):
            part = src_ref[pl.ds(pl.multiple_of(at * chunk, chunk), chunk), :]
            a_scr[...] += dot_tn(part, part)
            return carry

        lax.fori_loop(0, chunks, add, 0)
        return a_scr[...]

    def advance(src_ref, factor, scale):
        factor = low(factor)

        def step(at, carry):
            at = pl.ds(pl.multiple_of(at * chunk, chunk), chunk)
            x_scr[at, :] = low(dot_nn(src_ref[at, :], factor) * scale)
            return carry

        lax.fori_loop(0, chunks, step, 0)

    def bend(a):
        return second * a + third * dot_nn(low(a), low(a))

    diagonal = lax.broadcasted_iota(jnp.int32, (D, D), 0) == lax.broadcasted_iota(jnp.int32, (D, D), 1)

    def two_turns(a):
        b = bend(a)
        q = b + jnp.where(diagonal, first, 0.0)
        r = first * a + dot_nn(low(a), low(b))
        a = first * r + dot_nn(low(r), low(b))
        b = bend(a)
        return first * q + dot_nn(low(b), low(q))

    a = gram(g_scr)
    scale = 1.0 / (jnp.sqrt(jnp.sum(jnp.where(diagonal, a, 0.0))) + MUON_EPSILON)
    advance(g_scr, two_turns(a * scale * scale), scale)
    q = two_turns(gram(x_scr))
    for which, ref in enumerate(sources):

        @pl.when(core == which)
        def _(ref=ref):
            mine = nt * heights[which]
            at = pl.ds(pl.multiple_of(dp * mine, mine), mine)
            y_scr[0:mine, :] = dot_nn(x_scr[at, :], low(q))

    advance(x_scr, q, 1.0)
    b = bend(gram(x_scr))
    here = y_scr[...]
    back[...] = low(first * here + dot_nn(low(here), low(b)))
    pl.semaphore_wait(barrier, nt - 1)

    def copy(which, d):
        to = lax.rem(t + d, nt)
        height = heights[which]
        return remote(
            back.at[pl.ds(pl.multiple_of(to * height, height), height)],
            landed[which].at[t // 2],
            send_sem.at[d - 1],
            recv_sem.at[d - 1],
            {"dp": dp, "tensor": to},
        )

    for which in range(2):

        @pl.when(core == which)
        def _(which=which):
            for d in range(1, nt):
                copy(which, d).start()
            height = heights[which]
            landed[which][t // 2] = back[pl.ds(pl.multiple_of(t * height, height), height), :]

    for d in range(1, nt):
        for which in range(2):

            @pl.when(lax.rem(t + nt - d, nt) % 2 == which)
            def _(d=d, which=which):
                copy(which, d).wait_recv()

    for which in range(2):

        @pl.when(core == which)
        def _(which=which):
            for d in range(1, nt):
                copy(which, d).wait_send()


def newton_schulz(bundles, collective_id):
    ndp, nt = bundles[0].shape[:2]
    heights = tuple(b.shape[2] for b in bundles)
    rows = [ndp * nt * h for h in heights]
    tall = max(rows)
    any_, vmem = pl.BlockSpec(memory_space=pl.ANY), pl.BlockSpec(memory_space=pltpu.VMEM)
    return pl.pallas_call(
        functools.partial(newton_schulz_kernel, nt, heights),
        out_shape=tuple(shape_of((nt // 2, h, D), BF16) for h in heights),
        in_specs=[any_, any_],
        out_specs=(vmem, vmem),
        scratch_shapes=[
            pltpu.VMEM((tall, D), BF16),
            pltpu.VMEM((tall, D), BF16),
            pltpu.VMEM((D, D), F32),
            pltpu.VMEM((tall // ndp, D), F32),
            pltpu.VMEM((tall // ndp, D), BF16),
            pltpu.SemaphoreType.DMA,
            pltpu.SemaphoreType.DMA((nt - 1,)),
            pltpu.SemaphoreType.DMA((nt - 1,)),
        ],
        compiler_params=pltpu.CompilerParams(
            collective_id=collective_id, has_side_effects=True, vmem_limit_bytes=VMEM_LIMIT
        ),
        name="newton_schulz",
    )(*(b.reshape(r, D) for b, r in zip(bundles, rows)))


def finish_kernel(nt, rates, *refs):
    refs = list(refs)

    def take(n):
        taken = refs[:n]
        del refs[:n]
        return taken

    landed, (total,) = take(2), take(1)
    grads, momenta, weights = take(nt), take(nt), take(nt)
    small_par, small_mom = take(5), take(5)
    grad_out, new_out, mom_out = take(nt), take(nt), take(nt)
    small_grad_out, small_new_out, small_mom_out = take(5), take(5), take(5)
    for m in range(nt):
        grad = grads[m][...]
        grad_out[m][...] = grad
        mom_out[m][...] = MOMENTUM * momenta[m][...] + grad
        new_out[m][...] = weights[m][...] - rates[m] * landed[m % 2][m // 2, 0 : grad.shape[0], :].astype(F32)

    def small_update(i, at, grad):
        small_grad_out[i][at] = grad
        grad = MOMENTUM * small_mom[i][at] + grad
        small_mom_out[i][at] = grad
        small_new_out[i][at] = small_par[i][at] - VECTOR_RATE * grad

    for i, (low, high) in enumerate(((0, 2), (2, 6), (6, 8))):
        small_update(i, (slice(None), slice(None)), total[low:high, :])
    for i in range(small_par[3].shape[1] // D):
        small_update(3, (slice(0, 1), slice(i * D, (i + 1) * D)), total[8 + i : 9 + i, :])
    heads, rows = small_par[4].shape
    small_update(4, (slice(None), slice(None)), total[TABLE_ROW : TABLE_ROW + heads, 0:rows])


def finish(landed, total, grads, momenta, weights, small_params, small_moms, rates):
    nt = len(grads)
    like = lambda arrays: tuple(shape_of(a.shape, F32) for a in arrays)
    return pl.pallas_call(
        functools.partial(finish_kernel, nt, rates),
        out_shape=like(grads) * 3 + like(small_params) * 3,
        compiler_params=pltpu.CompilerParams(vmem_limit_bytes=VMEM_LIMIT),
        name="finish",
    )(*landed, total, *grads, *momenta, *weights, *small_params, *small_moms)


def key_by_query(index_ref, idx_scr):
    idx_scr[...] = jnp.zeros_like(idx_scr)
    idx_scr[0:SPOTS, 0:SPOTS] = index_ref[...].astype(F32)
    index = idx_scr[...].T[0:SLOT, :]
    return jnp.where(lane_iota(SLOT) < SLOT, index, pltpu.roll(index, SLOT, 1))


def table_sums(dbias_ref, index_ref, table_scr, idx_scr, turned_idx):
    turned_idx[...] = key_by_query(index_ref, idx_scr)
    table_scr[...] = jnp.zeros_like(table_scr)
    lanes = lane_iota(PAIRS)
    entries = lax.broadcasted_iota(jnp.int32, (2 * LANES, LANES), 0).astype(F32)
    count = OCTS * OCT

    def one_key(key, carry):
        picks = (entries == turned_idx[pl.ds(key, 1), :]).astype(F32).astype(BF16)
        values = []
        for octet in range(OCTS):
            pairs = dbias_ref[octet, pl.ds(key, PAIRS, SLOT), :]
            values += [jnp.where(lanes < SLOT, pairs, 0.0), jnp.where(lanes < SLOT, 0.0, pairs)]
        values = jnp.concatenate(values, axis=0)
        parts = []
        for _ in range(3):
            low = values.astype(BF16).astype(F32)
            parts.append(low)
            values = values - low
        sums = dot_nt(jnp.concatenate(parts, axis=0).astype(BF16), picks)
        table_scr[...] += sums[0:count] + sums[count : 2 * count] + sums[2 * count :]
        return carry

    lax.fori_loop(0, SPOTS, one_key, 0)
    sums = table_scr[...]
    for octet in range(OCTS):
        for head in range(OCT):
            at = octet * OCT + head % 2 * PAIRS + head // 2
            table_scr[octet * OCT + head : octet * OCT + head + 1, :] = sums[at : at + 1]


def attention_forward_kernel(ndp, nt, steps, fused, *refs):
    refs = list(refs)

    def take(n):
        taken = refs[:n]
        del refs[:n]
        return taken

    x_ref, gain_ref, shift_ref, qkvb_ref, table_ref, index_ref, region_ref = take(7)
    slabs, (wqkv_in,) = take(3), take(1)
    xs_ref, a1_ref, qkv_ref, p_ref, o_ref = take(5)
    gathered = take(3)
    wqkv_all = take(1) if fused else None
    bias_scr, idx_scr, tab_scr, pair_scr, side_scr, a1_scr = take(6)
    place = Place(ndp, nt)
    rest = Gather(place, slabs, gathered, take(6))
    step, last = pl.program_id(0), pl.num_programs(0) - 1
    if fused:
        qkv_gather = Gather(place, (wqkv_in,), wqkv_all, take(4))
        wqkv_ref, load_sem = take(2)
    else:
        wqkv_ref = wqkv_in

    @pl.when(step == 0)
    def _():
        place.greet()
        if fused:
            qkv_gather.begin()
            qkv_gather.column(0)

    @pl.when(step < steps)
    def _():
        xs_ref[...] = jnp.zeros_like(xs_ref)
        into_slots(x_ref, xs_ref)
        white, _ = whiten(xs_ref[...])
        a1 = (white * gain_ref[0:1, :] + shift_ref[0:1, :]).astype(BF16)
        a1_ref[...] = a1
        a1_scr[pl.ds(pl.multiple_of(step * STEP_SLOTS, STEP_SLOTS), STEP_SLOTS), :] = a1

    @pl.when(step == 0)
    def _():
        if fused:
            for k in qkv_gather.round()[1:]:
                qkv_gather.column(k)
        build_bias(region_ref, index_ref, table_ref, bias_scr, idx_scr, tab_scr)
        pair_scr[...] = pair_mask()
        side_scr[...] = side_mask()

    if fused:

        @pl.when(step == 1)
        def _():
            for k in qkv_gather.round():
                qkv_gather.first(k)

        @pl.when(step == 2)
        def _():
            for a in range(2):
                for k in qkv_gather.round():
                    qkv_gather.second(a, k)

    @pl.when(step == 2)
    def _():
        rest.begin()
        rest.column(0)

    @pl.when(step == steps - 1)
    def _():
        if fused:
            qkv_gather.end()
            copies = []
            for i in range(ndp * nt):
                rows = wqkv_in.shape[0]
                copies.append(
                    pltpu.make_async_copy(
                        wqkv_all[0].at[i], wqkv_ref.at[i * rows : (i + 1) * rows], load_sem.at[i]
                    )
                )
                copies[i].start()
            for copy in copies:
                copy.wait()

    @pl.when(step >= steps)
    def _():
        at = pl.multiple_of((step - steps) * STEP_SLOTS, STEP_SLOTS)
        a1 = a1_scr[pl.ds(at, STEP_SLOTS), :]
        scale = HEAD ** (-0.5)
        for half in range(2):
            columns = 3 * PART * GROUPS // 2
            u = dot_nt(a1, wqkv_ref[half * columns : (half + 1) * columns, :])
            for inner in range(GROUPS // 2):
                group = half * (GROUPS // 2) + inner
                for part in range(3):
                    piece = u[:, (inner * 3 + part) * PART : (inner * 3 + part + 1) * PART]
                    if part == 0:
                        piece = (piece + qkvb_ref[0:1, group * PART : (group + 1) * PART]) * scale
                    elif part == 2:
                        piece = piece + qkvb_ref[1:2, group * PART : (group + 1) * PART]
                    lanes = part * D + group * PART
                    qkv_ref[:, lanes : lanes + PART] = piece.astype(BF16)

    real_query = (lane_iota(1) % SLOT < SPOTS).astype(F32)
    first_side = lax.broadcasted_iota(jnp.int32, (SLOT, OCT_W), 1) // HEAD % 2 == 0

    def one_window(at, carry):
        rows = pl.ds(pl.multiple_of(at * SLOT, SLOT), SLOT)
        for octet in range(OCTS):
            q = qkv_ref[rows, octet * OCT_W : (octet + 1) * OCT_W]
            k = qkv_ref[rows, D + octet * OCT_W : D + (octet + 1) * OCT_W]
            v = qkv_ref[rows, 2 * D + octet * OCT_W : 2 * D + (octet + 1) * OCT_W]
            scores = dot_nt(spread(k, pair_scr), spread(q, side_scr)) + bias_scr[lax.rem(at, WINDOWS), octet]
            probs = []
            for pair in range(PAIRS):
                part = scores[pair * SLOT : (pair + 1) * SLOT]
                grown = jnp.exp(part - jnp.max(part, axis=0, keepdims=True))
                probs.append(grown * (real_query / jnp.sum(grown, axis=0, keepdims=True)))
            probs = jnp.concatenate(probs, axis=0)
            p_ref[pl.ds(pl.multiple_of((at * OCTS + octet) * ROWS_S, ROWS_S), ROWS_S), :] = probs.astype(BF16)
            mixed = dot_nn(turned(probs).astype(BF16), spread(v, pair_scr))
            o_ref[rows, octet * OCT_W : (octet + 1) * OCT_W] = by_side(mixed, first_side).astype(BF16)
        return carry

    half_loop = STEP_IMAGES * WINDOWS // 2

    @pl.when(step >= steps)
    def _():
        lax.fori_loop(0, half_loop, one_window, 0, unroll=4)

    @pl.when(step == steps + 1)
    def _():
        for k in rest.round()[1:]:
            rest.column(k)

    @pl.when(step == steps + 2)
    def _():
        for k in rest.round():
            rest.first(k)

    @pl.when(step == last)
    def _():
        for a in range(2):
            for k in rest.round():
                rest.second(a, k)

    @pl.when(step >= steps)
    def _():
        lax.fori_loop(half_loop, 2 * half_loop, one_window, 0, unroll=4)

    @pl.when(step == last)
    def _():
        rest.end()


def mlp_kernel(
    xs_ref,
    o_ref,
    e_ref,
    wproj_ref,
    w1_ref,
    w2_ref,
    gain_ref,
    shift_ref,
    hb_ref,
    out_ref,
    dy_ref,
    g1_ref,
    g2_ref,
    gproj_ref,
    hsum_ref,
    sums_ref,
    acc1,
    acc2,
    accp,
    m_scr,
    da_scr,
    a2_scr,
    e_scr,
    slot_scr,
    y_ref,
):
    step = pl.program_id(0)

    @pl.when(step == 0)
    def _():
        acc1[...] = jnp.zeros_like(acc1)
        acc2[...] = jnp.zeros_like(acc2)
        accp[...] = jnp.zeros_like(accp)
        hsum_ref[...] = jnp.zeros_like(hsum_ref)
        sums_ref[...] = jnp.zeros_like(sums_ref)

    slot_scr[...] = xs_ref[...] + dot_nn(o_ref[...], wproj_ref[...]) + shift_ref[2:3, :]
    out_of_slots(slot_scr, y_ref)
    white, inverse = whiten(y_ref[...])
    a2_scr[...] = (white * gain_ref[1:2, :] + shift_ref[1:2, :]).astype(BF16)
    e_scr[...] = e_ref[...].astype(BF16)
    m_scr[...] = jnp.zeros_like(m_scr)
    da_scr[...] = jnp.zeros_like(da_scr)
    root = math.sqrt(2.0 / math.pi)
    width = 512

    def chunk(c, carry):
        at = pl.ds(pl.multiple_of(c * width, width), width)
        w1, w2 = w1_ref[at, :], w2_ref[at, :]
        a2, e = a2_scr[...], e_scr[...]
        z = dot_nt(a2, w1) + hb_ref[0:1, at]
        square = z * z
        t = jnp.tanh(z * (root + (root * 0.044715) * square))
        half = 0.5 * z
        f = (half + half * t).astype(BF16)
        slope = 0.5 + 0.5 * t + half * (1.0 - t * t) * (root + (3.0 * root * 0.044715) * square)
        dz = dot_nt(e, w2) * slope
        hsum_ref[0:1, at] += jnp.sum(dz, axis=0, keepdims=True)
        dz = dz.astype(BF16)
        m_scr[...] += dot_nn(f, w2)
        da_scr[...] += dot_nn(dz, w1)
        acc2[at, :] += dot_tn(f, e)
        acc1[at, :] += dot_tn(dz, a2)
        return carry

    lax.fori_loop(0, w1_ref.shape[0] // width, chunk, 0)
    white, inverse = whiten(y_ref[...])
    out_ref[...] = y_ref[...] + m_scr[...] + shift_ref[3:4, :]
    da = da_scr[...]
    t2 = da * gain_ref[1:2, :]
    dy = e_ref[...] + inverse * (t2 - row_mean(t2) - white * row_mean(t2 * white))
    m_scr[...] = dy
    dy_ref[...] = jnp.zeros_like(dy_ref)
    into_slots(m_scr, dy_ref)
    accp[...] += dot_tn(o_ref[...], dy_ref[...].astype(BF16))
    sums_ref[0:1, :] += jnp.sum(da * white, axis=0, keepdims=True)
    sums_ref[1:2, :] += jnp.sum(da, axis=0, keepdims=True)
    sums_ref[2:3, :] += jnp.sum(dy, axis=0, keepdims=True)
    sums_ref[3:4, :] += jnp.sum(e_ref[...], axis=0, keepdims=True)

    @pl.when(step == pl.num_programs(0) - 1)
    def _():
        g1_ref[...] = acc1[...].astype(BF16)
        g2_ref[...] = acc2[...].astype(BF16)
        gproj_ref[...] = accp[...].astype(BF16)


def attention_backward_kernel(ndp, nt, images, steps, *refs):
    refs = list(refs)

    def take(n):
        taken = refs[:n]
        del refs[:n]
        return taken

    dy_ref, xs_ref, a1_ref, qkv_ref, p_ref, wqkv_ref, wproj_ref, gain_ref, index_ref = take(9)
    hidden_ref, sums2_ref = take(2)
    grads, momenta, (qkv_momentum,) = take(3), take(3), take(1)
    (gin_ref,) = take(1)
    slabs, (qkv_slab,) = take(3), take(1)
    bundle0, bundle1, small_out = take(3)
    accq, gq, do_scr, du_scr, pair_scr, side_scr, g_scr, dbias_ref, hsum_ref, sums_ref = take(10)
    idx_scr, turned_idx, table_scr, fresh0, fresh1 = take(5)
    small, small_in, small_send, small_recv = take(4)
    place = Place(ndp, nt)
    step, last = pl.program_id(0), pl.num_programs(0) - 1
    share0 = Share(place, 0, fresh0, bundle0, take(3))
    share1 = Share(place, 1, fresh1, bundle1, take(3))
    early = Reduce(place, grads, take(18))
    late = Reduce(place, (gq,), take(8))
    tiny = SmallSum(place, small, small_in, small_send, small_recv)

    @pl.when(step == 0)
    def _():
        place.greet()
        early.begin()
        fresh0[...] = jnp.zeros_like(fresh0)
        fresh1[...] = jnp.zeros_like(fresh1)
        pair_scr[...] = pair_mask()
        side_scr[...] = side_mask()
        accq[...] = jnp.zeros_like(accq)
        dbias_ref[...] = jnp.zeros_like(dbias_ref)
        hsum_ref[...] = jnp.zeros_like(hsum_ref)
        sums_ref[...] = jnp.zeros_like(sums_ref)

    first_row = pl.multiple_of(lax.rem(step, steps) * STEP_SLOTS, STEP_SLOTS)
    step_rows = pl.ds(first_row, STEP_SLOTS)

    @pl.when(step < steps)
    def _():
        do_scr[...] = dot_nt(dy_ref[...].astype(BF16), wproj_ref[...]).astype(BF16)

    scale = HEAD ** (-0.5)
    first_side = lax.broadcasted_iota(jnp.int32, (SLOT, OCT_W), 1) // HEAD % 2 == 0

    def one_window(at, carry):
        rows = pl.ds(pl.multiple_of(at * SLOT, SLOT), SLOT)
        out_rows = pl.ds(pl.multiple_of(first_row + at * SLOT, SLOT), SLOT)
        for octet in range(OCTS):
            q = qkv_ref[rows, octet * OCT_W : (octet + 1) * OCT_W]
            k = qkv_ref[rows, D + octet * OCT_W : D + (octet + 1) * OCT_W]
            v = qkv_ref[rows, 2 * D + octet * OCT_W : 2 * D + (octet + 1) * OCT_W]
            do = do_scr[rows, octet * OCT_W : (octet + 1) * OCT_W]
            probs = p_ref[pl.ds(pl.multiple_of((at * OCTS + octet) * ROWS_S, ROWS_S), ROWS_S), :]
            side_do = spread(do, side_scr)
            weighted = probs.astype(F32) * dot_nt(spread(v, pair_scr), side_do)
            ds = []
            for pair in range(PAIRS):
                part = slice(pair * SLOT, (pair + 1) * SLOT)
                total = jnp.sum(weighted[part], axis=0, keepdims=True)
                ds.append(weighted[part] - probs[part].astype(F32) * total)
            ds = jnp.concatenate(ds, axis=0)
            dbias_ref[octet] += ds
            dq = by_side(dot_nn(turned(ds).astype(BF16), spread(k, pair_scr)), first_side) * scale
            dk = by_pair(ds.astype(BF16), spread(q, side_scr))
            dv = by_pair(probs, side_do)
            lanes = slice(octet * OCT_W, (octet + 1) * OCT_W)
            hsum_ref[0:1, lanes] += jnp.sum(dq, axis=0, keepdims=True)
            hsum_ref[1:2, lanes] += jnp.sum(dv, axis=0, keepdims=True)
            for part, grad in enumerate((dq, dk, dv)):
                for inner in range(OCT_W // PART):
                    group = octet * (OCT_W // PART) + inner
                    at_col = (group * 3 + part) * PART
                    du_scr[out_rows, at_col : at_col + PART] = grad[
                        :, inner * PART : (inner + 1) * PART
                    ].astype(BF16)
        return carry

    half_loop = STEP_IMAGES * WINDOWS // 2

    @pl.when(step < steps)
    def _():
        lax.fori_loop(0, half_loop, one_window, 0, unroll=4)

    @pl.when(step == 2)
    def _():
        early.pass_on(0, 1)

    @pl.when(step == 3)
    def _():
        early.pass_on(0, 0)

    @pl.when(step < steps)
    def _():
        lax.fori_loop(half_loop, 2 * half_loop, one_window, 0, unroll=4)

    @pl.when(step == 0)
    def _():
        early.pass_on(1, 1)
        early.pass_on(1, 0)

    @pl.when(step < steps)
    def _():
        accq[...] += dot_tn(du_scr[step_rows, :], a1_ref[...])

    @pl.when(step == steps - 1)
    def _():
        rows = gq.shape[1]
        for i in range(gq.shape[0]):
            gq[i] = accq[i * rows : (i + 1) * rows, :].astype(BF16)
        late.begin()

    @pl.when(step >= steps)
    def _():
        white, inverse = whiten(xs_ref[...])
        da = dot_nn(du_scr[step_rows, :], wqkv_ref[...])
        t1 = da * gain_ref[0:1, :]
        g_scr[...] = dy_ref[...] + inverse * (t1 - row_mean(t1) - white * row_mean(t1 * white))
        out_of_slots(g_scr, gin_ref)
        sums_ref[0:1, :] += jnp.sum(da * white, axis=0, keepdims=True)
        sums_ref[1:2, :] += jnp.sum(da, axis=0, keepdims=True)

    @pl.when(step == steps)
    def _():
        late.pass_on(1, 1)
        late.pass_on(1, 0)

    @pl.when(step == steps + 1)
    def _():
        late.pass_on(0, 1)

    @pl.when(step == steps + 2)
    def _():
        late.pass_on(0, 0)
        renew(early.totals(), momenta, slabs, (fresh0.at[1], fresh1.at[0], fresh1.at[1]), images)
        share1.hand()

    @pl.when(step == last)
    def _():
        share1.along_z()
        table_sums(dbias_ref, index_ref, table_scr, idx_scr, turned_idx)
        pack_small(small, sums_ref, sums2_ref, hsum_ref, hidden_ref, table_scr)
        tiny.begin()
        renew(late.totals(), (qkv_momentum,), (qkv_slab,), (fresh0.at[0],), images)
        tiny.step()
        share0.hand()
        tiny.go_on()
        tiny.step()
        tiny.go_on()
        share0.along_z()
        share1.along_y()
        tiny.step()
        tiny.go_on()
        share0.along_y()
        small_out[...] = tiny.end() / images
        share1.end()
        share0.end()
        early.end()
        late.end()


def whole(shape):
    return pl.BlockSpec(shape, lambda i: (0,) * len(shape))


def rows_of(rows, columns):
    return pl.BlockSpec((rows, columns), lambda i: (i, 0))


def shape_of(shape, dtype):
    return jax.ShapeDtypeStruct(shape, dtype)


PARAMS = pltpu.CompilerParams(dimension_semantics=("arbitrary",), vmem_limit_bytes=VMEM_LIMIT)


def remote_params(collective_id):
    return pltpu.CompilerParams(
        dimension_semantics=("arbitrary",),
        vmem_limit_bytes=VMEM_LIMIT,
        collective_id=collective_id,
        has_side_effects=True,
    )


def attention_forward(
    tokens, gains, shifts, head_biases, table, index, regions, slabs, qkv_slab, ndp, nt, collective_ids
):
    n = ndp * nt
    steps = tokens.shape[0] // STEP_ROWS
    slots = steps * STEP_SLOTS
    fused = qkv_slab.shape[0] % 16 == 0
    if not fused:
        (qkv_slab,) = gather_weights((qkv_slab,), ndp, nt, collective_ids[1])
    early = lambda i: (jnp.minimum(i, steps - 1), 0)
    late = lambda i: (jnp.maximum(i - steps, 0), 0)
    any_ = pl.BlockSpec(memory_space=pl.ANY)
    gathered = tuple(slabs) + ((qkv_slab,) if fused else ())
    results = pl.pallas_call(
        functools.partial(attention_forward_kernel, ndp, nt, steps, fused),
        grid=(2 * steps,),
        out_shape=(
            shape_of((slots, D), F32),
            shape_of((slots, D), BF16),
            shape_of((slots, 3 * D), BF16),
            shape_of((slots * OCTS * PAIRS, LANES), BF16),
            shape_of((slots, D), BF16),
        )
        + tuple(shape_of((n,) + s.shape, BF16) for s in gathered),
        in_specs=[
            pl.BlockSpec((STEP_ROWS, D), early),
            whole(gains.shape),
            whole(shifts.shape),
            whole(head_biases.shape),
            whole(table.shape),
            whole(index.shape),
            pl.BlockSpec(memory_space=pltpu.SMEM),
        ]
        + [whole(s.shape) for s in slabs]
        + [whole(qkv_slab.shape)],
        out_specs=(
            pl.BlockSpec((STEP_SLOTS, D), early),
            pl.BlockSpec((STEP_SLOTS, D), early),
            pl.BlockSpec((STEP_SLOTS, 3 * D), late),
            pl.BlockSpec((STEP_SLOTS * OCTS * PAIRS, LANES), late),
            pl.BlockSpec((STEP_SLOTS, D), late),
        )
        + (any_,) * len(gathered),
        scratch_shapes=[
            pltpu.VMEM((WINDOWS, OCTS, ROWS_S, LANES), F32),
            pltpu.VMEM((LANES, LANES), F32),
            pltpu.VMEM((HEADS, 2 * LANES), F32),
            pltpu.VMEM((ROWS_S, OCT_W), BF16),
            pltpu.VMEM((2 * SLOT, OCT_W), BF16),
            pltpu.VMEM((slots, D), BF16),
        ]
        + Gather.scratch([s.shape for s in slabs], n)
        + (
            Gather.scratch([qkv_slab.shape], n)
            + [pltpu.VMEM((n * qkv_slab.shape[0], D), BF16), pltpu.SemaphoreType.DMA((n,))]
            if fused
            else []
        ),
        compiler_params=remote_params(collective_ids[0]),
        name="attention_forward",
    )(tokens, gains, shifts, head_biases, table, index, regions, *slabs, qkv_slab)
    weights = [g.reshape(-1, D) for g in results[5:]]
    if not fused:
        weights.append(qkv_slab)
    return results[:5], weights


def mlp(xs, mixed, out_grad, wproj, w1, w2, gains, shifts, hidden_bias):
    steps = out_grad.shape[0] // STEP_ROWS
    hidden = w1.shape[0]
    return pl.pallas_call(
        mlp_kernel,
        grid=(steps,),
        out_shape=(
            shape_of(out_grad.shape, F32),
            shape_of(xs.shape, F32),
            shape_of(w1.shape, BF16),
            shape_of(w2.shape, BF16),
            shape_of(wproj.shape, BF16),
            shape_of((1, hidden), F32),
            shape_of((4, D), F32),
        ),
        in_specs=[
            rows_of(STEP_SLOTS, D),
            rows_of(STEP_SLOTS, D),
            rows_of(STEP_ROWS, D),
            whole(wproj.shape),
            whole(w1.shape),
            whole(w2.shape),
            whole(gains.shape),
            whole(shifts.shape),
            whole((1, hidden)),
        ],
        out_specs=(
            rows_of(STEP_ROWS, D),
            rows_of(STEP_SLOTS, D),
            whole(w1.shape),
            whole(w2.shape),
            whole(wproj.shape),
            whole((1, hidden)),
            whole((4, D)),
        ),
        scratch_shapes=[
            pltpu.VMEM(w1.shape, F32),
            pltpu.VMEM(w2.shape, F32),
            pltpu.VMEM(wproj.shape, F32),
            pltpu.VMEM((STEP_ROWS, D), F32),
            pltpu.VMEM((STEP_ROWS, D), F32),
            pltpu.VMEM((STEP_ROWS, D), BF16),
            pltpu.VMEM((STEP_ROWS, D), BF16),
            pltpu.VMEM((STEP_SLOTS, D), F32),
            pltpu.VMEM((STEP_ROWS, D), F32),
        ],
        compiler_params=PARAMS,
        name="mlp",
    )(xs, mixed, out_grad, wproj, w1, w2, gains, shifts, hidden_bias.reshape(1, hidden))


def attention_backward(
    dy,
    xs,
    a1,
    qkv,
    probs,
    wqkv,
    wproj,
    gains,
    index,
    hidden_sum,
    sums2,
    grads,
    momenta,
    qkv_momentum,
    ndp,
    nt,
    images,
    collective_id,
):
    n = ndp * nt
    rows = [m.shape[0] for m in momenta]
    qkv_rows = qkv_momentum.shape[0]
    steps = dy.shape[0] // STEP_SLOTS
    grads = tuple(g.reshape(n, r, D) for g, r in zip(grads, rows))
    any_ = pl.BlockSpec(memory_space=pl.ANY)
    early = lambda i: (jnp.minimum(i, steps - 1), 0)
    late = lambda i: (jnp.maximum(i - steps, 0), 0)
    both = lambda i: (lax.rem(i, steps), 0)
    tall0, tall1 = padded((qkv_rows, rows[0])), padded(rows[1:])
    small_steps = 3 + (ndp // 2 - 1).bit_length()
    return pl.pallas_call(
        functools.partial(attention_backward_kernel, ndp, nt, images, steps),
        grid=(2 * steps,),
        out_shape=(shape_of((steps * STEP_ROWS, D), F32),)
        + tuple(shape_of((r, D), F32) for r in rows + [qkv_rows])
        + (
            shape_of((ndp, nt, tall0, D), BF16),
            shape_of((ndp, nt, tall1, D), BF16),
            shape_of((SMALL_ROWS, D), F32),
        ),
        in_specs=[
            pl.BlockSpec((STEP_SLOTS, D), both),
            pl.BlockSpec((STEP_SLOTS, D), late),
            pl.BlockSpec((STEP_SLOTS, D), early),
            pl.BlockSpec((STEP_SLOTS, 3 * D), early),
            pl.BlockSpec((STEP_SLOTS * OCTS * PAIRS, LANES), early),
            whole(wqkv.shape),
            whole(wproj.shape),
            whole(gains.shape),
            whole(index.shape),
            whole(hidden_sum.shape),
            whole(sums2.shape),
            any_,
            any_,
            any_,
        ]
        + [whole((r, D)) for r in rows + [qkv_rows]],
        out_specs=(pl.BlockSpec((STEP_ROWS, D), late),)
        + tuple(whole((r, D)) for r in rows + [qkv_rows])
        + (any_, any_, whole((SMALL_ROWS, D))),
        scratch_shapes=[
            pltpu.VMEM(wqkv.shape, F32),
            pltpu.VMEM((n, qkv_rows, D), BF16),
            pltpu.VMEM((STEP_SLOTS, D), BF16),
            pltpu.VMEM((steps * STEP_SLOTS, 3 * D), BF16),
            pltpu.VMEM((ROWS_S, OCT_W), BF16),
            pltpu.VMEM((2 * SLOT, OCT_W), BF16),
            pltpu.VMEM((STEP_SLOTS, D), F32),
            pltpu.VMEM((OCTS, ROWS_S, LANES), F32),
            pltpu.VMEM((2, D), F32),
            pltpu.VMEM((2, D), F32),
            pltpu.VMEM((LANES, LANES), F32),
            pltpu.VMEM((SLOT, LANES), F32),
            pltpu.VMEM((HEADS, 2 * LANES), F32),
            pltpu.VMEM((2, tall0, D), BF16),
            pltpu.VMEM((2, tall1, D), BF16),
            pltpu.VMEM((small_steps + 1, SMALL_ROWS, D), F32),
            pltpu.VMEM((small_steps, SMALL_ROWS, D), F32),
            pltpu.SemaphoreType.DMA((small_steps,)),
            pltpu.SemaphoreType.DMA((small_steps,)),
        ]
        + Share.scratch(n, nt)
        + Share.scratch(n, nt)
        + Reduce.scratch(rows, n)
        + Reduce.scratch([qkv_rows], n),
        compiler_params=remote_params(collective_id),
        name="attention_backward",
    )(
        dy,
        xs,
        a1,
        qkv,
        probs,
        wqkv,
        wproj,
        gains,
        index,
        hidden_sum,
        sums2,
        *grads,
        *momenta,
        qkv_momentum,
    )


ORDER = (0, 2, 1, 3)
WIDE = (True, True, False, False)
FACTORS = (
    math.sqrt(3.0),
    math.sqrt(max(1.0, FF / D)),
    1.0,
    math.sqrt(max(1.0, D / FF)),
)


def as_slab(block, wide):
    return block.reshape(D, -1).T if wide else block.reshape(-1, D)


def as_block(slab, like, wide):
    return (slab.T if wide else slab).reshape(like.shape)


def shards(
    tokens,
    out_grad,
    qkv_weight,
    proj_weight,
    fc1_weight,
    fc2_weight,
    qkv_momentum,
    proj_momentum,
    fc1_momentum,
    fc2_momentum,
    norm_gains,
    shift_biases,
    head_biases,
    hidden_bias,
    position_table,
    gain_momentum,
    shift_momentum,
    head_bias_momentum,
    hidden_bias_momentum,
    table_momentum,
    region_ids,
    position_index,
):
    devices = lax.axis_size("dp") * lax.axis_size("tensor")
    images = tokens.shape[0] // AREA * devices
    blocks = (qkv_weight, fc1_weight, proj_weight, fc2_weight)
    weights = tuple(as_slab(w, wide) for w, wide in zip(blocks, WIDE))
    momenta = tuple(
        as_slab(m, wide)
        for m, wide in zip((qkv_momentum, fc1_momentum, proj_momentum, fc2_momentum), WIDE)
    )
    ndp, nt = lax.axis_size("dp"), lax.axis_size("tensor")
    forward, gathered = attention_forward(
        tokens,
        norm_gains,
        shift_biases,
        head_biases,
        position_table.T,
        position_index,
        region_ids,
        weights[1:],
        weights[0],
        ndp,
        nt,
        (1, 0),
    )
    xs, a1, qkv, probs, mixed = forward
    w1, wproj, w2, wqkv = gathered
    output, dy, g1, g2, gproj, hidden_sum, sums2 = mlp(
        xs, mixed, out_grad, wproj, w1, w2, norm_gains, shift_biases, hidden_bias
    )
    input_grad, slab2, slab1, slab3, slab0, bundle0, bundle1, total = attention_backward(
        dy,
        xs,
        a1,
        qkv,
        probs,
        wqkv,
        wproj,
        norm_gains,
        position_index,
        hidden_sum,
        sums2,
        (gproj, g1, g2),
        (momenta[2], momenta[1], momenta[3]),
        momenta[0],
        ndp,
        nt,
        images,
        2,
    )
    small_params = (norm_gains, shift_biases, head_biases, hidden_bias.reshape(1, -1), position_table.T)
    small_moms = (
        gain_momentum,
        shift_momentum,
        head_bias_momentum,
        hidden_bias_momentum.reshape(1, -1),
        table_momentum.T,
    )
    slab_grads = (slab0, slab1, slab2, slab3)
    landed = newton_schulz((bundle0, bundle1), 3)
    rates = tuple(MATRIX_RATE * factor for factor in FACTORS)
    results = finish(landed, total, slab_grads, momenta, weights, small_params, small_moms, rates)
    slab_grads, new_weights, new_momenta = (results[i * nt : (i + 1) * nt] for i in range(3))
    smalls = tuple(
        s.reshape(-1) if i % 5 == 3 else s.T if i % 5 == 4 else s
        for i, s in enumerate(results[3 * nt :])
    )

    def placed(slabs):
        placed = tuple(as_block(s, like, wide) for s, like, wide in zip(slabs, blocks, WIDE))
        return tuple(placed[i] for i in ORDER)

    return (
        (output, input_grad)
        + placed(slab_grads)
        + placed(new_weights)
        + placed(new_momenta)
        + smalls
    )


def solution(mesh):
    rows = P(("dp", "tensor"), None)
    wide, tall = P(None, "tensor", "dp"), P("tensor", "dp", None)
    matrices = (wide, tall, wide, tall)
    return jax.shard_map(
        shards,
        mesh=mesh,
        in_specs=(rows, rows) + matrices * 2 + (P(),) * 12,
        out_specs=(rows, rows) + matrices * 3 + (P(),) * 15,
        check_vma=False,
    )
```

```python
import functools
import math

import jax
import jax.numpy as jnp
from jax import lax
from jax.experimental import pallas as pl
from jax.experimental.pallas import tpu as pltpu
from jax.sharding import PartitionSpec as P

D = 512
HEADS = 16
FF = 2048
HEAD = 32
WIN = 7
SIDE = 14
SHIFT = 3
NS_STEPS = 5

NORM_EPSILON = 1e-05
MASK_VALUE = -100.0
MUON_EPSILON = 1e-07
QUINTIC = (3.4445, -4.775, 2.0315)
MOMENTUM = 0.9
MATRIX_RATE = 0.5
VECTOR_RATE = 1.0

AREA = SIDE * SIDE
SPOTS = WIN * WIN
ACROSS = SIDE // WIN
WINDOWS = ACROSS * ACROSS
SLOT = 64
LANES = 128
OCT = 8
OCTS = HEADS // OCT
OCT_W = OCT * HEAD
PAIRS = OCT // 2
ROWS_S = PAIRS * SLOT
PAD_SCORE = -1e30
STEP_IMAGES = 2
STEP_ROWS = STEP_IMAGES * AREA
STEP_SLOTS = STEP_IMAGES * WINDOWS * SLOT
PART = 128
GROUPS = 4
F32 = jnp.float32
BF16 = jnp.bfloat16
VMEM_LIMIT = 60 * 1024 * 1024


def window_pieces():
    pieces = []
    for down in range(ACROSS):
        for over in range(ACROSS):
            for line in range(WIN):
                src_row = (down * WIN + line + SHIFT) % SIDE
                column = 0
                while column < WIN:
                    src_col = (over * WIN + column + SHIFT) % SIDE
                    length = min(WIN - column, SIDE - src_col)
                    slot = (down * ACROSS + over) * SLOT + line * WIN + column
                    pieces.append((slot, src_row * SIDE + src_col, length))
                    column += length
    return pieces


PIECES = window_pieces()


def dot_nn(a, b):
    return lax.dot_general(a, b, (((1,), (0,)), ((), ())), preferred_element_type=F32)


def dot_nt(a, b):
    return lax.dot_general(a, b, (((1,), (1,)), ((), ())), preferred_element_type=F32)


def dot_tn(a, b):
    return lax.dot_general(a, b, (((0,), (0,)), ((), ())), preferred_element_type=F32)


def row_mean(values):
    return jnp.mean(values, axis=-1, keepdims=True)


def whiten(values):
    center = values - row_mean(values)
    inverse = lax.rsqrt(row_mean(center * center) + NORM_EPSILON)
    return center * inverse, inverse


def into_slots(src_ref, dst_ref):
    for image in range(STEP_IMAGES):
        for slot, raster, length in PIECES:
            dst_ref[image * WINDOWS * SLOT + slot : image * WINDOWS * SLOT + slot + length, :] = src_ref[
                image * AREA + raster : image * AREA + raster + length, :
            ]


def out_of_slots(src_ref, dst_ref):
    for image in range(STEP_IMAGES):
        for slot, raster, length in PIECES:
            dst_ref[image * AREA + raster : image * AREA + raster + length, :] = src_ref[
                image * WINDOWS * SLOT + slot : image * WINDOWS * SLOT + slot + length, :
            ]


def pair_mask():
    pair = lax.broadcasted_iota(jnp.int32, (SLOT, OCT_W), 1) // (2 * HEAD)
    return jnp.concatenate([(pair == at).astype(F32) for at in range(PAIRS)], axis=0).astype(BF16)


def side_mask():
    side = lax.broadcasted_iota(jnp.int32, (SLOT, OCT_W), 1) // HEAD % 2
    return jnp.concatenate([(side == at).astype(F32) for at in range(2)], axis=0).astype(BF16)


def spread(values, mask_ref):
    return jnp.concatenate([values] * (mask_ref.shape[0] // SLOT), axis=0) * mask_ref[...]


def turned(values):
    return jnp.concatenate([values[at : at + LANES].T for at in range(0, ROWS_S, LANES)], axis=1)


def by_side(values, first_side):
    return jnp.where(first_side, values[0:SLOT], values[SLOT:])


def by_pair(weights, side_values):
    tiles = []
    first = lane_iota(SLOT) < SLOT
    for at in range(0, OCT_W, LANES):
        tile = dot_nn(weights[at : at + LANES], side_values[:, at : at + LANES])
        tiles.append(jnp.where(first, tile[0:SLOT], tile[SLOT:]))
    return jnp.concatenate(tiles, axis=1)


def lane_iota(rows):
    return lax.broadcasted_iota(jnp.int32, (rows, LANES), 1)


def build_bias(region_ref, index_ref, table_ref, bias_ref, idx_scr, tab_scr):
    heads, rows = table_ref.shape
    tab_scr[...] = jnp.zeros_like(tab_scr)
    tab_scr[:, 0:rows] = table_ref[...]
    by_head = tab_scr[...]
    lanes = lane_iota(SLOT)
    index = key_by_query(index_ref, idx_scr).astype(jnp.int32)
    sublanes = lax.broadcasted_iota(jnp.int32, (SLOT, LANES), 0)
    spot = lanes % SLOT
    masks = []
    for down in range(ACROSS):
        for over in range(ACROSS):
            row_ids = jnp.full((SLOT, LANES), -1, jnp.int32)
            col_ids = jnp.full((SLOT, LANES), -1, jnp.int32)
            for at in range(SPOTS):
                value = region_ref[down * WIN + at // WIN, over * WIN + at % WIN]
                row_ids = jnp.where(sublanes == at, value, row_ids)
                col_ids = jnp.where(spot == at, value, col_ids)
            masks.append(
                jnp.where(sublanes < SPOTS, jnp.where(row_ids == col_ids, 0.0, MASK_VALUE), PAD_SCORE)
            )
    low = index < LANES
    index_low = jnp.where(low, index, 0)
    index_high = jnp.where(low, 0, index - LANES)

    def gathered(head):
        first = jnp.broadcast_to(by_head[head : head + 1, 0:LANES], (SLOT, LANES))
        second = jnp.broadcast_to(by_head[head : head + 1, LANES : 2 * LANES], (SLOT, LANES))
        return jnp.where(
            low,
            jnp.take_along_axis(first, index_low, axis=1),
            jnp.take_along_axis(second, index_high, axis=1),
        )

    for octet in range(OCTS):
        for pair in range(PAIRS):
            head = octet * OCT + 2 * pair
            tile = jnp.where(lanes < SLOT, gathered(head), gathered(head + 1))
            for window in range(WINDOWS):
                bias_ref[window, octet, pair * SLOT : (pair + 1) * SLOT, :] = tile + masks[window]


MESH = pl.DeviceIdType.MESH


def flipped(bit, by):
    return bit + by - 2 * bit * by


class Place:
    def __init__(self, ndp, nt):
        self.ndp, self.nt = ndp, nt
        self.nz = ndp // 2
        self.dp, self.t = lax.axis_index("dp"), lax.axis_index("tensor")
        self.z, self.y = self.dp // 2, self.dp % 2
        self.x, self.c = self.t // 2, self.t % 2

    def up(self, k):
        return lax.rem(self.z + k, self.nz)

    def down(self, k):
        return lax.rem(self.z + self.nz - k, self.nz)

    def device(self, z=None, y=None, x=None, c=None):
        z, y = self.z if z is None else z, self.y if y is None else y
        x, c = self.x if x is None else x, self.c if c is None else c
        return {"dp": z * 2 + y, "tensor": x * 2 + c}

    def block(self, z, y, x, c):
        return (x * 2 + c) * self.ndp + z * 2 + y

    def across(self, c, a, b):
        return flipped(self.y, c * a + (1 - c) * b), flipped(self.x, (1 - c) * a + c * b)

    def chip(self, c, a, b):
        y, x = self.across(c, a, b)
        return self.device(y=y, x=x)

    def bit_partner(self, b):
        size = 2**b
        return self.z + size * (1 - 2 * lax.rem(self.z // size, 2))

    def greet(self):
        others = [self.device(c=1 - self.c), self.device(x=1 - self.x)]
        others += [self.device(x=1 - self.x, c=1 - self.c), self.device(y=1 - self.y)]
        others += [self.device(z=self.up(k)) for k in range(1, self.nz)]
        barrier = pltpu.get_barrier_semaphore()
        for other in others:
            pl.semaphore_signal(barrier, inc=1, device_id=other, device_id_type=MESH)
        pl.semaphore_wait(barrier, len(others))


def remote(src, dst, send_sem, recv_sem, device):
    return pltpu.make_async_remote_copy(
        src_ref=src,
        dst_ref=dst,
        send_sem=send_sem,
        recv_sem=recv_sem,
        device_id=device,
        device_id_type=MESH,
    )


class Gather:
    def __init__(self, place, slabs, outs, scratch):
        count = len(slabs)
        self.place, self.slabs, self.outs, self.count = place, slabs, outs, count
        self.lows = scratch[:count]
        self.send_sem, self.recv_sem, self.local_sem = scratch[count:]

    @staticmethod
    def scratch(shapes, n):
        messages = len(shapes) * (n - 1)
        return [pltpu.VMEM(s, BF16) for s in shapes] + [
            pltpu.SemaphoreType.DMA((messages,)),
            pltpu.SemaphoreType.DMA((messages,)),
            pltpu.SemaphoreType.DMA((len(shapes),)),
        ]

    def copy(self, stage, m, a, b, k):
        place, nz = self.place, self.place.nz
        order = 1 - place.c
        base = {"z": -1, "p": nz - 1, "q": 2 * nz - 1, "c": 4 * nz - 1}[stage]
        at = m * (8 * nz - 1) + base + (b * 2 + a) * nz + k
        y, x = place.across(order, a, b)
        where = place.block(place.down(k), y, x, place.c)
        device = {
            "p": lambda: place.chip(order, 1, 0),
            "q": lambda: place.chip(order, 0, 1),
            "c": lambda: place.device(c=1 - place.c),
            "z": lambda: place.device(z=place.up(k)),
        }[stage]()
        if stage == "z":
            where = place.block(place.z, place.y, place.x, place.c)
        mine = stage == "z" or (a, b, k) == (0, 0, 0)
        src = self.lows[m] if mine else self.outs[m].at[where]
        return remote(src, self.outs[m].at[where], self.send_sem.at[at], self.recv_sem.at[at], device)

    def local(self, m):
        place = self.place
        where = place.block(place.z, place.y, place.x, place.c)
        return pltpu.make_async_copy(self.lows[m], self.outs[m].at[where], self.local_sem.at[m])

    def send(self, stage, a, b, k):
        for m in range(self.count):
            self.copy(stage, m, a, b, k).start()

    def wait(self, stage, a, b, k):
        for m in range(self.count):
            self.copy(stage, m, a, b, k).wait_recv()

    def column(self, k):
        if k:
            self.wait("z", 0, 0, k)
        self.send("p", 0, 0, k)
        self.send("q", 0, 0, k)
        self.send("c", 0, 0, k)

    def first(self, k):
        self.wait("p", 0, 0, k)
        self.send("q", 1, 0, k)
        self.send("c", 1, 0, k)

    def second(self, a, k):
        self.wait("q", a, 0, k)
        self.send("c", a, 1, k)

    def round(self):
        return range(self.place.nz)

    def begin(self):
        for slab, low in zip(self.slabs, self.lows):
            low[...] = slab[...].astype(BF16)
        for m in range(self.count):
            self.local(m).start()
        for k in self.round()[1:]:
            self.send("z", 0, 0, k)

    def end(self):
        everything = [("z", 0, 0, k) for k in self.round()[1:]]
        everything += [("p", 0, 0, k) for k in self.round()]
        everything += [("q", a, 0, k) for a in range(2) for k in self.round()]
        last = [("c", a, b, k) for b in range(2) for a in range(2) for k in self.round()]
        for key in last:
            self.wait(*key)
        for m in range(self.count):
            self.local(m).wait()
            for stage, a, b, k in everything + last:
                self.copy(stage, m, a, b, k).wait_send()

    def at_once(self):
        self.place.greet()
        self.begin()
        self.column(0)
        self.spread()
        self.end()

    def spread(self):
        for k in self.round()[1:]:
            self.column(k)
            self.first(k - 1)
        self.first(self.place.nz - 1)
        for a in range(2):
            for k in self.round():
                self.second(a, k)


class Reduce:
    def __init__(self, place, grads, scratch):
        count = len(grads)
        self.place, self.grads, self.count = place, grads, count
        self.own, self.from_core, self.from_p, self.from_q, self.from_z = (
            scratch[i * count : (i + 1) * count] for i in range(5)
        )
        self.send_sem, self.recv_sem, self.local_sem = scratch[5 * count :]

    @staticmethod
    def scratch(rows, n):
        nz, count = n // 8, len(rows)
        shapes = []
        for lead in ((2, 2, nz), (2, 2, nz), (2, nz), (nz,), (nz - 1,)):
            shapes += [pltpu.VMEM(lead + (r, D), BF16) for r in rows]
        return shapes + [
            pltpu.SemaphoreType.DMA((count * (8 * nz - 1),)),
            pltpu.SemaphoreType.DMA((count * (8 * nz - 1),)),
            pltpu.SemaphoreType.DMA((count * 4 * nz,)),
        ]

    def ks(self):
        return list(range(1, self.place.nz)) + [0]

    def copy(self, stage, m, a, b, k):
        place, nz = self.place, self.place.nz
        base = {"c": 0, "p": 4 * nz, "q": 6 * nz, "z": 7 * nz - 1}[stage]
        at = m * (8 * nz - 1) + base + {"c": (a * 2 + b) * nz + k, "p": b * nz + k}.get(stage, k)
        sems = self.send_sem.at[at], self.recv_sem.at[at]
        if stage == "c":
            y, x = place.across(1 - place.c, a, b)
            where = place.block(place.up(k), y, x, 1 - place.c)
            return remote(
                self.grads[m].at[where], self.from_core[m].at[a, b, k], *sems, place.device(c=1 - place.c)
            )
        src = self.own[m].at[a, b, k]
        if stage == "p":
            return remote(src, self.from_p[m].at[b, k], *sems, place.chip(place.c, 1, 0))
        if stage == "q":
            return remote(src, self.from_q[m].at[k], *sems, place.chip(place.c, 0, 1))
        return remote(src, self.from_z[m].at[k - 1], *sems, place.device(z=place.up(k)))

    def local(self, m, a, b, k):
        place, nz = self.place, self.place.nz
        y, x = place.across(place.c, a, b)
        where = place.block(place.up(k), y, x, place.c)
        at = m * 4 * nz + (a * 2 + b) * nz + k
        return pltpu.make_async_copy(
            self.grads[m].at[where], self.own[m].at[a, b, k], self.local_sem.at[at]
        )

    def order(self):
        return [(a, b, k) for a in (1, 0) for b in (1, 0) for k in self.ks()]

    def begin(self):
        for a, b, k in self.order():
            for m in range(self.count):
                self.copy("c", m, a, b, k).start()
        for a, b, k in self.order():
            for m in range(self.count):
                self.local(m, a, b, k).start()

    def value(self, m, a, b, k):
        self.local(m, a, b, k).wait()
        self.copy("c", m, a, b, k).wait_recv()
        value = self.own[m][a, b, k].astype(F32) + self.from_core[m][a, b, k].astype(F32)
        if a == 0:
            self.copy("p", m, 1, b, k).wait_recv()
            value = value + self.from_p[m][b, k].astype(F32)
            if b == 0:
                self.copy("q", m, 0, 1, k).wait_recv()
                value = value + self.from_q[m][k].astype(F32)
        return value

    def pass_on(self, a, b, between=None):
        stage = "p" if a else "q" if b else "z"
        waiting = []
        for k in self.ks():
            if stage == "z" and k == 0:
                continue
            for m in range(self.count):
                self.own[m][a, b, k] = self.value(m, a, b, k).astype(BF16)
            for copy in waiting:
                copy.start()
            waiting = [self.copy(stage, m, a, b, k) for m in range(self.count)]
        if between is not None:
            between()
        for copy in waiting:
            copy.start()

    def totals(self):
        values = [self.value(m, 0, 0, 0) for m in range(self.count)]
        for m in range(self.count):
            for k in self.ks()[:-1]:
                self.copy("z", m, 0, 0, k).wait_recv()
                values[m] = values[m] + self.from_z[m][k - 1].astype(F32)
        return values

    def end(self):
        for m in range(self.count):
            for a, b, k in self.order():
                self.copy("c", m, a, b, k).wait_send()
                if a:
                    self.copy("p", m, a, b, k).wait_send()
                elif b:
                    self.copy("q", m, a, b, k).wait_send()
                elif k:
                    self.copy("z", m, a, b, k).wait_send()


class Share:
    def __init__(self, place, core, fresh, bundle, scratch):
        self.place, self.core, self.fresh, self.bundle = place, core, fresh, bundle
        self.send_sem, self.recv_sem, self.near_sem = scratch

    @staticmethod
    def scratch(n, nt):
        messages = 2 + (nt - 1) + (n // 8 - 1) + n // 8
        return [
            pltpu.SemaphoreType.DMA((messages,)),
            pltpu.SemaphoreType.DMA((messages,)),
            pltpu.SemaphoreType.DMA,
        ]

    def near(self, i):
        place = self.place
        return pltpu.make_async_copy(self.fresh.at[i], self.bundle.at[place.dp, place.t], self.near_sem)

    def handed(self, i, label):
        place = self.place
        to = self.core + 2 * i
        return remote(
            self.fresh.at[i],
            self.bundle.at[place.dp, place.t],
            self.send_sem.at[i],
            self.recv_sem.at[label],
            {"dp": place.dp, "tensor": to},
        )

    def each(self, then):
        for i in range(2):
            to = self.core + 2 * i

            @pl.when(self.place.t != to)
            def _(i=i, to=to):
                then(self.handed(i, lax.rem(self.place.t + self.place.nt - to, self.place.nt) - 1))

    def hand(self):
        self.each(lambda copy: copy.start())
        for i in range(2):

            @pl.when(self.place.t == self.core + 2 * i)
            def _(i=i):
                self.near(i).start()

    def move(self, stage, k):
        place, nz = self.place, self.place.nz
        at = self.place.nt - 1 + (k - 1 if stage == "z" else nz - 1 + k)
        sems = self.send_sem.at[2 + at], self.recv_sem.at[at]
        if stage == "z":
            where, device = place.dp, place.device(z=place.up(k))
        else:
            where, device = place.down(k) * 2 + place.y, place.device(y=1 - place.y)
        return remote(self.bundle.at[where], self.bundle.at[where], *sems, device)

    def mine(self):
        return pl.when(self.place.c == self.core)

    def along_z(self):
        @self.mine()
        def _():
            self.near(0).wait()
            for label in range(self.place.nt - 1):
                self.handed(0, label).wait_recv()
            for k in range(1, self.place.nz):
                self.move("z", k).start()
            self.move("y", 0).start()

    def along_y(self):
        @self.mine()
        def _():
            for k in range(1, self.place.nz):
                self.move("z", k).wait_recv()
                self.move("y", k).start()

    def end(self):
        self.each(lambda copy: copy.wait_send())

        @self.mine()
        def _():
            for k in range(self.place.nz):
                self.move("y", k).wait_recv()
            for k in range(self.place.nz):
                self.move("y", k).wait_send()
                if k:
                    self.move("z", k).wait_send()


def renew(totals, momenta, grad_out, fresh, images):
    values = []
    for total, momentum, out in zip(totals, momenta, grad_out):
        grad = total / images
        out[...] = grad
        values.append(MOMENTUM * momentum[...] + grad)
    for value, ref in zip(values, fresh):
        ref[0 : value.shape[0], :] = value.astype(BF16)


def gather_kernel(ndp, nt, count, *refs):
    Gather(Place(ndp, nt), refs[:count], refs[count : 2 * count], refs[2 * count :]).at_once()


def gather_weights(slabs, ndp, nt, collective_id):
    count, n = len(slabs), ndp * nt
    gathered = pl.pallas_call(
        functools.partial(gather_kernel, ndp, nt, count),
        out_shape=tuple(shape_of((n,) + s.shape, BF16) for s in slabs),
        in_specs=[pl.BlockSpec(memory_space=pltpu.VMEM)] * count,
        out_specs=tuple(pl.BlockSpec(memory_space=pl.ANY) for _ in slabs),
        scratch_shapes=Gather.scratch([s.shape for s in slabs], n),
        compiler_params=pltpu.CompilerParams(
            collective_id=collective_id, has_side_effects=True, vmem_limit_bytes=VMEM_LIMIT
        ),
        name="gather_weights",
    )(*slabs)
    return tuple(g.reshape(n * s.shape[0], D) for g, s in zip(gathered, slabs))


SMALL_ROWS = 32
TABLE_ROW = 16


class SmallSum:
    def __init__(self, place, values, arrived, send_sem, recv_sem):
        self.values, self.arrived = values, arrived
        self.send_sem, self.recv_sem = send_sem, recv_sem
        self.steps = [
            place.device(c=1 - place.c),
            place.device(x=1 - place.x),
            place.device(y=1 - place.y),
        ]
        bit = 0
        while 2**bit < place.nz:
            self.steps.append(place.device(z=place.bit_partner(bit)))
            bit += 1
        self.done = 0

    def copy(self, i):
        return remote(
            self.values.at[i], self.arrived.at[i], self.send_sem.at[i], self.recv_sem.at[i], self.steps[i]
        )

    def begin(self):
        self.copy(0).start()

    def step(self):
        i = self.done
        if i < len(self.steps):
            self.copy(i).wait_recv()
            self.values[i + 1] = self.values[i] + self.arrived[i]
            self.done += 1

    def go_on(self):
        if 0 < self.done < len(self.steps):
            self.copy(self.done).start()

    def end(self):
        while self.done < len(self.steps):
            self.step()
            self.go_on()
        for i in range(len(self.steps)):
            self.copy(i).wait_send()
        return self.values[len(self.steps)]


def padded(rows):
    return -(-max(rows) // 16) * 16


def pack_small(small, sums1, sums2, head, hidden, table):
    small[0] = jnp.zeros_like(small[0])
    small[0, 0:1, :] = sums1[0:1, :]
    small[0, 1:2, :] = sums2[0:1, :]
    small[0, 2:3, :] = sums1[1:2, :]
    small[0, 3:6, :] = sums2[1:4, :]
    small[0, 6:8, :] = head[...]
    for i in range(hidden.shape[1] // D):
        small[0, 8 + i : 9 + i, :] = hidden[0:1, i * D : (i + 1) * D]
    small[0, TABLE_ROW : TABLE_ROW + table.shape[0], 0 : table.shape[1]] = table[...]


def newton_schulz_kernel(nt, heights, first_ref, second_ref, landed0, landed1, g_scr, x_scr, a_scr, y_scr, back, sem, send_sem, recv_sem):
    first, second, third = QUINTIC
    chunk = 512
    t, dp = lax.axis_index("tensor"), lax.axis_index("dp")
    core = t % 2
    sources = (first_ref, second_ref)
    landed = (landed0, landed1)
    barrier = pltpu.get_barrier_semaphore()
    for d in range(1, nt):
        other = {"dp": dp, "tensor": lax.rem(t + d, nt)}
        pl.semaphore_signal(barrier, inc=1, device_id=other, device_id_type=MESH)
    for which, ref in enumerate(sources):

        @pl.when(core == which)
        def _(ref=ref):
            copy = pltpu.make_async_copy(ref, g_scr.at[0 : ref.shape[0]], sem)
            copy.start()
            copy.wait()

    chunks = jnp.where(core == 0, first_ref.shape[0] // chunk, second_ref.shape[0] // chunk)

    def low(values):
        return values.astype(BF16)

    def gram(src_ref):
        a_scr[...] = jnp.zeros_like(a_scr)

        def add(at, carry):
            part = src_ref[pl.ds(pl.multiple_of(at * chunk, chunk), chunk), :]
            a_scr[...] += dot_tn(part, part)
            return carry

        lax.fori_loop(0, chunks, add, 0)
        return a_scr[...]

    def advance(src_ref, factor, scale):
        factor = low(factor)

        def step(at, carry):
            at = pl.ds(pl.multiple_of(at * chunk, chunk), chunk)
            x_scr[at, :] = low(dot_nn(src_ref[at, :], factor) * scale)
            return carry

        lax.fori_loop(0, chunks, step, 0)

    def bend(a):
        return second * a + third * dot_nn(low(a), low(a))

    diagonal = lax.broadcasted_iota(jnp.int32, (D, D), 0) == lax.broadcasted_iota(jnp.int32, (D, D), 1)

    def two_turns(a):
        b = bend(a)
        q = b + jnp.where(diagonal, first, 0.0)
        r = first * a + dot_nn(low(a), low(b))
        a = first * r + dot_nn(low(r), low(b))
        b = bend(a)
        return first * q + dot_nn(low(b), low(q))

    a = gram(g_scr)
    scale = 1.0 / (jnp.sqrt(jnp.sum(jnp.where(diagonal, a, 0.0))) + MUON_EPSILON)
    advance(g_scr, two_turns(a * scale * scale), scale)
    q = two_turns(gram(x_scr))
    for which, ref in enumerate(sources):

        @pl.when(core == which)
        def _(ref=ref):
            mine = nt * heights[which]
            at = pl.ds(pl.multiple_of(dp * mine, mine), mine)
            y_scr[0:mine, :] = dot_nn(x_scr[at, :], low(q))

    advance(x_scr, q, 1.0)
    b = bend(gram(x_scr))
    here = y_scr[...]
    back[...] = low(first * here + dot_nn(low(here), low(b)))
    pl.semaphore_wait(barrier, nt - 1)

    def copy(which, d):
        to = lax.rem(t + d, nt)
        height = heights[which]
        return remote(
            back.at[pl.ds(pl.multiple_of(to * height, height), height)],
            landed[which].at[t // 2],
            send_sem.at[d - 1],
            recv_sem.at[d - 1],
            {"dp": dp, "tensor": to},
        )

    for which in range(2):

        @pl.when(core == which)
        def _(which=which):
            for d in range(1, nt):
                copy(which, d).start()
            height = heights[which]
            landed[which][t // 2] = back[pl.ds(pl.multiple_of(t * height, height), height), :]

    for d in range(1, nt):
        for which in range(2):

            @pl.when(lax.rem(t + nt - d, nt) % 2 == which)
            def _(d=d, which=which):
                copy(which, d).wait_recv()

    for which in range(2):

        @pl.when(core == which)
        def _(which=which):
            for d in range(1, nt):
                copy(which, d).wait_send()


def newton_schulz(bundles, collective_id):
    ndp, nt = bundles[0].shape[:2]
    heights = tuple(b.shape[2] for b in bundles)
    rows = [ndp * nt * h for h in heights]
    tall = max(rows)
    any_, vmem = pl.BlockSpec(memory_space=pl.ANY), pl.BlockSpec(memory_space=pltpu.VMEM)
    return pl.pallas_call(
        functools.partial(newton_schulz_kernel, nt, heights),
        out_shape=tuple(shape_of((nt // 2, h, D), BF16) for h in heights),
        in_specs=[any_, any_],
        out_specs=(vmem, vmem),
        scratch_shapes=[
            pltpu.VMEM((tall, D), BF16),
            pltpu.VMEM((tall, D), BF16),
            pltpu.VMEM((D, D), F32),
            pltpu.VMEM((tall // ndp, D), F32),
            pltpu.VMEM((tall // ndp, D), BF16),
            pltpu.SemaphoreType.DMA,
            pltpu.SemaphoreType.DMA((nt - 1,)),
            pltpu.SemaphoreType.DMA((nt - 1,)),
        ],
        compiler_params=pltpu.CompilerParams(
            collective_id=collective_id, has_side_effects=True, vmem_limit_bytes=VMEM_LIMIT
        ),
        name="newton_schulz",
    )(*(b.reshape(r, D) for b, r in zip(bundles, rows)))


def finish_kernel(nt, rates, *refs):
    refs = list(refs)

    def take(n):
        taken = refs[:n]
        del refs[:n]
        return taken

    landed, (total,) = take(2), take(1)
    grads, momenta, weights = take(nt), take(nt), take(nt)
    small_par, small_mom = take(5), take(5)
    grad_out, new_out, mom_out = take(nt), take(nt), take(nt)
    small_grad_out, small_new_out, small_mom_out = take(5), take(5), take(5)
    for m in range(nt):
        grad = grads[m][...]
        grad_out[m][...] = grad
        mom_out[m][...] = MOMENTUM * momenta[m][...] + grad
        new_out[m][...] = weights[m][...] - rates[m] * landed[m % 2][m // 2, 0 : grad.shape[0], :].astype(F32)

    def small_update(i, at, grad):
        small_grad_out[i][at] = grad
        grad = MOMENTUM * small_mom[i][at] + grad
        small_mom_out[i][at] = grad
        small_new_out[i][at] = small_par[i][at] - VECTOR_RATE * grad

    for i, (low, high) in enumerate(((0, 2), (2, 6), (6, 8))):
        small_update(i, (slice(None), slice(None)), total[low:high, :])
    for i in range(small_par[3].shape[1] // D):
        small_update(3, (slice(0, 1), slice(i * D, (i + 1) * D)), total[8 + i : 9 + i, :])
    heads, rows = small_par[4].shape
    small_update(4, (slice(None), slice(None)), total[TABLE_ROW : TABLE_ROW + heads, 0:rows])


def finish(landed, total, grads, momenta, weights, small_params, small_moms, rates):
    nt = len(grads)
    like = lambda arrays: tuple(shape_of(a.shape, F32) for a in arrays)
    return pl.pallas_call(
        functools.partial(finish_kernel, nt, rates),
        out_shape=like(grads) * 3 + like(small_params) * 3,
        compiler_params=pltpu.CompilerParams(vmem_limit_bytes=VMEM_LIMIT),
        name="finish",
    )(*landed, total, *grads, *momenta, *weights, *small_params, *small_moms)


def key_by_query(index_ref, idx_scr):
    idx_scr[...] = jnp.zeros_like(idx_scr)
    idx_scr[0:SPOTS, 0:SPOTS] = index_ref[...].astype(F32)
    index = idx_scr[...].T[0:SLOT, :]
    return jnp.where(lane_iota(SLOT) < SLOT, index, pltpu.roll(index, SLOT, 1))


def table_sums(dbias_ref, index_ref, table_scr, idx_scr, turned_idx):
    turned_idx[...] = key_by_query(index_ref, idx_scr)
    table_scr[...] = jnp.zeros_like(table_scr)
    lanes = lane_iota(PAIRS)
    entries = lax.broadcasted_iota(jnp.int32, (2 * LANES, LANES), 0).astype(F32)
    count = OCTS * OCT

    def one_key(key, carry):
        picks = (entries == turned_idx[pl.ds(key, 1), :]).astype(F32).astype(BF16)
        values = []
        for octet in range(OCTS):
            pairs = dbias_ref[octet, pl.ds(key, PAIRS, SLOT), :]
            values += [jnp.where(lanes < SLOT, pairs, 0.0), jnp.where(lanes < SLOT, 0.0, pairs)]
        values = jnp.concatenate(values, axis=0)
        parts = []
        for _ in range(3):
            low = values.astype(BF16).astype(F32)
            parts.append(low)
            values = values - low
        sums = dot_nt(jnp.concatenate(parts, axis=0).astype(BF16), picks)
        table_scr[...] += sums[0:count] + sums[count : 2 * count] + sums[2 * count :]
        return carry

    lax.fori_loop(0, SPOTS, one_key, 0)
    sums = table_scr[...]
    for octet in range(OCTS):
        for head in range(OCT):
            at = octet * OCT + head % 2 * PAIRS + head // 2
            table_scr[octet * OCT + head : octet * OCT + head + 1, :] = sums[at : at + 1]


def attention_forward_kernel(ndp, nt, steps, fused, *refs):
    refs = list(refs)

    def take(n):
        taken = refs[:n]
        del refs[:n]
        return taken

    x_ref, gain_ref, shift_ref, qkvb_ref, table_ref, index_ref, region_ref = take(7)
    slabs, (wqkv_in,) = take(3), take(1)
    xs_ref, a1_ref, qkv_ref, p_ref, o_ref = take(5)
    gathered = take(3)
    wqkv_all = take(1) if fused else None
    bias_scr, idx_scr, tab_scr, pair_scr, side_scr, a1_scr = take(6)
    place = Place(ndp, nt)
    rest = Gather(place, slabs, gathered, take(6))
    step, last = pl.program_id(0), pl.num_programs(0) - 1
    if fused:
        qkv_gather = Gather(place, (wqkv_in,), wqkv_all, take(4))
        wqkv_ref, load_sem = take(2)
    else:
        wqkv_ref = wqkv_in

    @pl.when(step == 0)
    def _():
        place.greet()
        if fused:
            qkv_gather.begin()
            qkv_gather.column(0)

    @pl.when(step < steps)
    def _():
        xs_ref[...] = jnp.zeros_like(xs_ref)
        into_slots(x_ref, xs_ref)
        white, _ = whiten(xs_ref[...])
        a1 = (white * gain_ref[0:1, :] + shift_ref[0:1, :]).astype(BF16)
        a1_ref[...] = a1
        a1_scr[pl.ds(pl.multiple_of(step * STEP_SLOTS, STEP_SLOTS), STEP_SLOTS), :] = a1

    @pl.when(step == 0)
    def _():
        if fused:
            for k in qkv_gather.round()[1:]:
                qkv_gather.column(k)
        build_bias(region_ref, index_ref, table_ref, bias_scr, idx_scr, tab_scr)
        pair_scr[...] = pair_mask()
        side_scr[...] = side_mask()

    if fused:

        @pl.when(step == 1)
        def _():
            for k in qkv_gather.round():
                qkv_gather.first(k)

        @pl.when(step == 2)
        def _():
            for a in range(2):
                for k in qkv_gather.round():
                    qkv_gather.second(a, k)

    @pl.when(step == 2)
    def _():
        rest.begin()
        rest.column(0)

    @pl.when(step == steps - 1)
    def _():
        if fused:
            qkv_gather.end()
            copies = []
            for i in range(ndp * nt):
                rows = wqkv_in.shape[0]
                copies.append(
                    pltpu.make_async_copy(
                        wqkv_all[0].at[i], wqkv_ref.at[i * rows : (i + 1) * rows], load_sem.at[i]
                    )
                )
                copies[i].start()
            for copy in copies:
                copy.wait()

    @pl.when(step >= steps)
    def _():
        at = pl.multiple_of((step - steps) * STEP_SLOTS, STEP_SLOTS)
        a1 = a1_scr[pl.ds(at, STEP_SLOTS), :]
        scale = HEAD ** (-0.5)
        for half in range(2):
            columns = 3 * PART * GROUPS // 2
            u = dot_nt(a1, wqkv_ref[half * columns : (half + 1) * columns, :])
            for inner in range(GROUPS // 2):
                group = half * (GROUPS // 2) + inner
                for part in range(3):
                    piece = u[:, (inner * 3 + part) * PART : (inner * 3 + part + 1) * PART]
                    if part == 0:
                        piece = (piece + qkvb_ref[0:1, group * PART : (group + 1) * PART]) * scale
                    elif part == 2:
                        piece = piece + qkvb_ref[1:2, group * PART : (group + 1) * PART]
                    lanes = part * D + group * PART
                    qkv_ref[:, lanes : lanes + PART] = piece.astype(BF16)

    real_query = (lane_iota(1) % SLOT < SPOTS).astype(F32)
    first_side = lax.broadcasted_iota(jnp.int32, (SLOT, OCT_W), 1) // HEAD % 2 == 0

    def one_window(at, carry):
        rows = pl.ds(pl.multiple_of(at * SLOT, SLOT), SLOT)
        for octet in range(OCTS):
            q = qkv_ref[rows, octet * OCT_W : (octet + 1) * OCT_W]
            k = qkv_ref[rows, D + octet * OCT_W : D + (octet + 1) * OCT_W]
            v = qkv_ref[rows, 2 * D + octet * OCT_W : 2 * D + (octet + 1) * OCT_W]
            scores = dot_nt(spread(k, pair_scr), spread(q, side_scr)) + bias_scr[lax.rem(at, WINDOWS), octet]
            probs = []
            for pair in range(PAIRS):
                part = scores[pair * SLOT : (pair + 1) * SLOT]
                grown = jnp.exp(part - jnp.max(part, axis=0, keepdims=True))
                probs.append(grown * (real_query / jnp.sum(grown, axis=0, keepdims=True)))
            probs = jnp.concatenate(probs, axis=0)
            p_ref[pl.ds(pl.multiple_of((at * OCTS + octet) * ROWS_S, ROWS_S), ROWS_S), :] = probs.astype(BF16)
            mixed = dot_nn(turned(probs).astype(BF16), spread(v, pair_scr))
            o_ref[rows, octet * OCT_W : (octet + 1) * OCT_W] = by_side(mixed, first_side).astype(BF16)
        return carry

    half_loop = STEP_IMAGES * WINDOWS // 2

    @pl.when(step >= steps)
    def _():
        lax.fori_loop(0, half_loop, one_window, 0, unroll=4)

    @pl.when(step == steps + 1)
    def _():
        for k in rest.round()[1:]:
            rest.column(k)

    @pl.when(step == steps + 2)
    def _():
        for k in rest.round():
            rest.first(k)

    @pl.when(step == last)
    def _():
        for a in range(2):
            for k in rest.round():
                rest.second(a, k)

    @pl.when(step >= steps)
    def _():
        lax.fori_loop(half_loop, 2 * half_loop, one_window, 0, unroll=4)

    @pl.when(step == last)
    def _():
        rest.end()


def mlp_kernel(
    xs_ref,
    o_ref,
    e_ref,
    wproj_ref,
    w1_ref,
    w2_ref,
    gain_ref,
    shift_ref,
    hb_ref,
    out_ref,
    dy_ref,
    g1_ref,
    g2_ref,
    gproj_ref,
    hsum_ref,
    sums_ref,
    acc1,
    acc2,
    accp,
    m_scr,
    da_scr,
    a2_scr,
    e_scr,
    slot_scr,
    y_ref,
):
    step = pl.program_id(0)

    @pl.when(step == 0)
    def _():
        acc1[...] = jnp.zeros_like(acc1)
        acc2[...] = jnp.zeros_like(acc2)
        accp[...] = jnp.zeros_like(accp)
        hsum_ref[...] = jnp.zeros_like(hsum_ref)
        sums_ref[...] = jnp.zeros_like(sums_ref)

    slot_scr[...] = xs_ref[...] + dot_nn(o_ref[...], wproj_ref[...]) + shift_ref[2:3, :]
    out_of_slots(slot_scr, y_ref)
    white, inverse = whiten(y_ref[...])
    a2_scr[...] = (white * gain_ref[1:2, :] + shift_ref[1:2, :]).astype(BF16)
    e_scr[...] = e_ref[...].astype(BF16)
    m_scr[...] = jnp.zeros_like(m_scr)
    da_scr[...] = jnp.zeros_like(da_scr)
    root = math.sqrt(2.0 / math.pi)
    width = 512

    def chunk(c, carry):
        at = pl.ds(pl.multiple_of(c * width, width), width)
        w1, w2 = w1_ref[at, :], w2_ref[at, :]
        a2, e = a2_scr[...], e_scr[...]
        z = dot_nt(a2, w1) + hb_ref[0:1, at]
        square = z * z
        t = jnp.tanh(z * (root + (root * 0.044715) * square))
        half = 0.5 * z
        f = (half + half * t).astype(BF16)
        slope = 0.5 + 0.5 * t + half * (1.0 - t * t) * (root + (3.0 * root * 0.044715) * square)
        dz = dot_nt(e, w2) * slope
        hsum_ref[0:1, at] += jnp.sum(dz, axis=0, keepdims=True)
        dz = dz.astype(BF16)
        m_scr[...] += dot_nn(f, w2)
        da_scr[...] += dot_nn(dz, w1)
        acc2[at, :] += dot_tn(f, e)
        acc1[at, :] += dot_tn(dz, a2)
        return carry

    lax.fori_loop(0, w1_ref.shape[0] // width, chunk, 0, unroll=4)
    white, inverse = whiten(y_ref[...])
    out_ref[...] = y_ref[...] + m_scr[...] + shift_ref[3:4, :]
    da = da_scr[...]
    t2 = da * gain_ref[1:2, :]
    dy = e_ref[...] + inverse * (t2 - row_mean(t2) - white * row_mean(t2 * white))
    m_scr[...] = dy
    dy_ref[...] = jnp.zeros_like(dy_ref)
    into_slots(m_scr, dy_ref)
    accp[...] += dot_tn(o_ref[...], dy_ref[...].astype(BF16))
    sums_ref[0:1, :] += jnp.sum(da * white, axis=0, keepdims=True)
    sums_ref[1:2, :] += jnp.sum(da, axis=0, keepdims=True)
    sums_ref[2:3, :] += jnp.sum(dy, axis=0, keepdims=True)
    sums_ref[3:4, :] += jnp.sum(e_ref[...], axis=0, keepdims=True)

    @pl.when(step == pl.num_programs(0) - 1)
    def _():
        g1_ref[...] = acc1[...].astype(BF16)
        g2_ref[...] = acc2[...].astype(BF16)
        gproj_ref[...] = accp[...].astype(BF16)


def attention_backward_kernel(ndp, nt, images, steps, *refs):
    refs = list(refs)

    def take(n):
        taken = refs[:n]
        del refs[:n]
        return taken

    dy_ref, xs_ref, a1_ref, qkv_ref, p_ref, wqkv_ref, wproj_ref, gain_ref, index_ref = take(9)
    hidden_ref, sums2_ref = take(2)
    grads, momenta, (qkv_momentum,) = take(3), take(3), take(1)
    (gin_ref,) = take(1)
    slabs, (qkv_slab,) = take(3), take(1)
    bundle0, bundle1, small_out = take(3)
    accq, gq, do_scr, du_scr, pair_scr, side_scr, g_scr, dbias_ref, hsum_ref, sums_ref = take(10)
    idx_scr, turned_idx, table_scr, fresh0, fresh1 = take(5)
    small, small_in, small_send, small_recv = take(4)
    place = Place(ndp, nt)
    step, last = pl.program_id(0), pl.num_programs(0) - 1
    share0 = Share(place, 0, fresh0, bundle0, take(3))
    share1 = Share(place, 1, fresh1, bundle1, take(3))
    early = Reduce(place, grads, take(18))
    late = Reduce(place, (gq,), take(8))
    tiny = SmallSum(place, small, small_in, small_send, small_recv)

    @pl.when(step == 0)
    def _():
        place.greet()
        early.begin()
        fresh0[...] = jnp.zeros_like(fresh0)
        fresh1[...] = jnp.zeros_like(fresh1)
        pair_scr[...] = pair_mask()
        side_scr[...] = side_mask()
        accq[...] = jnp.zeros_like(accq)
        dbias_ref[...] = jnp.zeros_like(dbias_ref)
        hsum_ref[...] = jnp.zeros_like(hsum_ref)
        sums_ref[...] = jnp.zeros_like(sums_ref)

    first_row = pl.multiple_of(lax.rem(step, steps) * STEP_SLOTS, STEP_SLOTS)
    step_rows = pl.ds(first_row, STEP_SLOTS)

    @pl.when(step < steps)
    def _():
        do_scr[...] = dot_nt(dy_ref[...].astype(BF16), wproj_ref[...]).astype(BF16)

    scale = HEAD ** (-0.5)
    first_side = lax.broadcasted_iota(jnp.int32, (SLOT, OCT_W), 1) // HEAD % 2 == 0

    def one_window(at, carry):
        rows = pl.ds(pl.multiple_of(at * SLOT, SLOT), SLOT)
        out_rows = pl.ds(pl.multiple_of(first_row + at * SLOT, SLOT), SLOT)
        for octet in range(OCTS):
            q = qkv_ref[rows, octet * OCT_W : (octet + 1) * OCT_W]
            k = qkv_ref[rows, D + octet * OCT_W : D + (octet + 1) * OCT_W]
            v = qkv_ref[rows, 2 * D + octet * OCT_W : 2 * D + (octet + 1) * OCT_W]
            do = do_scr[rows, octet * OCT_W : (octet + 1) * OCT_W]
            probs = p_ref[pl.ds(pl.multiple_of((at * OCTS + octet) * ROWS_S, ROWS_S), ROWS_S), :]
            side_do = spread(do, side_scr)
            weighted = probs.astype(F32) * dot_nt(spread(v, pair_scr), side_do)
            ds = []
            for pair in range(PAIRS):
                part = slice(pair * SLOT, (pair + 1) * SLOT)
                total = jnp.sum(weighted[part], axis=0, keepdims=True)
                ds.append(weighted[part] - probs[part].astype(F32) * total)
            ds = jnp.concatenate(ds, axis=0)
            dbias_ref[octet] += ds
            dq = by_side(dot_nn(turned(ds).astype(BF16), spread(k, pair_scr)), first_side) * scale
            dk = by_pair(ds.astype(BF16), spread(q, side_scr))
            dv = by_pair(probs, side_do)
            lanes = slice(octet * OCT_W, (octet + 1) * OCT_W)
            hsum_ref[0:1, lanes] += jnp.sum(dq, axis=0, keepdims=True)
            hsum_ref[1:2, lanes] += jnp.sum(dv, axis=0, keepdims=True)
            for part, grad in enumerate((dq, dk, dv)):
                for inner in range(OCT_W // PART):
                    group = octet * (OCT_W // PART) + inner
                    at_col = (group * 3 + part) * PART
                    du_scr[out_rows, at_col : at_col + PART] = grad[
                        :, inner * PART : (inner + 1) * PART
                    ].astype(BF16)
        return carry

    half_loop = STEP_IMAGES * WINDOWS // 2

    @pl.when(step < steps)
    def _():
        lax.fori_loop(0, half_loop, one_window, 0, unroll=4)

    @pl.when(step == 2)
    def _():
        early.pass_on(0, 1)

    @pl.when(step == 3)
    def _():
        early.pass_on(0, 0)

    @pl.when(step < steps)
    def _():
        lax.fori_loop(half_loop, 2 * half_loop, one_window, 0, unroll=4)

    @pl.when(step == 0)
    def _():
        early.pass_on(1, 1)
        early.pass_on(1, 0)

    @pl.when(step < steps)
    def _():
        accq[...] += dot_tn(du_scr[step_rows, :], a1_ref[...])

    @pl.when(step == steps - 1)
    def _():
        rows = gq.shape[1]
        for i in range(gq.shape[0]):
            gq[i] = accq[i * rows : (i + 1) * rows, :].astype(BF16)
        late.begin()

    @pl.when(step >= steps)
    def _():
        white, inverse = whiten(xs_ref[...])
        da = dot_nn(du_scr[step_rows, :], wqkv_ref[...])
        t1 = da * gain_ref[0:1, :]
        g_scr[...] = dy_ref[...] + inverse * (t1 - row_mean(t1) - white * row_mean(t1 * white))
        out_of_slots(g_scr, gin_ref)
        sums_ref[0:1, :] += jnp.sum(da * white, axis=0, keepdims=True)
        sums_ref[1:2, :] += jnp.sum(da, axis=0, keepdims=True)

    @pl.when(step == steps)
    def _():
        late.pass_on(1, 1)
        late.pass_on(1, 0)

    @pl.when(step == steps + 1)
    def _():
        late.pass_on(0, 1)

    @pl.when(step == steps + 2)
    def _():
        late.pass_on(0, 0)
        renew(early.totals(), momenta, slabs, (fresh0.at[1], fresh1.at[0], fresh1.at[1]), images)
        share1.hand()

    @pl.when(step == last)
    def _():
        share1.along_z()
        table_sums(dbias_ref, index_ref, table_scr, idx_scr, turned_idx)
        pack_small(small, sums_ref, sums2_ref, hsum_ref, hidden_ref, table_scr)
        tiny.begin()
        renew(late.totals(), (qkv_momentum,), (qkv_slab,), (fresh0.at[0],), images)
        tiny.step()
        share0.hand()
        tiny.go_on()
        tiny.step()
        tiny.go_on()
        share0.along_z()
        share1.along_y()
        tiny.step()
        tiny.go_on()
        share0.along_y()
        small_out[...] = tiny.end() / images
        share1.end()
        share0.end()
        early.end()
        late.end()


def whole(shape):
    return pl.BlockSpec(shape, lambda i: (0,) * len(shape))


def rows_of(rows, columns):
    return pl.BlockSpec((rows, columns), lambda i: (i, 0))


def shape_of(shape, dtype):
    return jax.ShapeDtypeStruct(shape, dtype)


PARAMS = pltpu.CompilerParams(dimension_semantics=("arbitrary",), vmem_limit_bytes=VMEM_LIMIT)


def remote_params(collective_id):
    return pltpu.CompilerParams(
        dimension_semantics=("arbitrary",),
        vmem_limit_bytes=VMEM_LIMIT,
        collective_id=collective_id,
        has_side_effects=True,
    )


def attention_forward(
    tokens, gains, shifts, head_biases, table, index, regions, slabs, qkv_slab, ndp, nt, collective_ids
):
    n = ndp * nt
    steps = tokens.shape[0] // STEP_ROWS
    slots = steps * STEP_SLOTS
    fused = qkv_slab.shape[0] % 16 == 0
    if not fused:
        (qkv_slab,) = gather_weights((qkv_slab,), ndp, nt, collective_ids[1])
    early = lambda i: (jnp.minimum(i, steps - 1), 0)
    late = lambda i: (jnp.maximum(i - steps, 0), 0)
    any_ = pl.BlockSpec(memory_space=pl.ANY)
    gathered = tuple(slabs) + ((qkv_slab,) if fused else ())
    results = pl.pallas_call(
        functools.partial(attention_forward_kernel, ndp, nt, steps, fused),
        grid=(2 * steps,),
        out_shape=(
            shape_of((slots, D), F32),
            shape_of((slots, D), BF16),
            shape_of((slots, 3 * D), BF16),
            shape_of((slots * OCTS * PAIRS, LANES), BF16),
            shape_of((slots, D), BF16),
        )
        + tuple(shape_of((n,) + s.shape, BF16) for s in gathered),
        in_specs=[
            pl.BlockSpec((STEP_ROWS, D), early),
            whole(gains.shape),
            whole(shifts.shape),
            whole(head_biases.shape),
            whole(table.shape),
            whole(index.shape),
            pl.BlockSpec(memory_space=pltpu.SMEM),
        ]
        + [whole(s.shape) for s in slabs]
        + [whole(qkv_slab.shape)],
        out_specs=(
            pl.BlockSpec((STEP_SLOTS, D), early),
            pl.BlockSpec((STEP_SLOTS, D), early),
            pl.BlockSpec((STEP_SLOTS, 3 * D), late),
            pl.BlockSpec((STEP_SLOTS * OCTS * PAIRS, LANES), late),
            pl.BlockSpec((STEP_SLOTS, D), late),
        )
        + (any_,) * len(gathered),
        scratch_shapes=[
            pltpu.VMEM((WINDOWS, OCTS, ROWS_S, LANES), F32),
            pltpu.VMEM((LANES, LANES), F32),
            pltpu.VMEM((HEADS, 2 * LANES), F32),
            pltpu.VMEM((ROWS_S, OCT_W), BF16),
            pltpu.VMEM((2 * SLOT, OCT_W), BF16),
            pltpu.VMEM((slots, D), BF16),
        ]
        + Gather.scratch([s.shape for s in slabs], n)
        + (
            Gather.scratch([qkv_slab.shape], n)
            + [pltpu.VMEM((n * qkv_slab.shape[0], D), BF16), pltpu.SemaphoreType.DMA((n,))]
            if fused
            else []
        ),
        compiler_params=remote_params(collective_ids[0]),
        name="attention_forward",
    )(tokens, gains, shifts, head_biases, table, index, regions, *slabs, qkv_slab)
    weights = [g.reshape(-1, D) for g in results[5:]]
    if not fused:
        weights.append(qkv_slab)
    return results[:5], weights


def mlp(xs, mixed, out_grad, wproj, w1, w2, gains, shifts, hidden_bias):
    steps = out_grad.shape[0] // STEP_ROWS
    hidden = w1.shape[0]
    return pl.pallas_call(
        mlp_kernel,
        grid=(steps,),
        out_shape=(
            shape_of(out_grad.shape, F32),
            shape_of(xs.shape, F32),
            shape_of(w1.shape, BF16),
            shape_of(w2.shape, BF16),
            shape_of(wproj.shape, BF16),
            shape_of((1, hidden), F32),
            shape_of((4, D), F32),
        ),
        in_specs=[
            rows_of(STEP_SLOTS, D),
            rows_of(STEP_SLOTS, D),
            rows_of(STEP_ROWS, D),
            whole(wproj.shape),
            whole(w1.shape),
            whole(w2.shape),
            whole(gains.shape),
            whole(shifts.shape),
            whole((1, hidden)),
        ],
        out_specs=(
            rows_of(STEP_ROWS, D),
            rows_of(STEP_SLOTS, D),
            whole(w1.shape),
            whole(w2.shape),
            whole(wproj.shape),
            whole((1, hidden)),
            whole((4, D)),
        ),
        scratch_shapes=[
            pltpu.VMEM(w1.shape, F32),
            pltpu.VMEM(w2.shape, F32),
            pltpu.VMEM(wproj.shape, F32),
            pltpu.VMEM((STEP_ROWS, D), F32),
            pltpu.VMEM((STEP_ROWS, D), F32),
            pltpu.VMEM((STEP_ROWS, D), BF16),
            pltpu.VMEM((STEP_ROWS, D), BF16),
            pltpu.VMEM((STEP_SLOTS, D), F32),
            pltpu.VMEM((STEP_ROWS, D), F32),
        ],
        compiler_params=PARAMS,
        name="mlp",
    )(xs, mixed, out_grad, wproj, w1, w2, gains, shifts, hidden_bias.reshape(1, hidden))


def attention_backward(
    dy,
    xs,
    a1,
    qkv,
    probs,
    wqkv,
    wproj,
    gains,
    index,
    hidden_sum,
    sums2,
    grads,
    momenta,
    qkv_momentum,
    ndp,
    nt,
    images,
    collective_id,
):
    n = ndp * nt
    rows = [m.shape[0] for m in momenta]
    qkv_rows = qkv_momentum.shape[0]
    steps = dy.shape[0] // STEP_SLOTS
    grads = tuple(g.reshape(n, r, D) for g, r in zip(grads, rows))
    any_ = pl.BlockSpec(memory_space=pl.ANY)
    early = lambda i: (jnp.minimum(i, steps - 1), 0)
    late = lambda i: (jnp.maximum(i - steps, 0), 0)
    both = lambda i: (lax.rem(i, steps), 0)
    tall0, tall1 = padded((qkv_rows, rows[0])), padded(rows[1:])
    small_steps = 3 + (ndp // 2 - 1).bit_length()
    return pl.pallas_call(
        functools.partial(attention_backward_kernel, ndp, nt, images, steps),
        grid=(2 * steps,),
        out_shape=(shape_of((steps * STEP_ROWS, D), F32),)
        + tuple(shape_of((r, D), F32) for r in rows + [qkv_rows])
        + (
            shape_of((ndp, nt, tall0, D), BF16),
            shape_of((ndp, nt, tall1, D), BF16),
            shape_of((SMALL_ROWS, D), F32),
        ),
        in_specs=[
            pl.BlockSpec((STEP_SLOTS, D), both),
            pl.BlockSpec((STEP_SLOTS, D), late),
            pl.BlockSpec((STEP_SLOTS, D), early),
            pl.BlockSpec((STEP_SLOTS, 3 * D), early),
            pl.BlockSpec((STEP_SLOTS * OCTS * PAIRS, LANES), early),
            whole(wqkv.shape),
            whole(wproj.shape),
            whole(gains.shape),
            whole(index.shape),
            whole(hidden_sum.shape),
            whole(sums2.shape),
            any_,
            any_,
            any_,
        ]
        + [whole((r, D)) for r in rows + [qkv_rows]],
        out_specs=(pl.BlockSpec((STEP_ROWS, D), late),)
        + tuple(whole((r, D)) for r in rows + [qkv_rows])
        + (any_, any_, whole((SMALL_ROWS, D))),
        scratch_shapes=[
            pltpu.VMEM(wqkv.shape, F32),
            pltpu.VMEM((n, qkv_rows, D), BF16),
            pltpu.VMEM((STEP_SLOTS, D), BF16),
            pltpu.VMEM((steps * STEP_SLOTS, 3 * D), BF16),
            pltpu.VMEM((ROWS_S, OCT_W), BF16),
            pltpu.VMEM((2 * SLOT, OCT_W), BF16),
            pltpu.VMEM((STEP_SLOTS, D), F32),
            pltpu.VMEM((OCTS, ROWS_S, LANES), F32),
            pltpu.VMEM((2, D), F32),
            pltpu.VMEM((2, D), F32),
            pltpu.VMEM((LANES, LANES), F32),
            pltpu.VMEM((SLOT, LANES), F32),
            pltpu.VMEM((HEADS, 2 * LANES), F32),
            pltpu.VMEM((2, tall0, D), BF16),
            pltpu.VMEM((2, tall1, D), BF16),
            pltpu.VMEM((small_steps + 1, SMALL_ROWS, D), F32),
            pltpu.VMEM((small_steps, SMALL_ROWS, D), F32),
            pltpu.SemaphoreType.DMA((small_steps,)),
            pltpu.SemaphoreType.DMA((small_steps,)),
        ]
        + Share.scratch(n, nt)
        + Share.scratch(n, nt)
        + Reduce.scratch(rows, n)
        + Reduce.scratch([qkv_rows], n),
        compiler_params=remote_params(collective_id),
        name="attention_backward",
    )(
        dy,
        xs,
        a1,
        qkv,
        probs,
        wqkv,
        wproj,
        gains,
        index,
        hidden_sum,
        sums2,
        *grads,
        *momenta,
        qkv_momentum,
    )


ORDER = (0, 2, 1, 3)
WIDE = (True, True, False, False)
FACTORS = (
    math.sqrt(3.0),
    math.sqrt(max(1.0, FF / D)),
    1.0,
    math.sqrt(max(1.0, D / FF)),
)


def as_slab(block, wide):
    return block.reshape(D, -1).T if wide else block.reshape(-1, D)


def as_block(slab, like, wide):
    return (slab.T if wide else slab).reshape(like.shape)


def shards(
    tokens,
    out_grad,
    qkv_weight,
    proj_weight,
    fc1_weight,
    fc2_weight,
    qkv_momentum,
    proj_momentum,
    fc1_momentum,
    fc2_momentum,
    norm_gains,
    shift_biases,
    head_biases,
    hidden_bias,
    position_table,
    gain_momentum,
    shift_momentum,
    head_bias_momentum,
    hidden_bias_momentum,
    table_momentum,
    region_ids,
    position_index,
):
    devices = lax.axis_size("dp") * lax.axis_size("tensor")
    images = tokens.shape[0] // AREA * devices
    blocks = (qkv_weight, fc1_weight, proj_weight, fc2_weight)
    weights = tuple(as_slab(w, wide) for w, wide in zip(blocks, WIDE))
    momenta = tuple(
        as_slab(m, wide)
        for m, wide in zip((qkv_momentum, fc1_momentum, proj_momentum, fc2_momentum), WIDE)
    )
    ndp, nt = lax.axis_size("dp"), lax.axis_size("tensor")
    forward, gathered = attention_forward(
        tokens,
        norm_gains,
        shift_biases,
        head_biases,
        position_table.T,
        position_index,
        region_ids,
        weights[1:],
        weights[0],
        ndp,
        nt,
        (1, 0),
    )
    xs, a1, qkv, probs, mixed = forward
    w1, wproj, w2, wqkv = gathered
    output, dy, g1, g2, gproj, hidden_sum, sums2 = mlp(
        xs, mixed, out_grad, wproj, w1, w2, norm_gains, shift_biases, hidden_bias
    )
    input_grad, slab2, slab1, slab3, slab0, bundle0, bundle1, total = attention_backward(
        dy,
        xs,
        a1,
        qkv,
        probs,
        wqkv,
        wproj,
        norm_gains,
        position_index,
        hidden_sum,
        sums2,
        (gproj, g1, g2),
        (momenta[2], momenta[1], momenta[3]),
        momenta[0],
        ndp,
        nt,
        images,
        2,
    )
    small_params = (norm_gains, shift_biases, head_biases, hidden_bias.reshape(1, -1), position_table.T)
    small_moms = (
        gain_momentum,
        shift_momentum,
        head_bias_momentum,
        hidden_bias_momentum.reshape(1, -1),
        table_momentum.T,
    )
    slab_grads = (slab0, slab1, slab2, slab3)
    landed = newton_schulz((bundle0, bundle1), 3)
    rates = tuple(MATRIX_RATE * factor for factor in FACTORS)
    results = finish(landed, total, slab_grads, momenta, weights, small_params, small_moms, rates)
    slab_grads, new_weights, new_momenta = (results[i * nt : (i + 1) * nt] for i in range(3))
    smalls = tuple(
        s.reshape(-1) if i % 5 == 3 else s.T if i % 5 == 4 else s
        for i, s in enumerate(results[3 * nt :])
    )

    def placed(slabs):
        placed = tuple(as_block(s, like, wide) for s, like, wide in zip(slabs, blocks, WIDE))
        return tuple(placed[i] for i in ORDER)

    return (
        (output, input_grad)
        + placed(slab_grads)
        + placed(new_weights)
        + placed(new_momenta)
        + smalls
    )


def solution(mesh):
    rows = P(("dp", "tensor"), None)
    wide, tall = P(None, "tensor", "dp"), P("tensor", "dp", None)
    matrices = (wide, tall, wide, tall)
    return jax.shard_map(
        shards,
        mesh=mesh,
        in_specs=(rows, rows) + matrices * 2 + (P(),) * 12,
        out_specs=(rows, rows) + matrices * 3 + (P(),) * 15,
        check_vma=False,
    )
```
